32 devices in a mesh: patch: 4 (over z), seq: 4 (over y, x), req: 2 (over core).
Axes of the slice: x: 2, y: 2, z: 4, core: 2. Of those that a mesh axis runs over, the one named last changes fastest.
Arguments:
- query: bfloat16 [4, 8, 3584], P(None, ('patch', 'req')), may hold values from -20 to 20
- text_cache: bfloat16 [4, 8, 3072, 1024], P(None, ('patch', 'req'), 'seq'), may hold values from -6 to 6
- text_len: int32 [8], P(('patch', 'req')), may hold values from 0 to 3072
- image_rows: bfloat16 [4, 8192, 1024], P(None, ('patch', 'seq', 'req')), may hold values from -6 to 6
- patch_map: int32 [8192], P(('patch', 'seq', 'req')), may hold values from 0 to 7, as said below
- image_places: int32 [8192], P(('patch', 'seq', 'req')), may hold values from 0 to 1023, as said below
Outputs:
- attended: bfloat16 [4, 8, 3584], P(None, ('patch', 'req'), 'seq')
- image_cache: bfloat16 [4, 8, 1024, 1024], P(None, ('patch', 'req'), 'seq')
The draws below stay inside these ranges and needn't reach their ends.
Inputs may be any that keep to these rules, and one draw needn't show every extreme that they name: `patch_map`: each aligned block of 256 rows (the rows of one prefill device) holds exactly 32 rows of every request. `image_places`: together with patch_map every pair of request and position occurs exactly once. The rows of a device whose seq index is s have positions from s * 256 to (s + 1) * 256 - 1.
All inputs are finite; a program needn't handle non-finite values.
Results may differ from the reference program's by a relative error of at most 0.0026.
Values may be sent and summed in bfloat16 or wider, within the bound.
No kernel may reach another device: no remote copies, remote signals or barrier semaphores. Data moves between devices by JAX's collectives and lax.ppermute only.
A program may use at most 64 MiB of HBM per device.

```python
import math
import jax
import jax.numpy as jnp
from jax import lax

HEADS = 28
KV_HEADS = 4
HEAD_DIM = 128
LAYERS = 4
IMG = 1024
TXT = 3072
REQUESTS = 8
KVW = 512
N_PATCH = 4
N_SEQ = 4
N_REQ = 2


def layout_rows(key):
    groups = N_PATCH * N_REQ
    band_size = IMG // N_SEQ
    per_source = band_size // groups
    device_count = N_PATCH * N_SEQ * N_REQ
    pair_keys = jax.random.split(jax.random.fold_in(key, 7001), N_SEQ * REQUESTS)
    shuffled = jax.vmap(lambda piece: jax.random.permutation(piece, band_size))(pair_keys)
    shuffled = shuffled.astype(jnp.int32).reshape(N_SEQ, REQUESTS, N_PATCH, N_REQ, per_source)
    band_start = (jnp.arange(N_SEQ, dtype=jnp.int32) * band_size)[:, None, None, None, None]
    places = shuffled + band_start
    owners = jnp.broadcast_to(jnp.arange(REQUESTS, dtype=jnp.int32)[None, :, None, None, None], places.shape)
    places = jnp.transpose(places, (2, 0, 3, 1, 4)).reshape(device_count, REQUESTS * per_source)
    owners = jnp.transpose(owners, (2, 0, 3, 1, 4)).reshape(device_count, REQUESTS * per_source)
    row_keys = jax.random.split(jax.random.fold_in(key, 7002), device_count)
    mixing = jax.vmap(lambda piece: jax.random.permutation(piece, REQUESTS * per_source))(row_keys)
    mixing = mixing.astype(jnp.int32)
    places = jnp.take_along_axis(places, mixing, axis=1).reshape(-1)
    owners = jnp.take_along_axis(owners, mixing, axis=1).reshape(-1)
    return (owners, places)


def draw_patch_map(key, part):
    return layout_rows(key)[0]


def draw_image_places(key, part):
    return layout_rows(key)[1]


def draw_query(key, part):
    shape = (LAYERS, REQUESTS, HEADS * HEAD_DIM)
    noise_key = jax.random.fold_in(key, 7004)
    values = jnp.clip(2.5 * jax.random.normal(noise_key, shape, jnp.float32), -12.0, 12.0)
    return values.astype(jnp.bfloat16)


def draw_image_rows(key, part):
    shape = (LAYERS, REQUESTS * IMG, 2 * KV_HEADS * HEAD_DIM)
    noise_key = jax.random.fold_in(key, 7005)
    values = jnp.clip(jax.random.normal(noise_key, shape, jnp.float32), -6.0, 6.0)
    return values.astype(jnp.bfloat16)


def place_ends(values, own_key, least, top_value):
    index_at = [jax.random.randint(jax.random.fold_in(own_key, axis), (), 0, length) for axis, length in enumerate(values.shape)]
    longest = values.shape.index(max(values.shape))
    neighbour = index_at[:longest] + [(index_at[longest] + 1) % values.shape[longest]] + index_at[longest + 1:]
    return values.at[tuple(index_at)].set(least).at[tuple(neighbour)].set(top_value)


def block_levels(rng, shape, cuts, low, largest):
    loudness, own = 1.0, jax.random.fold_in(rng, 6)
    for position, shards_of in cuts:
        steps = jnp.exp(jax.random.uniform(jax.random.fold_in(own, position), (shards_of,), jnp.float32, low / len(cuts), largest / len(cuts)))
        loudness = loudness * jnp.repeat(steps, shape[position] // shards_of).reshape([-1 if axis == position else 1 for axis in range(len(shape))])
    return loudness


def bell_draw(rng, dims, deviation, most, cuts=(), kind=jnp.bfloat16):
    result = deviation * jax.random.normal(rng, dims, jnp.float32)
    if cuts:
        result = result * block_levels(rng, dims, cuts, -0.22, 0.18)
    return jnp.clip(result, -most, most).astype(kind)


def setup_inputs(seed: int = 0) -> dict:
    seeds = jax.random.split(jax.random.key(seed), 7)
    return {
        "query": draw_query(jax.random.fold_in(seeds[6], 71), 0),
        "text_cache": bell_draw(seeds[1], (LAYERS, REQUESTS, TXT, 2 * KVW), 1.0, 6.0, ((1, 8), (2, 4))),
        "text_len": place_ends(jax.random.randint(seeds[2], (REQUESTS,), 0, TXT + 1), jax.random.fold_in(seeds[2], 1), 0, TXT).astype(jnp.int32),
        "image_rows": draw_image_rows(jax.random.fold_in(seeds[6], 71), 0),
        "patch_map": draw_patch_map(jax.random.fold_in(seeds[6], 71), 0),
        "image_places": draw_image_places(jax.random.fold_in(seeds[6], 71), 0),
    }


def attend_one(query_row, image_block, text_block, length):
    kv_width = KV_HEADS * HEAD_DIM
    group = HEADS // KV_HEADS
    band_size = IMG // N_SEQ
    text_band = TXT // N_SEQ
    image_banded = image_block.reshape(N_SEQ, band_size, 2 * kv_width)
    text_banded = text_block.reshape(N_SEQ, text_band, 2 * kv_width)
    keys_all = jnp.concatenate([image_banded, text_banded], axis=1)
    width = band_size + text_band
    keys = keys_all[:, :, :kv_width].reshape(N_SEQ, width, KV_HEADS, HEAD_DIM).astype(jnp.float32)
    values = keys_all[:, :, kv_width:].reshape(N_SEQ, width, KV_HEADS, HEAD_DIM).astype(jnp.float32)
    queries = query_row.reshape(KV_HEADS, group, HEAD_DIM).astype(jnp.float32)
    scores = jnp.einsum('kgd,stkd->skgt', queries, keys) * (1.0 / math.sqrt(HEAD_DIM))
    inner = jnp.arange(width, dtype=jnp.int32)
    bands = jnp.arange(N_SEQ, dtype=jnp.int32)
    text_pos = bands[:, None] * text_band + inner[None, :] - band_size
    used = (inner[None, :] < band_size) | (text_pos < length)
    scores = jnp.where(used[:, None, None, :], scores, -jnp.inf)
    band_top = lax.optimization_barrier(jnp.max(scores, axis=-1, keepdims=True))
    weights = jnp.exp(scores - band_top)
    band_total = lax.optimization_barrier(jnp.sum(weights, axis=-1))
    rounded = lax.optimization_barrier(weights.astype(jnp.bfloat16)).astype(jnp.float32)
    band_sum = jnp.einsum('skgt,stkd->skgd', rounded, values)
    band_top = band_top[..., 0]
    top = lax.optimization_barrier(jnp.max(band_top, axis=0, keepdims=True))
    factor = jnp.exp(band_top - top)
    total = lax.optimization_barrier(jnp.sum(factor * band_total, axis=0))
    summed = lax.optimization_barrier(jnp.sum(factor[..., None] * band_sum, axis=0))
    return (summed / total[..., None]).reshape(HEADS * HEAD_DIM).astype(jnp.bfloat16)

def attend_packed(packed):
    return attend_one(packed[0], packed[1], packed[2], packed[3])

def reference(query, text_cache, text_len, image_rows, patch_map, image_places):
    order = jnp.argsort(patch_map * IMG + image_places)
    image_cache = jnp.take(image_rows, order, axis=1).reshape(LAYERS, REQUESTS, IMG, image_rows.shape[2])

    def per_layer(packed):
        return lax.map(attend_packed, (packed[0], packed[1], packed[2], text_len))
    attended = lax.map(per_layer, (query, image_cache, text_cache))
    return (attended, image_cache)
```

```python
import functools
import math

import jax
import jax.numpy as jnp
from jax import lax
from jax.experimental import pallas as pl
from jax.experimental.pallas import tpu as pltpu
from jax.sharding import PartitionSpec as P

HEADS = 28
KV_HEADS = 4
HEAD_DIM = 128
LANES = 128
SUBLANES = 8
MASKED = -1e30


def gray(index):
    return index ^ (index >> 1)


def step_of(source, target, count):
    if count & (count - 1) == 0:
        return (gray(target) - gray(source)) & (count - 1)
    return (target - source + count) % count


def group_kernel(patch_count, req_count, map_ref, place_ref, rows_ref, *outs):
    layers, src_rows, width = rows_ref.shape
    groups = patch_count * req_count
    per = src_rows // groups
    blocks = width // LANES
    me = lax.axis_index("patch")
    mine = lax.axis_index("req")
    band_start = lax.axis_index("seq") * src_rows
    shape = (src_rows, src_rows)
    down = lax.broadcasted_iota(jnp.int32, shape, 0)
    across = lax.broadcasted_iota(jnp.int32, shape, 1)
    owner = map_ref[...]
    owner_row = jnp.broadcast_to(owner, shape)
    owner_col = jnp.sum(
        jnp.where(down == across, owner_row.astype(jnp.float32), 0.0), axis=1, keepdims=True
    ).astype(jnp.int32)
    ahead = (owner_row == owner_col) & (down < across)
    rank = jnp.sum(jnp.where(ahead, 1.0, 0.0), axis=0, keepdims=True).astype(jnp.int32)
    step = step_of(me, owner // req_count, patch_count)
    turn = (owner % req_count - mine + req_count) % req_count
    slot = (step * req_count + turn) * per + rank
    choose = jnp.where(down == slot, 1.0, 0.0).astype(jnp.bfloat16)
    local = place_ref[...] - band_start
    line = lax.broadcasted_iota(jnp.int32, (SUBLANES, src_rows), 0)
    digits = jnp.where(line == 0, local & (LANES - 1), jnp.where(line == 1, local // LANES, 0))
    places = lax.dot_general(
        digits.astype(jnp.float32).astype(jnp.bfloat16),
        choose,
        (((1,), (1,)), ((), ())),
        preferred_element_type=jnp.float32,
    ).astype(jnp.bfloat16)
    for layer in range(layers):
        moved = jnp.dot(
            choose, rows_ref[layer], preferred_element_type=jnp.float32
        ).astype(jnp.bfloat16)
        for k in range(groups):
            for c in range(blocks):
                outs[k][pl.ds((layer * blocks + c) * per, per), :] = moved[
                    k * per : (k + 1) * per, c * LANES : (c + 1) * LANES
                ]
    for k in range(groups):
        tile = k * per // LANES
        outs[k][pl.ds(layers * blocks * per, SUBLANES), :] = places[
            :, tile * LANES : (tile + 1) * LANES
        ]


def group_rows(patch_map, image_places, image_rows, patch_count, req_count):
    layers, src_rows, width = image_rows.shape
    groups = patch_count * req_count
    chunk_rows = layers * src_rows * width // groups // LANES + SUBLANES
    vmem = pl.BlockSpec(memory_space=pltpu.VMEM)
    return pl.pallas_call(
        functools.partial(group_kernel, patch_count, req_count),
        out_shape=[jax.ShapeDtypeStruct((chunk_rows, LANES), jnp.bfloat16)] * groups,
        in_specs=[vmem] * 3,
        out_specs=[vmem] * groups,
        cost_estimate=pl.CostEstimate(
            flops=2 * layers * src_rows * src_rows * width,
            bytes_accessed=4 * layers * src_rows * width,
            transcendentals=0,
        ),
        name="group_rows",
    )(patch_map.reshape(1, src_rows), image_places.reshape(1, src_rows), image_rows)


def heads_of(line, group):
    row = lax.broadcasted_iota(jnp.int32, (SUBLANES, HEAD_DIM), 0)
    tiles = []
    for g in range(KV_HEADS):
        tile = jnp.zeros((SUBLANES, HEAD_DIM), jnp.float32)
        for i in range(group):
            h = g * group + i
            tile = jnp.where(row == i, line[:, h * HEAD_DIM : (h + 1) * HEAD_DIM], tile)
        tiles.append(tile)
    return jnp.concatenate(tiles, axis=0).astype(jnp.bfloat16)


def attend(queries, keys, values, used, scale):
    scores = jnp.concatenate(
        [
            lax.dot_general(
                queries[g * SUBLANES : (g + 1) * SUBLANES],
                keys[g],
                (((1,), (1,)), ((), ())),
                preferred_element_type=jnp.float32,
            )
            for g in range(KV_HEADS)
        ],
        axis=0,
    )
    scores = scores * scale
    if used is not None:
        scores = jnp.where(used, scores, MASKED)
    top = jnp.max(scores, axis=1, keepdims=True)
    weights = jnp.exp(scores - top)
    if used is not None:
        weights = jnp.where(used, weights, 0.0)
    total = jnp.sum(weights, axis=1, keepdims=True)
    rounded = weights.astype(jnp.bfloat16)
    summed = jnp.concatenate(
        [
            jnp.dot(
                rounded[g * SUBLANES : (g + 1) * SUBLANES],
                values[g],
                preferred_element_type=jnp.float32,
            )
            for g in range(KV_HEADS)
        ],
        axis=0,
    )
    return top, total, summed


def text_kernel(scale, len_ref, query_ref, text_ref, q_ref, top_ref, total_ref, sum_ref):
    text_dev, width = text_ref.shape
    group = query_ref.shape[1] // HEAD_DIM // KV_HEADS
    queries = heads_of(query_ref[...].astype(jnp.float32), group)
    q_ref[...] = queries
    rows = KV_HEADS * SUBLANES
    positions = lax.axis_index("seq") * text_dev + lax.broadcasted_iota(
        jnp.int32, (rows, text_dev), 1
    )
    keys = [text_ref[:, g * HEAD_DIM : (g + 1) * HEAD_DIM] for g in range(KV_HEADS)]
    values = [
        text_ref[:, width // 2 + g * HEAD_DIM : width // 2 + (g + 1) * HEAD_DIM]
        for g in range(KV_HEADS)
    ]
    top, total, summed = attend(queries, keys, values, positions < len_ref[0], scale)
    top_ref[...] = jnp.broadcast_to(top, (rows, LANES))
    total_ref[...] = jnp.broadcast_to(total, (rows, LANES))
    sum_ref[...] = summed


def text_part(query, text_cache, text_len, scale):
    layers, _, query_width = query.shape
    text_dev, width = text_cache.shape[2:]
    rows = KV_HEADS * SUBLANES
    part = pl.BlockSpec((None, rows, LANES), lambda layer, _: (layer, 0, 0))
    return pl.pallas_call(
        functools.partial(text_kernel, scale),
        out_shape=[
            jax.ShapeDtypeStruct((layers, rows, HEAD_DIM), jnp.bfloat16),
            jax.ShapeDtypeStruct((layers, rows, LANES), jnp.float32),
            jax.ShapeDtypeStruct((layers, rows, LANES), jnp.float32),
            jax.ShapeDtypeStruct((layers, rows, HEAD_DIM), jnp.float32),
        ],
        grid_spec=pltpu.PrefetchScalarGridSpec(
            num_scalar_prefetch=1,
            grid=(layers,),
            in_specs=[
                pl.BlockSpec((None, 1, query_width), lambda layer, _: (layer, 0, 0)),
                pl.BlockSpec((None, None, text_dev, width), lambda layer, _: (layer, 0, 0, 0)),
            ],
            out_specs=[part] * 4,
        ),
        cost_estimate=pl.CostEstimate(
            flops=8 * layers * SUBLANES * LANES * text_dev * width,
            bytes_accessed=2 * layers * text_dev * width,
            transcendentals=layers * rows * text_dev,
        ),
        name="text_part",
    )(text_len, query, text_cache)


def image_kernel(scale, groups, q_ref, top_ref, total_ref, sum_ref, *refs):
    chunks, outs, packed = refs[:groups], refs[groups:-1], refs[-1]
    layers = q_ref.shape[0]
    blocks = 2 * KV_HEADS
    per = (chunks[0].shape[0] - SUBLANES) // layers // blocks
    lane = lax.broadcasted_iota(jnp.int32, (SUBLANES, LANES), 1)
    for layer in range(layers):

        def column(c):
            span = pl.ds((layer * blocks + c) * per, per)
            return jnp.concatenate([chunk[span, :] for chunk in chunks], axis=0)

        keys = [column(g) for g in range(KV_HEADS)]
        values = [column(KV_HEADS + g) for g in range(KV_HEADS)]
        top, total, summed = attend(q_ref[layer], keys, values, None, scale)
        text_top = top_ref[layer][:, :1]
        text_total = total_ref[layer][:, :1]
        both = jnp.maximum(top, text_top)
        image_factor = jnp.exp(top - both)
        text_factor = jnp.exp(text_top - both)
        total = image_factor * total + text_factor * text_total
        summed = image_factor * summed + text_factor * sum_ref[layer]
        for g in range(KV_HEADS):
            span = slice(g * SUBLANES, (g + 1) * SUBLANES)
            packed[g, pl.ds(layer * SUBLANES, SUBLANES), :] = summed[span]
            packed[g, pl.ds((layers + layer) * SUBLANES, SUBLANES), :] = jnp.where(
                lane == 0, both[span], total[span]
            )
    me = lax.axis_index("seq")
    for k in range(KV_HEADS):
        outs[k][...] = packed[me ^ k]


def image_part(parts, chunks, scale):
    layers = parts[0].shape[0]
    groups = len(chunks)
    shape = (2 * layers * SUBLANES, LANES)
    vmem = pl.BlockSpec(memory_space=pltpu.VMEM)
    rows = chunks[0].shape[0]
    return pl.pallas_call(
        functools.partial(image_kernel, scale, groups),
        out_shape=[jax.ShapeDtypeStruct(shape, jnp.float32)] * KV_HEADS,
        in_specs=[vmem] * (4 + groups),
        out_specs=[vmem] * KV_HEADS,
        scratch_shapes=[pltpu.VMEM((KV_HEADS,) + shape, jnp.float32)],
        cost_estimate=pl.CostEstimate(
            flops=8 * SUBLANES * rows * LANES * groups,
            bytes_accessed=2 * rows * LANES * groups,
            transcendentals=SUBLANES * rows * groups,
        ),
        name="image_part",
    )(*parts, *chunks)


def place_kernel(groups, *refs):
    chunks, out_ref = refs[:groups], refs[-1]
    layers, band, width = out_ref.shape
    blocks = width // LANES
    per = band // groups
    base = layers * blocks * per
    lane = lax.broadcasted_iota(jnp.int32, (SUBLANES, LANES), 1)
    tiles = []
    for tile in range(band // LANES):
        row = jnp.zeros((SUBLANES, LANES), jnp.float32)
        for k in range(groups):
            if k * per // LANES == tile:
                extra = chunks[k][pl.ds(base, SUBLANES), :].astype(jnp.float32)
                inside = (lane >= k * per % LANES) & (lane < k * per % LANES + per)
                row = jnp.where(inside, extra, row)
        tiles.append(row)
    digits = jnp.concatenate(tiles, axis=1).astype(jnp.int32)
    places = digits[0:1] + digits[1:2] * LANES
    down = lax.broadcasted_iota(jnp.int32, (band, band), 0)
    choose = jnp.where(down == places, 1.0, 0.0).astype(jnp.bfloat16)
    for layer in range(layers):
        for c in range(blocks):
            span = pl.ds((layer * blocks + c) * per, per)
            column = jnp.concatenate([chunk[span, :] for chunk in chunks], axis=0)
            out_ref[layer, :, c * LANES : (c + 1) * LANES] = jnp.dot(
                choose, column, preferred_element_type=jnp.float32
            ).astype(jnp.bfloat16)


def place_rows(chunks, layers, band, width):
    groups = len(chunks)
    vmem = pl.BlockSpec(memory_space=pltpu.VMEM)
    return pl.pallas_call(
        functools.partial(place_kernel, groups),
        out_shape=jax.ShapeDtypeStruct((layers, band, width), jnp.bfloat16),
        in_specs=[vmem] * groups,
        out_specs=vmem,
        cost_estimate=pl.CostEstimate(
            flops=2 * layers * band * band * width,
            bytes_accessed=4 * layers * band * width,
            transcendentals=0,
        ),
        name="place_rows",
    )(*chunks)


def merge_kernel(group, *refs):
    parts, out_ref = refs[:-1], refs[-1]
    half = parts[0].shape[0] // 2
    layers = half // SUBLANES
    tops = [part[pl.ds(half, half), :][:, 0:1] for part in parts]
    totals = [part[pl.ds(half, half), :][:, 1:2] for part in parts]
    top = functools.reduce(jnp.maximum, tops)
    factors = [jnp.exp(t - top) for t in tops]
    total = sum(f * t for f, t in zip(factors, totals))
    summed = sum(f * part[pl.ds(0, half), :] for f, part in zip(factors, parts))
    result = summed / total
    for layer in range(layers):
        for i in range(group):
            row = layer * SUBLANES + i
            out_ref[pl.ds(layer, 1), i * HEAD_DIM : (i + 1) * HEAD_DIM] = result[row : row + 1]


def merge(parts, layers, group):
    vmem = pl.BlockSpec(memory_space=pltpu.VMEM)
    return pl.pallas_call(
        functools.partial(merge_kernel, group),
        out_shape=jax.ShapeDtypeStruct((layers, group * HEAD_DIM), jnp.float32),
        in_specs=[vmem] * len(parts),
        out_specs=vmem,
        name="merge",
    )(*parts)


def exchange_pairs(patch_count, req_count, step, turn):
    pairs = []
    for patch in range(patch_count):
        for req in range(req_count):
            target = next(p for p in range(patch_count) if step_of(patch, p, patch_count) == step)
            pairs.append(
                (patch * req_count + req, target * req_count + (req + turn) % req_count)
            )
    return pairs


def fast_body(query, text_cache, text_len, image_rows, patch_map, image_places):
    layers = query.shape[0]
    patch_count = lax.axis_size("patch")
    req_count = lax.axis_size("req")
    band, width = image_rows.shape[1:]
    group = HEADS // KV_HEADS
    scale = 1.0 / math.sqrt(HEAD_DIM)
    grouped = group_rows(patch_map, image_places, image_rows, patch_count, req_count)
    order = [k for k in range(1, len(grouped)) if k >= req_count]
    order += [k for k in range(1, len(grouped)) if k < req_count]
    chunks = [grouped[0]] + [None] * (len(grouped) - 1)
    for k in order:
        pairs = exchange_pairs(patch_count, req_count, k // req_count, k % req_count)
        chunks[k] = lax.ppermute(grouped[k], ("patch", "req"), pairs)
    parts = text_part(query, text_cache, text_len, scale)
    packed = image_part(parts, chunks, scale)
    gathered = [packed[0]]
    for k in range(1, KV_HEADS):
        gathered.append(lax.ppermute(packed[k], "seq", [(s, s ^ k) for s in range(KV_HEADS)]))
    image_cache = place_rows(chunks, layers, band, width)
    attended = merge(gathered, layers, group).astype(jnp.bfloat16)
    return attended[:, None, :], image_cache[:, None]


def plain_body(query, text_cache, text_len, image_rows, patch_map, image_places):
    layers, req_dev, query_width = query.shape
    text_dev = text_cache.shape[2]
    full_width = text_cache.shape[3]
    kv_width = full_width // 2
    head_dim = HEAD_DIM
    kv_heads = KV_HEADS
    heads = HEADS
    group = heads // kv_heads
    src_rows = image_rows.shape[1]
    patch_count = lax.axis_size("patch")
    req_count = lax.axis_size("req")
    seq_count = lax.axis_size("seq")
    seq_index = lax.axis_index("seq")
    per_source = src_rows // (patch_count * req_count * req_dev)
    band_size = per_source * patch_count * req_count
    scale = 1.0 / math.sqrt(head_dim)
    order = jnp.argsort(patch_map, stable=True)
    grouped = jnp.take(image_rows, order, axis=1)
    grouped_places = jnp.take(image_places, order)
    sending = grouped.reshape(layers, patch_count * req_count, req_dev, per_source, full_width)
    arrived = lax.all_to_all(sending, ("patch", "req"), split_axis=1, concat_axis=3, tiled=True)
    place_send = grouped_places.reshape(patch_count * req_count, req_dev, per_source)
    arrived_places = lax.all_to_all(
        place_send, ("patch", "req"), split_axis=0, concat_axis=2, tiled=True
    )
    image_block = arrived.reshape(layers, req_dev, band_size, full_width)
    local_places = arrived_places.reshape(req_dev, band_size) - seq_index * band_size
    inverse = jnp.argsort(local_places, axis=1)
    image_cache = jnp.take_along_axis(image_block, inverse[None, :, :, None], axis=2)
    queries = query.reshape(layers, req_dev, kv_heads, group, head_dim)
    text_keys = text_cache[..., :kv_width].reshape(layers, req_dev, text_dev, kv_heads, head_dim)
    text_values = text_cache[..., kv_width:].reshape(layers, req_dev, text_dev, kv_heads, head_dim)
    image_keys = image_block[..., :kv_width].reshape(layers, req_dev, band_size, kv_heads, head_dim)
    image_values = image_block[..., kv_width:].reshape(
        layers, req_dev, band_size, kv_heads, head_dim
    )
    positions = seq_index * text_dev + jnp.arange(text_dev, dtype=jnp.int32)
    used = positions[None, :] < text_len[:, None]
    text_raw = (
        jnp.einsum("lrkgd,lrtkd->lrkgt", queries, text_keys, preferred_element_type=jnp.float32)
        * scale
    )
    text_scores = jnp.where(used[None, :, None, None, :], text_raw, -jnp.inf)
    image_scores = (
        jnp.einsum("lrkgd,lrtkd->lrkgt", queries, image_keys, preferred_element_type=jnp.float32)
        * scale
    )
    local_top = jnp.maximum(jnp.max(text_scores, axis=-1), jnp.max(image_scores, axis=-1))
    text_weights = jnp.exp(text_scores - local_top[..., None])
    image_weights = jnp.exp(image_scores - local_top[..., None])
    local_total = jnp.sum(text_weights, axis=-1) + jnp.sum(image_weights, axis=-1)
    text_rounded = text_weights.astype(jnp.bfloat16)
    image_rounded = image_weights.astype(jnp.bfloat16)
    local_values = jnp.einsum(
        "lrkgt,lrtkd->lrkgd", image_rounded, image_values, preferred_element_type=jnp.float32
    )
    local_values = local_values + jnp.einsum(
        "lrkgt,lrtkd->lrkgd", text_rounded, text_values, preferred_element_type=jnp.float32
    )
    width_dev = query_width // seq_count
    top = lax.pmax(local_top, "seq")
    factor = jnp.exp(local_top - top)
    scaled_total = factor * local_total
    scaled_values = factor[..., None] * local_values
    total_sum, value_sum = lax.psum((scaled_total, scaled_values), "seq")
    result = (value_sum / total_sum[..., None]).reshape(layers, req_dev, query_width)
    attended = lax.dynamic_slice_in_dim(result, seq_index * width_dev, width_dev, 2).astype(
        jnp.bfloat16
    )
    return (attended, image_cache)


def body(query, text_cache, text_len, image_rows, patch_map, image_places):
    groups = lax.axis_size("patch") * lax.axis_size("req")
    band = image_rows.shape[1]
    per = band // groups
    fast = (
        query.shape[1] == 1
        and groups <= 16
        and band == per * groups
        and band % LANES == 0
        and per % 16 == 0
        and LANES % per == 0
        and lax.axis_size("seq") == KV_HEADS
        and HEADS // KV_HEADS <= SUBLANES
    )
    chosen = fast_body if fast else plain_body
    return chosen(query, text_cache, text_len, image_rows, patch_map, image_places)


def solution(mesh):
    return jax.shard_map(
        body,
        mesh=mesh,
        in_specs=(
            P(None, ("patch", "req"), None),
            P(None, ("patch", "req"), "seq", None),
            P(("patch", "req")),
            P(None, ("patch", "seq", "req"), None),
            P(("patch", "seq", "req")),
            P(("patch", "seq", "req")),
        ),
        out_specs=(P(None, ("patch", "req"), "seq"), P(None, ("patch", "req"), "seq", None)),
        check_vma=False,
    )
```

```python
import functools
import math

import jax
import jax.numpy as jnp
from jax import lax
from jax.experimental import pallas as pl
from jax.experimental.pallas import tpu as pltpu
from jax.sharding import PartitionSpec as P

HEADS = 28
KV_HEADS = 4
HEAD_DIM = 128
LANES = 128
SUBLANES = 8
MASKED = -1e30

VMEM_LIMIT = 16 * 1024 * 1024
WIDE_VMEM_LIMIT = 62 * 1024 * 1024


def gray(index):
    return index ^ (index >> 1)


def step_of(source, target, count):
    if count & (count - 1) == 0:
        return (gray(target) - gray(source) + count - 1) & (count - 1)
    return (target - source + count - 1) % count


def slot_choice(patch_count, req_count, owner, place):
    src_rows = owner.shape[1]
    per = src_rows // (patch_count * req_count)
    me = lax.axis_index("patch")
    mine = lax.axis_index("req")
    shape = (src_rows, src_rows)
    down = lax.broadcasted_iota(jnp.int32, shape, 0)
    across = lax.broadcasted_iota(jnp.int32, shape, 1)
    owner_row = jnp.broadcast_to(owner, shape)
    owner_col = jnp.sum(
        jnp.where(down == across, owner_row.astype(jnp.float32), 0.0), axis=1, keepdims=True
    ).astype(jnp.int32)
    ahead = (owner_row == owner_col) & (down < across)
    rank = jnp.sum(jnp.where(ahead, 1.0, 0.0), axis=0, keepdims=True).astype(jnp.int32)
    step = step_of(me, owner // req_count, patch_count)
    turn = (owner % req_count - mine + req_count) % req_count
    slot = (step * req_count + turn) * per + rank
    choose = jnp.where(down == slot, 1.0, 0.0).astype(jnp.bfloat16)
    local = place - lax.axis_index("seq") * src_rows
    line = lax.broadcasted_iota(jnp.int32, (SUBLANES, src_rows), 0)
    digits = jnp.where(line == 0, local & (LANES - 1), jnp.where(line == 1, local // LANES, 0))
    places = lax.dot_general(
        digits.astype(jnp.float32).astype(jnp.bfloat16),
        choose,
        (((1,), (1,)), ((), ())),
        preferred_element_type=jnp.float32,
    ).astype(jnp.bfloat16)
    return choose, places


def pack_slots(first, per, choose, places, layer_rows, layers, outs):
    for k, out in enumerate(outs):
        tile = (first + k) * per // LANES
        out[pl.ds(out.shape[0] - SUBLANES, SUBLANES), :] = places[
            :, tile * LANES : (tile + 1) * LANES
        ]
    taken = choose[first * per : (first + len(outs)) * per]
    for layer in range(layers):
        rows = layer_rows(layer)
        blocks = rows.shape[1] // LANES
        moved = jnp.dot(taken, rows, preferred_element_type=jnp.float32).astype(jnp.bfloat16)
        for k, out in enumerate(outs):
            for c in range(blocks):
                out[pl.ds((layer * blocks + c) * per, per), :] = moved[
                    k * per : (k + 1) * per, c * LANES : (c + 1) * LANES
                ]


def first_kernel(patch_count, req_count, map_hbm, place_hbm, rows_hbm, *refs):
    choose_ref, places_ref, *outs = refs[:-5]
    owner_ref, place_ref, rows_ref, small_sem, rows_sem = refs[-5:]
    layers, src_rows, _ = rows_hbm.shape
    small = [
        pltpu.make_async_copy(map_hbm, owner_ref, small_sem.at[0]),
        pltpu.make_async_copy(place_hbm, place_ref, small_sem.at[1]),
    ]
    loads = [
        pltpu.make_async_copy(rows_hbm.at[layer], rows_ref.at[layer], rows_sem.at[layer])
        for layer in range(layers)
    ]
    for copy in small + loads:
        copy.start()
    for copy in small:
        copy.wait()
    choose, places = slot_choice(patch_count, req_count, owner_ref[...], place_ref[...])
    choose_ref[...] = choose
    places_ref[...] = places

    def layer_rows(layer):
        loads[layer].wait()
        return rows_ref[layer]

    per = src_rows // (patch_count * req_count)
    pack_slots(0, per, choose, places, layer_rows, layers, outs)


def rest_kernel(first, per, choose_ref, places_ref, rows_ref, *outs):
    pack_slots(
        first,
        per,
        choose_ref[...],
        places_ref[...],
        lambda layer: rows_ref[layer],
        rows_ref.shape[0],
        outs,
    )


def group_rows(patch_map, image_places, image_rows, patch_count, req_count):
    layers, src_rows, width = image_rows.shape
    groups = patch_count * req_count
    per = src_rows // groups
    chunk = jax.ShapeDtypeStruct((layers * per * width // LANES + SUBLANES, LANES), jnp.bfloat16)
    hbm = pl.BlockSpec(memory_space=pltpu.HBM)
    vmem = pl.BlockSpec(memory_space=pltpu.VMEM)

    def cost(count):
        return pl.CostEstimate(
            flops=2 * layers * src_rows * per * count * width,
            bytes_accessed=2 * layers * (src_rows + per * count) * width,
            transcendentals=0,
        )

    choose, places, *first = pl.pallas_call(
        functools.partial(first_kernel, patch_count, req_count),
        out_shape=[
            jax.ShapeDtypeStruct((src_rows, src_rows), jnp.bfloat16),
            jax.ShapeDtypeStruct((SUBLANES, src_rows), jnp.bfloat16),
        ]
        + [chunk] * req_count,
        in_specs=[hbm] * 3,
        out_specs=[vmem] * (2 + req_count),
        scratch_shapes=[
            pltpu.VMEM((1, src_rows), jnp.int32),
            pltpu.VMEM((1, src_rows), jnp.int32),
            pltpu.VMEM(image_rows.shape, jnp.bfloat16),
            pltpu.SemaphoreType.DMA((2,)),
            pltpu.SemaphoreType.DMA((layers,)),
        ],
        cost_estimate=cost(req_count),
        compiler_params=pltpu.CompilerParams(vmem_limit_bytes=WIDE_VMEM_LIMIT),
        name="group_first",
    )(patch_map.reshape(1, src_rows), image_places.reshape(1, src_rows), image_rows)
    rest = pl.pallas_call(
        functools.partial(rest_kernel, req_count, per),
        out_shape=[chunk] * (groups - req_count),
        in_specs=[vmem] * 3,
        out_specs=[vmem] * (groups - req_count),
        cost_estimate=cost(groups - req_count),
        compiler_params=pltpu.CompilerParams(vmem_limit_bytes=VMEM_LIMIT),
        name="group_rest",
    )(choose, places, image_rows)
    return [*first, *rest]


def heads_of(line, group):
    row = lax.broadcasted_iota(jnp.int32, (SUBLANES, HEAD_DIM), 0)
    tiles = []
    for g in range(KV_HEADS):
        tile = jnp.zeros((SUBLANES, HEAD_DIM), jnp.float32)
        for i in range(group):
            h = g * group + i
            tile = jnp.where(row == i, line[:, h * HEAD_DIM : (h + 1) * HEAD_DIM], tile)
        tiles.append(tile)
    return jnp.concatenate(tiles, axis=0).astype(jnp.bfloat16)


def attend(queries, keys, values, used, scale):
    scores = jnp.concatenate(
        [
            lax.dot_general(
                queries[g * SUBLANES : (g + 1) * SUBLANES],
                keys[g],
                (((1,), (1,)), ((), ())),
                preferred_element_type=jnp.float32,
            )
            for g in range(KV_HEADS)
        ],
        axis=0,
    )
    scores = scores * scale
    if used is not None:
        scores = jnp.where(used, scores, MASKED)
    top = jnp.max(scores, axis=1, keepdims=True)
    weights = jnp.exp(scores - top)
    if used is not None:
        weights = jnp.where(used, weights, 0.0)
    total = jnp.sum(weights, axis=1, keepdims=True)
    rounded = weights.astype(jnp.bfloat16)
    summed = jnp.concatenate(
        [
            jnp.dot(
                rounded[g * SUBLANES : (g + 1) * SUBLANES],
                values[g],
                preferred_element_type=jnp.float32,
            )
            for g in range(KV_HEADS)
        ],
        axis=0,
    )
    return top, total, summed


def text_kernel(scale, len_ref, query_ref, text_ref, q_ref, top_ref, total_ref, sum_ref):
    text_dev, width = text_ref.shape
    group = query_ref.shape[1] // HEAD_DIM // KV_HEADS
    queries = heads_of(query_ref[...].astype(jnp.float32), group)
    q_ref[...] = queries
    rows = KV_HEADS * SUBLANES
    positions = lax.axis_index("seq") * text_dev + lax.broadcasted_iota(
        jnp.int32, (rows, text_dev), 1
    )
    keys = [text_ref[:, g * HEAD_DIM : (g + 1) * HEAD_DIM] for g in range(KV_HEADS)]
    values = [
        text_ref[:, width // 2 + g * HEAD_DIM : width // 2 + (g + 1) * HEAD_DIM]
        for g in range(KV_HEADS)
    ]
    top, total, summed = attend(queries, keys, values, positions < len_ref[0], scale)
    top_ref[...] = jnp.broadcast_to(top, (rows, LANES))
    total_ref[...] = jnp.broadcast_to(total, (rows, LANES))
    sum_ref[...] = summed


def text_part(query, text_cache, text_len, scale):
    layers, _, query_width = query.shape
    text_dev, width = text_cache.shape[2:]
    rows = KV_HEADS * SUBLANES
    part = pl.BlockSpec((None, rows, LANES), lambda layer, _: (layer, 0, 0))
    return pl.pallas_call(
        functools.partial(text_kernel, scale),
        out_shape=[
            jax.ShapeDtypeStruct((layers, rows, HEAD_DIM), jnp.bfloat16),
            jax.ShapeDtypeStruct((layers, rows, LANES), jnp.float32),
            jax.ShapeDtypeStruct((layers, rows, LANES), jnp.float32),
            jax.ShapeDtypeStruct((layers, rows, HEAD_DIM), jnp.float32),
        ],
        grid_spec=pltpu.PrefetchScalarGridSpec(
            num_scalar_prefetch=1,
            grid=(layers,),
            in_specs=[
                pl.BlockSpec((None, 1, query_width), lambda layer, _: (layer, 0, 0)),
                pl.BlockSpec((None, None, text_dev, width), lambda layer, _: (layer, 0, 0, 0)),
            ],
            out_specs=[part] * 4,
        ),
        cost_estimate=pl.CostEstimate(
            flops=8 * layers * SUBLANES * LANES * text_dev * width,
            bytes_accessed=2 * layers * text_dev * width,
            transcendentals=layers * rows * text_dev,
        ),
        compiler_params=pltpu.CompilerParams(vmem_limit_bytes=VMEM_LIMIT),
        name="text_part",
    )(text_len, query, text_cache)


def image_layer(scale, layer, chunks, q_ref, top, total, summed):
    layers = q_ref.shape[0]
    blocks = 2 * KV_HEADS
    per = (chunks[0].shape[0] - SUBLANES) // layers // blocks

    def column(c):
        span = pl.ds((layer * blocks + c) * per, per)
        return jnp.concatenate([chunk[span, :] for chunk in chunks], axis=0)

    keys = [column(g) for g in range(KV_HEADS)]
    values = [column(KV_HEADS + g) for g in range(KV_HEADS)]
    new_top, new_total, new_summed = attend(q_ref[layer], keys, values, None, scale)
    both = jnp.maximum(top, new_top)
    old_factor = jnp.exp(top - both)
    new_factor = jnp.exp(new_top - both)
    total = old_factor * total + new_factor * new_total
    summed = old_factor * summed + new_factor * new_summed
    return both, total, summed


def early_kernel(scale, groups, q_ref, top_in, total_in, sum_in, *refs):
    chunks, (top_ref, total_ref, sum_ref) = refs[:groups], refs[groups:]
    rows = q_ref.shape[1]
    for layer in range(q_ref.shape[0]):
        top, total, summed = image_layer(
            scale,
            layer,
            chunks,
            q_ref,
            top_in[layer][:, :1],
            total_in[layer][:, :1],
            sum_in[layer],
        )
        top_ref[layer] = jnp.broadcast_to(top, (rows, LANES))
        total_ref[layer] = jnp.broadcast_to(total, (rows, LANES))
        sum_ref[layer] = summed


def early_part(parts, chunks, scale):
    groups = len(chunks)
    vmem = pl.BlockSpec(memory_space=pltpu.VMEM)
    rows = chunks[0].shape[0]
    made = pl.pallas_call(
        functools.partial(early_kernel, scale, groups),
        out_shape=[jax.ShapeDtypeStruct(part.shape, part.dtype) for part in parts[1:]],
        in_specs=[vmem] * (4 + groups),
        out_specs=[vmem] * 3,
        cost_estimate=pl.CostEstimate(
            flops=8 * SUBLANES * rows * LANES * groups,
            bytes_accessed=2 * rows * LANES * groups,
            transcendentals=SUBLANES * rows * groups,
        ),
        compiler_params=pltpu.CompilerParams(vmem_limit_bytes=VMEM_LIMIT),
        name="early_part",
    )(*parts, *chunks)
    return [parts[0], *made]


def late_kernel(scale, groups, q_ref, top_in, total_in, sum_in, *refs):
    chunks, outs, packed = refs[:groups], refs[groups:-1], refs[-1]
    layers = q_ref.shape[0]
    lane = lax.broadcasted_iota(jnp.int32, (SUBLANES, LANES), 1)
    for layer in range(layers):
        top, total, summed = image_layer(
            scale,
            layer,
            chunks,
            q_ref,
            top_in[layer][:, :1],
            total_in[layer][:, :1],
            sum_in[layer],
        )
        for g in range(KV_HEADS):
            span = slice(g * SUBLANES, (g + 1) * SUBLANES)
            packed[g, pl.ds(layer * SUBLANES, SUBLANES), :] = summed[span]
            packed[g, pl.ds((layers + layer) * SUBLANES, SUBLANES), :] = jnp.where(
                lane == 0, top[span], total[span]
            )
    me = lax.axis_index("seq")
    for k in range(KV_HEADS):
        outs[k][...] = packed[me ^ k]


def late_part(parts, chunks, scale):
    layers = parts[0].shape[0]
    groups = len(chunks)
    shape = (2 * layers * SUBLANES, LANES)
    vmem = pl.BlockSpec(memory_space=pltpu.VMEM)
    rows = chunks[0].shape[0]
    return pl.pallas_call(
        functools.partial(late_kernel, scale, groups),
        out_shape=[jax.ShapeDtypeStruct(shape, jnp.float32)] * KV_HEADS,
        in_specs=[vmem] * (4 + groups),
        out_specs=[vmem] * KV_HEADS,
        scratch_shapes=[pltpu.VMEM((KV_HEADS,) + shape, jnp.float32)],
        cost_estimate=pl.CostEstimate(
            flops=8 * SUBLANES * rows * LANES * groups,
            bytes_accessed=2 * rows * LANES * groups,
            transcendentals=SUBLANES * rows * groups,
        ),
        compiler_params=pltpu.CompilerParams(vmem_limit_bytes=VMEM_LIMIT),
        name="late_part",
    )(*parts, *chunks)


def place_kernel(groups, *refs):
    chunks, (out_hbm, out_ref, sems) = refs[:groups], refs[groups:]
    layers, band, width = out_ref.shape
    blocks = width // LANES
    per = band // groups
    stores = [
        pltpu.make_async_copy(out_ref.at[layer], out_hbm.at[layer], sems.at[layer])
        for layer in range(layers)
    ]
    base = layers * blocks * per
    lane = lax.broadcasted_iota(jnp.int32, (SUBLANES, LANES), 1)
    tiles = []
    for tile in range(band // LANES):
        row = jnp.zeros((SUBLANES, LANES), jnp.float32)
        for k in range(groups):
            if k * per // LANES == tile:
                extra = chunks[k][pl.ds(base, SUBLANES), :].astype(jnp.float32)
                inside = (lane >= k * per % LANES) & (lane < k * per % LANES + per)
                row = jnp.where(inside, extra, row)
        tiles.append(row)
    digits = jnp.concatenate(tiles, axis=1).astype(jnp.int32)
    places = digits[0:1] + digits[1:2] * LANES
    down = lax.broadcasted_iota(jnp.int32, (band, band), 0)
    choose = jnp.where(down == places, 1.0, 0.0).astype(jnp.bfloat16)
    for layer in range(layers):
        for c in range(blocks):
            span = pl.ds((layer * blocks + c) * per, per)
            column = jnp.concatenate([chunk[span, :] for chunk in chunks], axis=0)
            out_ref[layer, :, c * LANES : (c + 1) * LANES] = jnp.dot(
                choose, column, preferred_element_type=jnp.float32
            ).astype(jnp.bfloat16)
        stores[layer].start()
    for store in stores:
        store.wait()


def place_rows(chunks, layers, band, width):
    groups = len(chunks)
    vmem = pl.BlockSpec(memory_space=pltpu.VMEM)
    return pl.pallas_call(
        functools.partial(place_kernel, groups),
        out_shape=jax.ShapeDtypeStruct((layers, band, width), jnp.bfloat16),
        in_specs=[vmem] * groups,
        out_specs=pl.BlockSpec(memory_space=pltpu.HBM),
        scratch_shapes=[
            pltpu.VMEM((layers, band, width), jnp.bfloat16),
            pltpu.SemaphoreType.DMA((layers,)),
        ],
        cost_estimate=pl.CostEstimate(
            flops=2 * layers * band * band * width,
            bytes_accessed=4 * layers * band * width,
            transcendentals=0,
        ),
        compiler_params=pltpu.CompilerParams(vmem_limit_bytes=VMEM_LIMIT),
        name="place_rows",
    )(*chunks)


def merge_kernel(group, *refs):
    parts, out_ref, lines = refs[:-2], refs[-2], refs[-1]
    half = parts[0].shape[0] // 2
    layers = half // SUBLANES
    tops = [part[pl.ds(half, half), :][:, 0:1] for part in parts]
    totals = [part[pl.ds(half, half), :][:, 1:2] for part in parts]
    top = functools.reduce(jnp.maximum, tops)
    factors = [jnp.exp(t - top) for t in tops]
    total = sum(f * t for f, t in zip(factors, totals))
    summed = sum(f * part[pl.ds(0, half), :] for f, part in zip(factors, parts))
    result = summed / total
    for layer in range(layers):
        for i in range(group):
            row = layer * SUBLANES + i
            lines[pl.ds(layer, 1), i * HEAD_DIM : (i + 1) * HEAD_DIM] = result[row : row + 1]
    out_ref[...] = lines[...].astype(jnp.bfloat16)


def merge(parts, layers, group):
    vmem = pl.BlockSpec(memory_space=pltpu.VMEM)
    return pl.pallas_call(
        functools.partial(merge_kernel, group),
        out_shape=jax.ShapeDtypeStruct((layers, group * HEAD_DIM), jnp.bfloat16),
        in_specs=[vmem] * len(parts),
        out_specs=vmem,
        scratch_shapes=[pltpu.VMEM((layers, group * HEAD_DIM), jnp.float32)],
        compiler_params=pltpu.CompilerParams(vmem_limit_bytes=VMEM_LIMIT),
        name="merge",
    )(*parts)


def exchange_pairs(patch_count, req_count, step, turn):
    pairs = []
    for patch in range(patch_count):
        for req in range(req_count):
            target = next(p for p in range(patch_count) if step_of(patch, p, patch_count) == step)
            pairs.append(
                (patch * req_count + req, target * req_count + (req + turn) % req_count)
            )
    return pairs


def fast_body(query, text_cache, text_len, image_rows, patch_map, image_places):
    layers = query.shape[0]
    patch_count = lax.axis_size("patch")
    req_count = lax.axis_size("req")
    band, width = image_rows.shape[1:]
    group = HEADS // KV_HEADS
    scale = 1.0 / math.sqrt(HEAD_DIM)
    grouped = group_rows(patch_map, image_places, image_rows, patch_count, req_count)
    slots = [[step * req_count + turn for turn in range(req_count)] for step in range(patch_count)]
    last = patch_count // 2 - 1
    late = slots[last]
    early = [k for step in range(patch_count - 1) if step != last for k in slots[step]]
    own, core = slots[-1][0], slots[-1][1:]
    chunks = list(grouped)
    for k in early + late + core:
        pairs = exchange_pairs(patch_count, req_count, k // req_count, k % req_count)
        chunks[k] = lax.ppermute(grouped[k], ("patch", "req"), pairs)
    parts = text_part(query, text_cache, text_len, scale)
    parts = early_part(parts, [chunks[k] for k in early + core + [own]], scale)
    packed = late_part(parts, [chunks[k] for k in late], scale)
    gathered = [packed[0]]
    for k in range(1, KV_HEADS):
        gathered.append(lax.ppermute(packed[k], "seq", [(s, s ^ k) for s in range(KV_HEADS)]))
    image_cache = place_rows(chunks, layers, band, width)
    attended = merge(gathered, layers, group)
    return attended[:, None, :], image_cache[:, None]


def plain_body(query, text_cache, text_len, image_rows, patch_map, image_places):
    layers, req_dev, query_width = query.shape
    text_dev = text_cache.shape[2]
    full_width = text_cache.shape[3]
    kv_width = full_width // 2
    head_dim = HEAD_DIM
    kv_heads = KV_HEADS
    heads = HEADS
    group = heads // kv_heads
    src_rows = image_rows.shape[1]
    patch_count = lax.axis_size("patch")
    req_count = lax.axis_size("req")
    seq_count = lax.axis_size("seq")
    seq_index = lax.axis_index("seq")
    per_source = src_rows // (patch_count * req_count * req_dev)
    band_size = per_source * patch_count * req_count
    scale = 1.0 / math.sqrt(head_dim)
    order = jnp.argsort(patch_map, stable=True)
    grouped = jnp.take(image_rows, order, axis=1)
    grouped_places = jnp.take(image_places, order)
    sending = grouped.reshape(layers, patch_count * req_count, req_dev, per_source, full_width)
    arrived = lax.all_to_all(sending, ("patch", "req"), split_axis=1, concat_axis=3, tiled=True)
    place_send = grouped_places.reshape(patch_count * req_count, req_dev, per_source)
    arrived_places = lax.all_to_all(
        place_send, ("patch", "req"), split_axis=0, concat_axis=2, tiled=True
    )
    image_block = arrived.reshape(layers, req_dev, band_size, full_width)
    local_places = arrived_places.reshape(req_dev, band_size) - seq_index * band_size
    inverse = jnp.argsort(local_places, axis=1)
    image_cache = jnp.take_along_axis(image_block, inverse[None, :, :, None], axis=2)
    queries = query.reshape(layers, req_dev, kv_heads, group, head_dim)
    text_keys = text_cache[..., :kv_width].reshape(layers, req_dev, text_dev, kv_heads, head_dim)
    text_values = text_cache[..., kv_width:].reshape(layers, req_dev, text_dev, kv_heads, head_dim)
    image_keys = image_block[..., :kv_width].reshape(layers, req_dev, band_size, kv_heads, head_dim)
    image_values = image_block[..., kv_width:].reshape(
        layers, req_dev, band_size, kv_heads, head_dim
    )
    positions = seq_index * text_dev + jnp.arange(text_dev, dtype=jnp.int32)
    used = positions[None, :] < text_len[:, None]
    text_raw = (
        jnp.einsum("lrkgd,lrtkd->lrkgt", queries, text_keys, preferred_element_type=jnp.float32)
        * scale
    )
    text_scores = jnp.where(used[None, :, None, None, :], text_raw, -jnp.inf)
    image_scores = (
        jnp.einsum("lrkgd,lrtkd->lrkgt", queries, image_keys, preferred_element_type=jnp.float32)
        * scale
    )
    local_top = jnp.maximum(jnp.max(text_scores, axis=-1), jnp.max(image_scores, axis=-1))
    text_weights = jnp.exp(text_scores - local_top[..., None])
    image_weights = jnp.exp(image_scores - local_top[..., None])
    local_total = jnp.sum(text_weights, axis=-1) + jnp.sum(image_weights, axis=-1)
    text_rounded = text_weights.astype(jnp.bfloat16)
    image_rounded = image_weights.astype(jnp.bfloat16)
    local_values = jnp.einsum(
        "lrkgt,lrtkd->lrkgd", image_rounded, image_values, preferred_element_type=jnp.float32
    )
    local_values = local_values + jnp.einsum(
        "lrkgt,lrtkd->lrkgd", text_rounded, text_values, preferred_element_type=jnp.float32
    )
    width_dev = query_width // seq_count
    top = lax.pmax(local_top, "seq")
    factor = jnp.exp(local_top - top)
    scaled_total = factor * local_total
    scaled_values = factor[..., None] * local_values
    total_sum, value_sum = lax.psum((scaled_total, scaled_values), "seq")
    result = (value_sum / total_sum[..., None]).reshape(layers, req_dev, query_width)
    attended = lax.dynamic_slice_in_dim(result, seq_index * width_dev, width_dev, 2).astype(
        jnp.bfloat16
    )
    return (attended, image_cache)


def body(query, text_cache, text_len, image_rows, patch_map, image_places):
    groups = lax.axis_size("patch") * lax.axis_size("req")
    band = image_rows.shape[1]
    per = band // groups
    fast = (
        query.shape[1] == 1
        and lax.axis_size("patch") >= 2
        and groups <= 16
        and band == per * groups
        and band % LANES == 0
        and per % 16 == 0
        and LANES % per == 0
        and lax.axis_size("seq") == KV_HEADS
        and HEADS // KV_HEADS <= SUBLANES
    )
    chosen = fast_body if fast else plain_body
    return chosen(query, text_cache, text_len, image_rows, patch_map, image_places)


def solution(mesh):
    return jax.shard_map(
        body,
        mesh=mesh,
        in_specs=(
            P(None, ("patch", "req"), None),
            P(None, ("patch", "req"), "seq", None),
            P(("patch", "req")),
            P(None, ("patch", "seq", "req"), None),
            P(("patch", "seq", "req")),
            P(("patch", "seq", "req")),
        ),
        out_specs=(P(None, ("patch", "req"), "seq"), P(None, ("patch", "req"), "seq", None)),
        check_vma=False,
    )
```

```python
import functools
import math

import jax
import jax.numpy as jnp
from jax import lax
from jax.experimental import pallas as pl
from jax.experimental.pallas import tpu as pltpu
from jax.sharding import PartitionSpec as P

HEADS = 28
KV_HEADS = 4
HEAD_DIM = 128
LANES = 128
SUBLANES = 8
MASKED = -1e30

VMEM_LIMIT = 16 * 1024 * 1024
WIDE_VMEM_LIMIT = 62 * 1024 * 1024


def gray(index):
    return index ^ (index >> 1)


def step_of(source, target, count):
    if count & (count - 1) == 0:
        return (gray(target) - gray(source) + count - 1) & (count - 1)
    return (target - source + count - 1) % count


def slot_choice(patch_count, req_count, owner, place):
    src_rows = owner.shape[1]
    per = src_rows // (patch_count * req_count)
    me = lax.axis_index("patch")
    mine = lax.axis_index("req")
    shape = (src_rows, src_rows)
    down = lax.broadcasted_iota(jnp.int32, shape, 0)
    across = lax.broadcasted_iota(jnp.int32, shape, 1)
    owner_row = jnp.broadcast_to(owner, shape)
    owner_col = jnp.sum(
        jnp.where(down == across, owner_row.astype(jnp.float32), 0.0), axis=1, keepdims=True
    ).astype(jnp.int32)
    ahead = (owner_row == owner_col) & (down < across)
    rank = jnp.sum(jnp.where(ahead, 1.0, 0.0), axis=0, keepdims=True).astype(jnp.int32)
    step = step_of(me, owner // req_count, patch_count)
    turn = (owner % req_count - mine + req_count) % req_count
    slot = (step * req_count + turn) * per + rank
    choose = jnp.where(down == slot, 1.0, 0.0).astype(jnp.bfloat16)
    local = place - lax.axis_index("seq") * src_rows
    line = lax.broadcasted_iota(jnp.int32, (SUBLANES, src_rows), 0)
    digits = jnp.where(line == 0, local & (LANES - 1), jnp.where(line == 1, local // LANES, 0))
    places = lax.dot_general(
        digits.astype(jnp.float32).astype(jnp.bfloat16),
        choose,
        (((1,), (1,)), ((), ())),
        preferred_element_type=jnp.float32,
    ).astype(jnp.bfloat16)
    return choose, places


def pack_slots(first, per, choose, places, layer_rows, layers, outs):
    for k, out in enumerate(outs):
        tile = (first + k) * per // LANES
        out[pl.ds(out.shape[0] - SUBLANES, SUBLANES), :] = places[
            :, tile * LANES : (tile + 1) * LANES
        ]
    taken = choose[first * per : (first + len(outs)) * per]
    for layer in range(layers):
        rows = layer_rows(layer)
        blocks = rows.shape[1] // LANES
        moved = jnp.dot(taken, rows, preferred_element_type=jnp.float32).astype(jnp.bfloat16)
        for k, out in enumerate(outs):
            for c in range(blocks):
                out[pl.ds((layer * blocks + c) * per, per), :] = moved[
                    k * per : (k + 1) * per, c * LANES : (c + 1) * LANES
                ]


def first_kernel(patch_count, req_count, map_hbm, place_hbm, rows_hbm, *refs):
    choose_ref, places_ref, *outs = refs[:-5]
    owner_ref, place_ref, rows_ref, small_sem, rows_sem = refs[-5:]
    layers, src_rows, _ = rows_hbm.shape
    small = [
        pltpu.make_async_copy(map_hbm, owner_ref, small_sem.at[0]),
        pltpu.make_async_copy(place_hbm, place_ref, small_sem.at[1]),
    ]
    loads = [
        pltpu.make_async_copy(rows_hbm.at[layer], rows_ref.at[layer], rows_sem.at[layer])
        for layer in range(layers)
    ]
    for copy in small + loads:
        copy.start()
    for copy in small:
        copy.wait()
    choose, places = slot_choice(patch_count, req_count, owner_ref[...], place_ref[...])
    choose_ref[...] = choose
    places_ref[...] = places

    def layer_rows(layer):
        loads[layer].wait()
        return rows_ref[layer]

    per = src_rows // (patch_count * req_count)
    pack_slots(0, per, choose, places, layer_rows, layers, outs)


def rest_kernel(first, per, choose_ref, places_ref, rows_ref, *outs):
    pack_slots(
        first,
        per,
        choose_ref[...],
        places_ref[...],
        lambda layer: rows_ref[layer],
        rows_ref.shape[0],
        outs,
    )


def group_rows(patch_map, image_places, image_rows, patch_count, req_count):
    layers, src_rows, width = image_rows.shape
    groups = patch_count * req_count
    per = src_rows // groups
    chunk = jax.ShapeDtypeStruct((layers * per * width // LANES + SUBLANES, LANES), jnp.bfloat16)
    hbm = pl.BlockSpec(memory_space=pltpu.HBM)
    vmem = pl.BlockSpec(memory_space=pltpu.VMEM)

    def cost(count):
        return pl.CostEstimate(
            flops=2 * layers * src_rows * per * count * width,
            bytes_accessed=2 * layers * (src_rows + per * count) * width,
            transcendentals=0,
        )

    choose, places, *first = pl.pallas_call(
        functools.partial(first_kernel, patch_count, req_count),
        out_shape=[
            jax.ShapeDtypeStruct((src_rows, src_rows), jnp.bfloat16),
            jax.ShapeDtypeStruct((SUBLANES, src_rows), jnp.bfloat16),
        ]
        + [chunk] * req_count,
        in_specs=[hbm] * 3,
        out_specs=[vmem] * (2 + req_count),
        scratch_shapes=[
            pltpu.VMEM((1, src_rows), jnp.int32),
            pltpu.VMEM((1, src_rows), jnp.int32),
            pltpu.VMEM(image_rows.shape, jnp.bfloat16),
            pltpu.SemaphoreType.DMA((2,)),
            pltpu.SemaphoreType.DMA((layers,)),
        ],
        cost_estimate=cost(req_count),
        compiler_params=pltpu.CompilerParams(vmem_limit_bytes=WIDE_VMEM_LIMIT),
        name="group_first",
    )(patch_map.reshape(1, src_rows), image_places.reshape(1, src_rows), image_rows)
    rest = pl.pallas_call(
        functools.partial(rest_kernel, req_count, per),
        out_shape=[chunk] * (groups - req_count),
        in_specs=[vmem] * 3,
        out_specs=[vmem] * (groups - req_count),
        cost_estimate=cost(groups - req_count),
        compiler_params=pltpu.CompilerParams(vmem_limit_bytes=VMEM_LIMIT),
        name="group_rest",
    )(choose, places, image_rows)
    return [*first, *rest]


def heads_of(line, group):
    row = lax.broadcasted_iota(jnp.int32, (SUBLANES, HEAD_DIM), 0)
    tiles = []
    for g in range(KV_HEADS):
        tile = jnp.zeros((SUBLANES, HEAD_DIM), jnp.float32)
        for i in range(group):
            h = g * group + i
            tile = jnp.where(row == i, line[:, h * HEAD_DIM : (h + 1) * HEAD_DIM], tile)
        tiles.append(tile)
    return jnp.concatenate(tiles, axis=0).astype(jnp.bfloat16)


def attend(queries, keys, values, used, scale):
    scores = jnp.concatenate(
        [
            lax.dot_general(
                queries[g * SUBLANES : (g + 1) * SUBLANES],
                keys[g],
                (((1,), (1,)), ((), ())),
                preferred_element_type=jnp.float32,
            )
            for g in range(KV_HEADS)
        ],
        axis=0,
    )
    scores = scores * scale
    if used is not None:
        scores = jnp.where(used, scores, MASKED)
    top = jnp.max(scores, axis=1, keepdims=True)
    weights = jnp.exp(scores - top)
    if used is not None:
        weights = jnp.where(used, weights, 0.0)
    total = jnp.sum(weights, axis=1, keepdims=True)
    rounded = weights.astype(jnp.bfloat16)
    summed = jnp.concatenate(
        [
            jnp.dot(
                rounded[g * SUBLANES : (g + 1) * SUBLANES],
                values[g],
                preferred_element_type=jnp.float32,
            )
            for g in range(KV_HEADS)
        ],
        axis=0,
    )
    return top, total, summed


def text_kernel(scale, len_ref, query_ref, text_ref, q_ref, top_ref, total_ref, sum_ref):
    text_dev, width = text_ref.shape
    group = query_ref.shape[1] // HEAD_DIM // KV_HEADS
    queries = heads_of(query_ref[...].astype(jnp.float32), group)
    q_ref[...] = queries
    rows = KV_HEADS * SUBLANES
    positions = lax.axis_index("seq") * text_dev + lax.broadcasted_iota(
        jnp.int32, (rows, text_dev), 1
    )
    keys = [text_ref[:, g * HEAD_DIM : (g + 1) * HEAD_DIM] for g in range(KV_HEADS)]
    values = [
        text_ref[:, width // 2 + g * HEAD_DIM : width // 2 + (g + 1) * HEAD_DIM]
        for g in range(KV_HEADS)
    ]
    top, total, summed = attend(queries, keys, values, positions < len_ref[0], scale)
    top_ref[...] = jnp.broadcast_to(top, (rows, LANES))
    total_ref[...] = jnp.broadcast_to(total, (rows, LANES))
    sum_ref[...] = summed


def text_part(query, text_cache, text_len, scale):
    layers, _, query_width = query.shape
    text_dev, width = text_cache.shape[2:]
    rows = KV_HEADS * SUBLANES
    part = pl.BlockSpec((None, rows, LANES), lambda layer, _: (layer, 0, 0))
    return pl.pallas_call(
        functools.partial(text_kernel, scale),
        out_shape=[
            jax.ShapeDtypeStruct((layers, rows, HEAD_DIM), jnp.bfloat16),
            jax.ShapeDtypeStruct((layers, rows, LANES), jnp.float32),
            jax.ShapeDtypeStruct((layers, rows, LANES), jnp.float32),
            jax.ShapeDtypeStruct((layers, rows, HEAD_DIM), jnp.float32),
        ],
        grid_spec=pltpu.PrefetchScalarGridSpec(
            num_scalar_prefetch=1,
            grid=(layers,),
            in_specs=[
                pl.BlockSpec((None, 1, query_width), lambda layer, _: (layer, 0, 0)),
                pl.BlockSpec((None, None, text_dev, width), lambda layer, _: (layer, 0, 0, 0)),
            ],
            out_specs=[part] * 4,
        ),
        cost_estimate=pl.CostEstimate(
            flops=8 * layers * SUBLANES * LANES * text_dev * width,
            bytes_accessed=2 * layers * text_dev * width,
            transcendentals=layers * rows * text_dev,
        ),
        compiler_params=pltpu.CompilerParams(vmem_limit_bytes=VMEM_LIMIT),
        name="text_part",
    )(text_len, query, text_cache)


def image_layer(scale, layer, chunks, q_ref, top, total, summed):
    layers = q_ref.shape[0]
    blocks = 2 * KV_HEADS
    per = (chunks[0].shape[0] - SUBLANES) // layers // blocks

    def column(c):
        span = pl.ds((layer * blocks + c) * per, per)
        return jnp.concatenate([chunk[span, :] for chunk in chunks], axis=0)

    keys = [column(g) for g in range(KV_HEADS)]
    values = [column(KV_HEADS + g) for g in range(KV_HEADS)]
    new_top, new_total, new_summed = attend(q_ref[layer], keys, values, None, scale)
    both = jnp.maximum(top, new_top)
    old_factor = jnp.exp(top - both)
    new_factor = jnp.exp(new_top - both)
    total = old_factor * total + new_factor * new_total
    summed = old_factor * summed + new_factor * new_summed
    return both, total, summed


def pack_part(top, total, summed):
    row = lax.broadcasted_iota(jnp.int32, (SUBLANES, LANES), 0)
    lane = lax.broadcasted_iota(jnp.int32, (SUBLANES, LANES), 1)
    stats = jnp.where(lane == row, top, jnp.where(lane == row + LANES // 2, total, 0.0))
    stats = jnp.sum(stats, axis=0, keepdims=True)
    return jnp.where(row == SUBLANES - 1, stats, summed)


def unpack_part(tile):
    row = lax.broadcasted_iota(jnp.int32, (SUBLANES, LANES), 0)
    lane = lax.broadcasted_iota(jnp.int32, (SUBLANES, LANES), 1)
    stats = jnp.broadcast_to(tile[SUBLANES - 1 :, :], (SUBLANES, LANES))
    top = jnp.sum(jnp.where(lane == row, stats, 0.0), axis=1, keepdims=True)
    total = jnp.sum(jnp.where(lane == row + LANES // 2, stats, 0.0), axis=1, keepdims=True)
    return top, total, tile


def merge_tiles(tiles):
    parts = [unpack_part(tile) for tile in tiles]
    top = functools.reduce(jnp.maximum, [part[0] for part in parts])
    factors = [jnp.exp(part[0] - top) for part in parts]
    total = sum(factor * part[1] for factor, part in zip(factors, parts))
    summed = sum(factor * part[2] for factor, part in zip(factors, parts))
    return top, total, summed


def here_kernel(scale, groups, q_ref, top_in, total_in, sum_in, *refs):
    chunks, outs, packed = refs[:groups], refs[groups:-1], refs[-1]
    for layer in range(q_ref.shape[0]):
        top, total, summed = image_layer(
            scale,
            layer,
            chunks,
            q_ref,
            top_in[layer][:, :1],
            total_in[layer][:, :1],
            sum_in[layer],
        )
        for g in range(KV_HEADS):
            span = slice(g * SUBLANES, (g + 1) * SUBLANES)
            packed[g, pl.ds(layer * SUBLANES, SUBLANES), :] = pack_part(
                top[span], total[span], summed[span]
            )
    me = lax.axis_index("seq")
    for k in range(KV_HEADS):
        outs[k][...] = packed[me ^ k]


def far_kernel(scale, count, *refs):
    queries, chunks = refs[:count], refs[count : 2 * count]
    outs, packed = refs[2 * count : -1], refs[-1]
    layers = queries[0].shape[0]
    blocks = 2 * KV_HEADS
    group = queries[0].shape[1] // HEAD_DIM // KV_HEADS
    for n in range(count):
        chunk = chunks[n]
        per = (chunk.shape[0] - SUBLANES) // layers // blocks
        for layer in range(layers):
            columns = [
                chunk[pl.ds((layer * blocks + c) * per, per), :] for c in range(blocks)
            ]
            line = queries[n][pl.ds(layer, 1), :].astype(jnp.float32)
            top, total, summed = attend(
                heads_of(line, group), columns[:KV_HEADS], columns[KV_HEADS:], None, scale
            )
            for g in range(KV_HEADS):
                span = slice(g * SUBLANES, (g + 1) * SUBLANES)
                packed[g, pl.ds((n * layers + layer) * SUBLANES, SUBLANES), :] = pack_part(
                    top[span], total[span], summed[span]
                )
    me = lax.axis_index("seq")
    for k in range(KV_HEADS):
        outs[k][...] = packed[me ^ k]


def seq_parts(kernel, name, operands, part_rows, chunk_rows, groups):
    shape = (part_rows, LANES)
    vmem = pl.BlockSpec(memory_space=pltpu.VMEM)
    return pl.pallas_call(
        kernel,
        out_shape=[jax.ShapeDtypeStruct(shape, jnp.float32)] * KV_HEADS,
        in_specs=[vmem] * len(operands),
        out_specs=[vmem] * KV_HEADS,
        scratch_shapes=[pltpu.VMEM((KV_HEADS,) + shape, jnp.float32)],
        cost_estimate=pl.CostEstimate(
            flops=8 * SUBLANES * chunk_rows * LANES * groups,
            bytes_accessed=2 * chunk_rows * LANES * groups,
            transcendentals=SUBLANES * chunk_rows * groups,
        ),
        compiler_params=pltpu.CompilerParams(vmem_limit_bytes=VMEM_LIMIT),
        name=name,
    )(*operands)


def seq_exchange(outs):
    arrived = [
        lax.ppermute(out, "seq", [(s, s ^ k) for s in range(KV_HEADS)])
        for k, out in enumerate(outs)
        if k
    ]
    return [outs[0], *arrived]


def merge_far_kernel(count, *refs):
    parts, outs = refs[:-count], refs[-count:]
    rows = parts[0].shape[0] // count
    for n, out in enumerate(outs):
        for at in range(0, rows, SUBLANES):
            tiles = [part[pl.ds(n * rows + at, SUBLANES), :] for part in parts]
            out[pl.ds(at, SUBLANES), :] = pack_part(*merge_tiles(tiles))


def merge_far(parts, count):
    rows = parts[0].shape[0] // count
    vmem = pl.BlockSpec(memory_space=pltpu.VMEM)
    return pl.pallas_call(
        functools.partial(merge_far_kernel, count),
        out_shape=[jax.ShapeDtypeStruct((rows, LANES), jnp.float32)] * count,
        in_specs=[vmem] * len(parts),
        out_specs=[vmem] * count,
        compiler_params=pltpu.CompilerParams(vmem_limit_bytes=VMEM_LIMIT),
        name="merge_far",
    )(*parts)


def place_kernel(groups, *refs):
    chunks, (out_hbm, out_ref, sems) = refs[:groups], refs[groups:]
    layers, band, width = out_ref.shape
    blocks = width // LANES
    per = band // groups
    stores = [
        pltpu.make_async_copy(out_ref.at[layer], out_hbm.at[layer], sems.at[layer])
        for layer in range(layers)
    ]
    base = layers * blocks * per
    lane = lax.broadcasted_iota(jnp.int32, (SUBLANES, LANES), 1)
    tiles = []
    for tile in range(band // LANES):
        row = jnp.zeros((SUBLANES, LANES), jnp.float32)
        for k in range(groups):
            if k * per // LANES == tile:
                extra = chunks[k][pl.ds(base, SUBLANES), :].astype(jnp.float32)
                inside = (lane >= k * per % LANES) & (lane < k * per % LANES + per)
                row = jnp.where(inside, extra, row)
        tiles.append(row)
    digits = jnp.concatenate(tiles, axis=1).astype(jnp.int32)
    places = digits[0:1] + digits[1:2] * LANES
    down = lax.broadcasted_iota(jnp.int32, (band, band), 0)
    choose = jnp.where(down == places, 1.0, 0.0).astype(jnp.bfloat16)
    for layer in range(layers):
        for c in range(blocks):
            span = pl.ds((layer * blocks + c) * per, per)
            column = jnp.concatenate([chunk[span, :] for chunk in chunks], axis=0)
            out_ref[layer, :, c * LANES : (c + 1) * LANES] = jnp.dot(
                choose, column, preferred_element_type=jnp.float32
            ).astype(jnp.bfloat16)
        stores[layer].start()
    for store in stores:
        store.wait()


def place_rows(chunks, layers, band, width):
    groups = len(chunks)
    vmem = pl.BlockSpec(memory_space=pltpu.VMEM)
    return pl.pallas_call(
        functools.partial(place_kernel, groups),
        out_shape=jax.ShapeDtypeStruct((layers, band, width), jnp.bfloat16),
        in_specs=[vmem] * groups,
        out_specs=pl.BlockSpec(memory_space=pltpu.HBM),
        scratch_shapes=[
            pltpu.VMEM((layers, band, width), jnp.bfloat16),
            pltpu.SemaphoreType.DMA((layers,)),
        ],
        cost_estimate=pl.CostEstimate(
            flops=2 * layers * band * band * width,
            bytes_accessed=4 * layers * band * width,
            transcendentals=0,
        ),
        compiler_params=pltpu.CompilerParams(vmem_limit_bytes=VMEM_LIMIT),
        name="place_rows",
    )(*chunks)


def merge_kernel(group, *refs):
    parts, out_ref, lines = refs[:-2], refs[-2], refs[-1]
    for layer in range(out_ref.shape[0]):
        tiles = [part[pl.ds(layer * SUBLANES, SUBLANES), :] for part in parts]
        _, total, summed = merge_tiles(tiles)
        result = summed / total
        for i in range(group):
            lines[pl.ds(layer, 1), i * HEAD_DIM : (i + 1) * HEAD_DIM] = result[i : i + 1]
    out_ref[...] = lines[...].astype(jnp.bfloat16)


def merge(parts, layers, group):
    vmem = pl.BlockSpec(memory_space=pltpu.VMEM)
    return pl.pallas_call(
        functools.partial(merge_kernel, group),
        out_shape=jax.ShapeDtypeStruct((layers, group * HEAD_DIM), jnp.bfloat16),
        in_specs=[vmem] * len(parts),
        out_specs=vmem,
        scratch_shapes=[pltpu.VMEM((layers, group * HEAD_DIM), jnp.float32)],
        compiler_params=pltpu.CompilerParams(vmem_limit_bytes=VMEM_LIMIT),
        name="merge",
    )(*parts)


def exchange_pairs(patch_count, req_count, step, turn):
    pairs = []
    for patch in range(patch_count):
        for req in range(req_count):
            target = next(p for p in range(patch_count) if step_of(patch, p, patch_count) == step)
            pairs.append(
                (patch * req_count + req, target * req_count + (req + turn) % req_count)
            )
    return pairs


def fast_body(query, text_cache, text_len, image_rows, patch_map, image_places):
    layers = query.shape[0]
    patch_count = lax.axis_size("patch")
    req_count = lax.axis_size("req")
    band, width = image_rows.shape[1:]
    group = HEADS // KV_HEADS
    scale = 1.0 / math.sqrt(HEAD_DIM)
    slots = [[step * req_count + turn for turn in range(req_count)] for step in range(patch_count)]
    last = patch_count // 2 - 1
    late = slots[last]
    early = [k for step in range(patch_count - 1) if step != last for k in slots[step]]
    own, core = slots[-1][0], slots[-1][1:]
    pairs = [
        exchange_pairs(patch_count, req_count, k // req_count, k % req_count)
        for k in range(patch_count * req_count)
    ]
    axes = ("patch", "req")
    flat_query = query[:, 0]
    far_queries = [
        lax.ppermute(flat_query, axes, [(target, source) for source, target in pairs[k]])
        for k in late
    ]
    grouped = group_rows(patch_map, image_places, image_rows, patch_count, req_count)
    chunks = list(grouped)
    for k in early + late + core:
        chunks[k] = lax.ppermute(grouped[k], axes, pairs[k])
    chunk_rows = grouped[0].shape[0]
    part_rows = layers * SUBLANES
    far = seq_parts(
        functools.partial(far_kernel, scale, len(late)),
        "far_part",
        [*far_queries, *(grouped[k] for k in late)],
        len(late) * part_rows,
        chunk_rows,
        len(late),
    )
    far = merge_far(seq_exchange(far), len(late))
    far = [lax.ppermute(part, axes, pairs[k]) for part, k in zip(far, late)]
    text = text_part(query, text_cache, text_len, scale)
    here = [chunks[k] for k in early + core + [own]]
    parts = seq_parts(
        functools.partial(here_kernel, scale, len(here)),
        "here_part",
        [*text, *here],
        part_rows,
        chunk_rows,
        len(here),
    )
    attended = merge([*seq_exchange(parts), *far], layers, group)
    image_cache = place_rows(chunks, layers, band, width)
    return attended[:, None, :], image_cache[:, None]


def plain_body(query, text_cache, text_len, image_rows, patch_map, image_places):
    layers, req_dev, query_width = query.shape
    text_dev = text_cache.shape[2]
    full_width = text_cache.shape[3]
    kv_width = full_width // 2
    head_dim = HEAD_DIM
    kv_heads = KV_HEADS
    heads = HEADS
    group = heads // kv_heads
    src_rows = image_rows.shape[1]
    patch_count = lax.axis_size("patch")
    req_count = lax.axis_size("req")
    seq_count = lax.axis_size("seq")
    seq_index = lax.axis_index("seq")
    per_source = src_rows // (patch_count * req_count * req_dev)
    band_size = per_source * patch_count * req_count
    scale = 1.0 / math.sqrt(head_dim)
    order = jnp.argsort(patch_map, stable=True)
    grouped = jnp.take(image_rows, order, axis=1)
    grouped_places = jnp.take(image_places, order)
    sending = grouped.reshape(layers, patch_count * req_count, req_dev, per_source, full_width)
    arrived = lax.all_to_all(sending, ("patch", "req"), split_axis=1, concat_axis=3, tiled=True)
    place_send = grouped_places.reshape(patch_count * req_count, req_dev, per_source)
    arrived_places = lax.all_to_all(
        place_send, ("patch", "req"), split_axis=0, concat_axis=2, tiled=True
    )
    image_block = arrived.reshape(layers, req_dev, band_size, full_width)
    local_places = arrived_places.reshape(req_dev, band_size) - seq_index * band_size
    inverse = jnp.argsort(local_places, axis=1)
    image_cache = jnp.take_along_axis(image_block, inverse[None, :, :, None], axis=2)
    queries = query.reshape(layers, req_dev, kv_heads, group, head_dim)
    text_keys = text_cache[..., :kv_width].reshape(layers, req_dev, text_dev, kv_heads, head_dim)
    text_values = text_cache[..., kv_width:].reshape(layers, req_dev, text_dev, kv_heads, head_dim)
    image_keys = image_block[..., :kv_width].reshape(layers, req_dev, band_size, kv_heads, head_dim)
    image_values = image_block[..., kv_width:].reshape(
        layers, req_dev, band_size, kv_heads, head_dim
    )
    positions = seq_index * text_dev + jnp.arange(text_dev, dtype=jnp.int32)
    used = positions[None, :] < text_len[:, None]
    text_raw = (
        jnp.einsum("lrkgd,lrtkd->lrkgt", queries, text_keys, preferred_element_type=jnp.float32)
        * scale
    )
    text_scores = jnp.where(used[None, :, None, None, :], text_raw, -jnp.inf)
    image_scores = (
        jnp.einsum("lrkgd,lrtkd->lrkgt", queries, image_keys, preferred_element_type=jnp.float32)
        * scale
    )
    local_top = jnp.maximum(jnp.max(text_scores, axis=-1), jnp.max(image_scores, axis=-1))
    text_weights = jnp.exp(text_scores - local_top[..., None])
    image_weights = jnp.exp(image_scores - local_top[..., None])
    local_total = jnp.sum(text_weights, axis=-1) + jnp.sum(image_weights, axis=-1)
    text_rounded = text_weights.astype(jnp.bfloat16)
    image_rounded = image_weights.astype(jnp.bfloat16)
    local_values = jnp.einsum(
        "lrkgt,lrtkd->lrkgd", image_rounded, image_values, preferred_element_type=jnp.float32
    )
    local_values = local_values + jnp.einsum(
        "lrkgt,lrtkd->lrkgd", text_rounded, text_values, preferred_element_type=jnp.float32
    )
    width_dev = query_width // seq_count
    top = lax.pmax(local_top, "seq")
    factor = jnp.exp(local_top - top)
    scaled_total = factor * local_total
    scaled_values = factor[..., None] * local_values
    total_sum, value_sum = lax.psum((scaled_total, scaled_values), "seq")
    result = (value_sum / total_sum[..., None]).reshape(layers, req_dev, query_width)
    attended = lax.dynamic_slice_in_dim(result, seq_index * width_dev, width_dev, 2).astype(
        jnp.bfloat16
    )
    return (attended, image_cache)


def body(query, text_cache, text_len, image_rows, patch_map, image_places):
    groups = lax.axis_size("patch") * lax.axis_size("req")
    band = image_rows.shape[1]
    per = band // groups
    fast = (
        query.shape[1] == 1
        and lax.axis_size("patch") >= 2
        and groups <= 16
        and band == per * groups
        and band % LANES == 0
        and per % 16 == 0
        and LANES % per == 0
        and lax.axis_size("seq") == KV_HEADS
        and HEADS // KV_HEADS < SUBLANES
    )
    chosen = fast_body if fast else plain_body
    return chosen(query, text_cache, text_len, image_rows, patch_map, image_places)


def solution(mesh):
    return jax.shard_map(
        body,
        mesh=mesh,
        in_specs=(
            P(None, ("patch", "req"), None),
            P(None, ("patch", "req"), "seq", None),
            P(("patch", "req")),
            P(None, ("patch", "seq", "req"), None),
            P(("patch", "seq", "req")),
            P(("patch", "seq", "req")),
        ),
        out_specs=(P(None, ("patch", "req"), "seq"), P(None, ("patch", "req"), "seq", None)),
        check_vma=False,
    )
```

```python
import functools
import math

import jax
import jax.numpy as jnp
from jax import lax
from jax.experimental import pallas as pl
from jax.experimental.pallas import tpu as pltpu
from jax.sharding import PartitionSpec as P


HEADS = 28
KV_HEADS = 4
HEAD_DIM = 128
LANES = 128
SUBLANES = 8
MASKED = -1e30

MOST_GROUPS = 16
VMEM_LIMIT = 16 * 1024 * 1024
WIDE_VMEM_LIMIT = 62 * 1024 * 1024


def gray(index):
    return index ^ (index >> 1)


def step_of(source, target, count):
    if count & (count - 1) == 0:
        return (gray(target) - gray(source) + count - 1) & (count - 1)
    return (target - source + count - 1) % count


def slot_choice(patch_count, req_count, owner, place):
    src_rows = owner.shape[1]
    per = src_rows // (patch_count * req_count)
    me = lax.axis_index("patch")
    mine = lax.axis_index("req")
    shape = (src_rows, src_rows)
    down = lax.broadcasted_iota(jnp.int32, shape, 0)
    across = lax.broadcasted_iota(jnp.int32, shape, 1)
    owner_row = jnp.broadcast_to(owner, shape)
    owner_col = jnp.sum(
        jnp.where(down == across, owner_row.astype(jnp.float32), 0.0), axis=1, keepdims=True
    ).astype(jnp.int32)
    ahead = (owner_row == owner_col) & (down < across)
    rank = jnp.sum(jnp.where(ahead, 1.0, 0.0), axis=0, keepdims=True).astype(jnp.int32)
    step = step_of(me, owner // req_count, patch_count)
    turn = (owner % req_count - mine + req_count) % req_count
    slot = (step * req_count + turn) * per + rank
    choose = jnp.where(down == slot, 1.0, 0.0).astype(jnp.bfloat16)
    local = place - lax.axis_index("seq") * src_rows
    line = lax.broadcasted_iota(jnp.int32, (SUBLANES, src_rows), 0)
    digits = jnp.where(line == 0, local & (LANES - 1), jnp.where(line == 1, local // LANES, 0))
    places = lax.dot_general(
        digits.astype(jnp.float32).astype(jnp.bfloat16),
        choose,
        (((1,), (1,)), ((), ())),
        preferred_element_type=jnp.float32,
    ).astype(jnp.bfloat16)
    return choose, places


def pack_slots(first, per, choose, places, layer_rows, layers, outs):
    for k, out in enumerate(outs):
        tile = (first + k) * per // LANES
        out[pl.ds(out.shape[0] - SUBLANES, SUBLANES), :] = places[
            :, tile * LANES : (tile + 1) * LANES
        ]
    taken = choose[first * per : (first + len(outs)) * per]
    for layer in range(layers):
        rows = layer_rows(layer)
        blocks = rows.shape[1] // LANES
        moved = jnp.dot(taken, rows, preferred_element_type=jnp.float32).astype(jnp.bfloat16)
        for k, out in enumerate(outs):
            for c in range(blocks):
                out[pl.ds((layer * blocks + c) * per, per), :] = moved[
                    k * per : (k + 1) * per, c * LANES : (c + 1) * LANES
                ]


def first_kernel(patch_count, req_count, map_hbm, place_hbm, rows_hbm, *refs):
    choose_ref, places_ref, *outs = refs[:-5]
    owner_ref, place_ref, rows_ref, small_sem, rows_sem = refs[-5:]
    layers, src_rows, _ = rows_hbm.shape
    small = [
        pltpu.make_async_copy(map_hbm, owner_ref, small_sem.at[0]),
        pltpu.make_async_copy(place_hbm, place_ref, small_sem.at[1]),
    ]
    loads = [
        pltpu.make_async_copy(rows_hbm.at[layer], rows_ref.at[layer], rows_sem.at[layer])
        for layer in range(layers)
    ]
    for copy in small + loads:
        copy.start()
    for copy in small:
        copy.wait()
    choose, places = slot_choice(patch_count, req_count, owner_ref[...], place_ref[...])
    choose_ref[...] = choose
    places_ref[...] = places

    def layer_rows(layer):
        loads[layer].wait()
        return rows_ref[layer]

    per = src_rows // (patch_count * req_count)
    pack_slots(0, per, choose, places, layer_rows, layers, outs)


def rest_kernel(first, per, choose_ref, places_ref, rows_ref, *outs):
    pack_slots(
        first,
        per,
        choose_ref[...],
        places_ref[...],
        lambda layer: rows_ref[layer],
        rows_ref.shape[0],
        outs,
    )


def group_rows(patch_map, image_places, image_rows, patch_count, req_count):
    layers, src_rows, width = image_rows.shape
    groups = patch_count * req_count
    per = src_rows // groups
    chunk = jax.ShapeDtypeStruct((layers * per * width // LANES + SUBLANES, LANES), jnp.bfloat16)
    hbm = pl.BlockSpec(memory_space=pltpu.HBM)
    vmem = pl.BlockSpec(memory_space=pltpu.VMEM)

    def cost(count):
        return pl.CostEstimate(
            flops=2 * layers * src_rows * per * count * width,
            bytes_accessed=2 * layers * (src_rows + per * count) * width,
            transcendentals=0,
        )

    choose, places, *first = pl.pallas_call(
        functools.partial(first_kernel, patch_count, req_count),
        out_shape=[
            jax.ShapeDtypeStruct((src_rows, src_rows), jnp.bfloat16),
            jax.ShapeDtypeStruct((SUBLANES, src_rows), jnp.bfloat16),
        ]
        + [chunk] * req_count,
        in_specs=[hbm] * 3,
        out_specs=[vmem] * (2 + req_count),
        scratch_shapes=[
            pltpu.VMEM((1, src_rows), jnp.int32),
            pltpu.VMEM((1, src_rows), jnp.int32),
            pltpu.VMEM(image_rows.shape, jnp.bfloat16),
            pltpu.SemaphoreType.DMA((2,)),
            pltpu.SemaphoreType.DMA((layers,)),
        ],
        cost_estimate=cost(req_count),
        compiler_params=pltpu.CompilerParams(vmem_limit_bytes=WIDE_VMEM_LIMIT),
        name="group_first",
    )(patch_map.reshape(1, src_rows), image_places.reshape(1, src_rows), image_rows)
    rest_call = pl.pallas_call(
        functools.partial(rest_kernel, req_count, per),
        out_shape=[chunk] * (groups - req_count),
        in_specs=[vmem] * 3,
        out_specs=[vmem] * (groups - req_count),
        cost_estimate=cost(groups - req_count),
        compiler_params=pltpu.CompilerParams(vmem_limit_bytes=VMEM_LIMIT),
        name="group_rest",
    )
    rest = rest_call(choose, places, image_rows)
    return [*first, *rest]


def heads_of(line, group):
    row = lax.broadcasted_iota(jnp.int32, (SUBLANES, HEAD_DIM), 0)
    tiles = []
    for g in range(KV_HEADS):
        tile = jnp.zeros((SUBLANES, HEAD_DIM), jnp.float32)
        for i in range(group):
            h = g * group + i
            tile = jnp.where(row == i, line[:, h * HEAD_DIM : (h + 1) * HEAD_DIM], tile)
        tiles.append(tile)
    return jnp.concatenate(tiles, axis=0).astype(jnp.bfloat16)


def attend(queries, keys, values, used, scale):
    scores = jnp.concatenate(
        [
            lax.dot_general(
                queries[g * SUBLANES : (g + 1) * SUBLANES],
                keys[g],
                (((1,), (1,)), ((), ())),
                preferred_element_type=jnp.float32,
            )
            for g in range(KV_HEADS)
        ],
        axis=0,
    )
    scores = scores * scale
    if used is not None:
        scores = jnp.where(used, scores, MASKED)
    top = jnp.max(scores, axis=1, keepdims=True)
    weights = jnp.exp(scores - top)
    if used is not None:
        weights = jnp.where(used, weights, 0.0)
    total = jnp.sum(weights, axis=1, keepdims=True)
    rounded = weights.astype(jnp.bfloat16)
    summed = jnp.concatenate(
        [
            jnp.dot(
                rounded[g * SUBLANES : (g + 1) * SUBLANES],
                values[g],
                preferred_element_type=jnp.float32,
            )
            for g in range(KV_HEADS)
        ],
        axis=0,
    )
    return top, total, summed


def text_kernel(scale, len_ref, query_ref, text_ref, q_ref, top_ref, total_ref, sum_ref):
    text_dev, width = text_ref.shape
    group = query_ref.shape[1] // HEAD_DIM // KV_HEADS
    queries = heads_of(query_ref[...].astype(jnp.float32), group)
    q_ref[...] = queries
    rows = KV_HEADS * SUBLANES
    positions = lax.axis_index("seq") * text_dev + lax.broadcasted_iota(
        jnp.int32, (rows, text_dev), 1
    )
    keys = [text_ref[:, g * HEAD_DIM : (g + 1) * HEAD_DIM] for g in range(KV_HEADS)]
    values = [
        text_ref[:, width // 2 + g * HEAD_DIM : width // 2 + (g + 1) * HEAD_DIM]
        for g in range(KV_HEADS)
    ]
    top, total, summed = attend(queries, keys, values, positions < len_ref[0], scale)
    top_ref[...] = jnp.broadcast_to(top, (rows, LANES))
    total_ref[...] = jnp.broadcast_to(total, (rows, LANES))
    sum_ref[...] = summed


def text_part(query, text_cache, text_len, scale):
    layers, _, query_width = query.shape
    text_dev, width = text_cache.shape[2:]
    rows = KV_HEADS * SUBLANES
    part = pl.BlockSpec((None, rows, LANES), lambda layer, _: (layer, 0, 0))
    return pl.pallas_call(
        functools.partial(text_kernel, scale),
        out_shape=[
            jax.ShapeDtypeStruct((layers, rows, HEAD_DIM), jnp.bfloat16),
            jax.ShapeDtypeStruct((layers, rows, LANES), jnp.float32),
            jax.ShapeDtypeStruct((layers, rows, LANES), jnp.float32),
            jax.ShapeDtypeStruct((layers, rows, HEAD_DIM), jnp.float32),
        ],
        grid_spec=pltpu.PrefetchScalarGridSpec(
            num_scalar_prefetch=1,
            grid=(layers,),
            in_specs=[
                pl.BlockSpec((None, 1, query_width), lambda layer, _: (layer, 0, 0)),
                pl.BlockSpec((None, None, text_dev, width), lambda layer, _: (layer, 0, 0, 0)),
            ],
            out_specs=[part] * 4,
        ),
        cost_estimate=pl.CostEstimate(
            flops=8 * layers * SUBLANES * LANES * text_dev * width,
            bytes_accessed=2 * layers * text_dev * width,
            transcendentals=layers * rows * text_dev,
        ),
        compiler_params=pltpu.CompilerParams(vmem_limit_bytes=VMEM_LIMIT),
        name="text_part",
    )(text_len, query, text_cache)


def image_layer(scale, layer, chunks, used, q_ref, top, total, summed):
    layers = q_ref.shape[0]
    blocks = 2 * KV_HEADS
    per = (chunks[0].shape[0] - SUBLANES) // layers // blocks

    def column(c):
        span = pl.ds((layer * blocks + c) * per, per)
        return jnp.concatenate([chunk[span, :] for chunk in chunks], axis=0)

    keys = [column(g) for g in range(KV_HEADS)]
    values = [column(KV_HEADS + g) for g in range(KV_HEADS)]
    new_top, new_total, new_summed = attend(q_ref[layer], keys, values, used, scale)
    both = jnp.maximum(top, new_top)
    old_factor = jnp.exp(top - both)
    new_factor = jnp.exp(new_top - both)
    total = old_factor * total + new_factor * new_total
    summed = old_factor * summed + new_factor * new_summed
    return both, total, summed


def pack_part(top, total, summed):
    row = lax.broadcasted_iota(jnp.int32, (SUBLANES, LANES), 0)
    lane = lax.broadcasted_iota(jnp.int32, (SUBLANES, LANES), 1)
    stats = jnp.where(lane == row, top, jnp.where(lane == row + LANES // 2, total, 0.0))
    stats = jnp.sum(stats, axis=0, keepdims=True)
    return jnp.where(row == SUBLANES - 1, stats, summed)


def unpack_part(tile):
    row = lax.broadcasted_iota(jnp.int32, (SUBLANES, LANES), 0)
    lane = lax.broadcasted_iota(jnp.int32, (SUBLANES, LANES), 1)
    stats = jnp.broadcast_to(tile[SUBLANES - 1 :, :], (SUBLANES, LANES))
    top = jnp.sum(jnp.where(lane == row, stats, 0.0), axis=1, keepdims=True)
    total = jnp.sum(jnp.where(lane == row + LANES // 2, stats, 0.0), axis=1, keepdims=True)
    return jnp.where(total > 0.0, top, MASKED), total, tile


def merge_tiles(tiles):
    parts = [unpack_part(tile) for tile in tiles]
    top = functools.reduce(jnp.maximum, [part[0] for part in parts])
    factors = [jnp.exp(part[0] - top) for part in parts]
    total = sum(factor * part[1] for factor, part in zip(factors, parts))
    summed = sum(factor * part[2] for factor, part in zip(factors, parts))
    return top, total, summed


def here_kernel(scale, groups, sure, outer, q_ref, top_in, total_in, sum_in, *refs):
    chunks, outs, packed = refs[:groups], refs[groups:-1], refs[-1]
    layers, rows = q_ref.shape[:2]
    per = (chunks[0].shape[0] - SUBLANES) // layers // (2 * KV_HEADS)
    patch = lax.axis_index("patch")
    limit = functools.reduce(
        lambda found, z: jnp.where(patch == z, groups * per, found), outer, sure * per
    )
    used = lax.broadcasted_iota(jnp.int32, (rows, groups * per), 1) < limit
    for layer in range(q_ref.shape[0]):
        top, total, summed = image_layer(
            scale,
            layer,
            chunks,
            used,
            q_ref,
            top_in[layer][:, :1],
            total_in[layer][:, :1],
            sum_in[layer],
        )
        for g in range(KV_HEADS):
            span = slice(g * SUBLANES, (g + 1) * SUBLANES)
            packed[g, pl.ds(layer * SUBLANES, SUBLANES), :] = pack_part(
                top[span], total[span], summed[span]
            )
    me = lax.axis_index("seq")
    for k in range(KV_HEADS):
        outs[k][...] = packed[me ^ k]


def far_kernel(scale, count, *refs):
    queries, chunks = refs[:count], refs[count : 2 * count]
    outs, packed = refs[2 * count : -1], refs[-1]
    layers = queries[0].shape[0]
    blocks = 2 * KV_HEADS
    group = queries[0].shape[1] // HEAD_DIM // KV_HEADS
    for n in range(count):
        chunk = chunks[n]
        per = (chunk.shape[0] - SUBLANES) // layers // blocks
        for layer in range(layers):
            columns = [
                chunk[pl.ds((layer * blocks + c) * per, per), :] for c in range(blocks)
            ]
            line = queries[n][pl.ds(layer, 1), :].astype(jnp.float32)
            top, total, summed = attend(
                heads_of(line, group), columns[:KV_HEADS], columns[KV_HEADS:], None, scale
            )
            for g in range(KV_HEADS):
                span = slice(g * SUBLANES, (g + 1) * SUBLANES)
                packed[g, pl.ds((n * layers + layer) * SUBLANES, SUBLANES), :] = pack_part(
                    top[span], total[span], summed[span]
                )
    me = lax.axis_index("seq")
    for k in range(KV_HEADS):
        outs[k][...] = packed[me ^ k]


def seq_parts(kernel, operands, part_rows, chunk_rows, groups):
    shape = (part_rows, LANES)
    vmem = pl.BlockSpec(memory_space=pltpu.VMEM)
    return pl.pallas_call(
        kernel,
        out_shape=[jax.ShapeDtypeStruct(shape, jnp.float32)] * KV_HEADS,
        in_specs=[vmem] * len(operands),
        out_specs=[vmem] * KV_HEADS,
        scratch_shapes=[pltpu.VMEM((KV_HEADS,) + shape, jnp.float32)],
        cost_estimate=pl.CostEstimate(
            flops=8 * SUBLANES * chunk_rows * LANES * groups,
            bytes_accessed=2 * chunk_rows * LANES * groups,
            transcendentals=SUBLANES * chunk_rows * groups,
        ),
        compiler_params=pltpu.CompilerParams(vmem_limit_bytes=VMEM_LIMIT),
    )(*operands)


def seq_exchange(outs):
    arrived = [
        lax.ppermute(out, "seq", [(s, s ^ k) for s in range(KV_HEADS)])
        for k, out in enumerate(outs)
        if k
    ]
    return [outs[0], *arrived]


def merge_far_kernel(count, *refs):
    parts, outs = refs[:-count], refs[-count:]
    rows = parts[0].shape[0] // count
    for n, out in enumerate(outs):
        for at in range(0, rows, SUBLANES):
            tiles = [part[pl.ds(n * rows + at, SUBLANES), :] for part in parts]
            out[pl.ds(at, SUBLANES), :] = pack_part(*merge_tiles(tiles))


def merge_far(parts, count):
    rows = parts[0].shape[0] // count
    vmem = pl.BlockSpec(memory_space=pltpu.VMEM)
    return pl.pallas_call(
        functools.partial(merge_far_kernel, count),
        out_shape=[jax.ShapeDtypeStruct((rows, LANES), jnp.float32)] * count,
        in_specs=[vmem] * len(parts),
        out_specs=[vmem] * count,
        compiler_params=pltpu.CompilerParams(vmem_limit_bytes=VMEM_LIMIT),
        name="merge_far",
    )(*parts)


def place_kernel(owners, *refs):
    out_hbm, out_ref, sems = refs[-3:]
    groups = len(owners)

    def rows_of(k, span):
        first, *others = [refs[n][span, :] for n in owners[k]]
        return sum(others, first)

    layers, band, width = out_ref.shape
    blocks = width // LANES
    per = band // groups
    stores = [
        pltpu.make_async_copy(out_ref.at[layer], out_hbm.at[layer], sems.at[layer])
        for layer in range(layers)
    ]
    base = layers * blocks * per
    lane = lax.broadcasted_iota(jnp.int32, (SUBLANES, LANES), 1)
    tiles = []
    for tile in range(band // LANES):
        row = jnp.zeros((SUBLANES, LANES), jnp.float32)
        for k in range(groups):
            if k * per // LANES == tile:
                extra = rows_of(k, pl.ds(base, SUBLANES)).astype(jnp.float32)
                inside = (lane >= k * per % LANES) & (lane < k * per % LANES + per)
                row = jnp.where(inside, extra, row)
        tiles.append(row)
    digits = jnp.concatenate(tiles, axis=1).astype(jnp.int32)
    places = digits[0:1] + digits[1:2] * LANES
    down = lax.broadcasted_iota(jnp.int32, (band, band), 0)
    choose = jnp.where(down == places, 1.0, 0.0).astype(jnp.bfloat16)
    for layer in range(layers):
        for c in range(blocks):
            span = pl.ds((layer * blocks + c) * per, per)
            column = jnp.concatenate([rows_of(k, span) for k in range(groups)], axis=0)
            out_ref[layer, :, c * LANES : (c + 1) * LANES] = jnp.dot(
                choose, column, preferred_element_type=jnp.float32
            ).astype(jnp.bfloat16)
        stores[layer].start()
    for store in stores:
        store.wait()


def place_rows(slots, layers, band, width):
    operands = [chunk for slot in slots for chunk in slot]
    count = iter(range(len(operands)))
    owners = [[next(count) for _ in slot] for slot in slots]
    vmem = pl.BlockSpec(memory_space=pltpu.VMEM)
    return pl.pallas_call(
        functools.partial(place_kernel, owners),
        out_shape=jax.ShapeDtypeStruct((layers, band, width), jnp.bfloat16),
        in_specs=[vmem] * len(operands),
        out_specs=pl.BlockSpec(memory_space=pltpu.HBM),
        scratch_shapes=[
            pltpu.VMEM((layers, band, width), jnp.bfloat16),
            pltpu.SemaphoreType.DMA((layers,)),
        ],
        cost_estimate=pl.CostEstimate(
            flops=2 * layers * band * band * width,
            bytes_accessed=4 * layers * band * width,
            transcendentals=0,
        ),
        compiler_params=pltpu.CompilerParams(vmem_limit_bytes=VMEM_LIMIT),
        name="place_rows",
    )(*operands)


def merge_kernel(group, *refs):
    parts, out_ref, lines = refs[:-2], refs[-2], refs[-1]
    for layer in range(out_ref.shape[0]):
        tiles = [part[pl.ds(layer * SUBLANES, SUBLANES), :] for part in parts]
        _, total, summed = merge_tiles(tiles)
        result = summed / total
        for i in range(group):
            lines[pl.ds(layer, 1), i * HEAD_DIM : (i + 1) * HEAD_DIM] = result[i : i + 1]
    out_ref[...] = lines[...].astype(jnp.bfloat16)


def merge(parts, layers, group):
    vmem = pl.BlockSpec(memory_space=pltpu.VMEM)
    return pl.pallas_call(
        functools.partial(merge_kernel, group),
        out_shape=jax.ShapeDtypeStruct((layers, group * HEAD_DIM), jnp.bfloat16),
        in_specs=[vmem] * len(parts),
        out_specs=vmem,
        scratch_shapes=[pltpu.VMEM((layers, group * HEAD_DIM), jnp.float32)],
        compiler_params=pltpu.CompilerParams(vmem_limit_bytes=VMEM_LIMIT),
        name="merge",
    )(*parts)


def exchange_pairs(patch_count, req_count, step, turn):
    pairs = []
    for patch in range(patch_count):
        for req in range(req_count):
            target = next(p for p in range(patch_count) if step_of(patch, p, patch_count) == step)
            pairs.append(
                (patch * req_count + req, target * req_count + (req + turn) % req_count)
            )
    return pairs


def fast_body(query, text_cache, text_len, image_rows, patch_map, image_places):
    layers = query.shape[0]
    patch_count = lax.axis_size("patch")
    req_count = lax.axis_size("req")
    band, width = image_rows.shape[1:]
    group = HEADS // KV_HEADS
    scale = 1.0 / math.sqrt(HEAD_DIM)
    slots = [[step * req_count + turn for turn in range(req_count)] for step in range(patch_count)]
    last = patch_count // 2 - 1
    late = slots[last]
    early = [k for step in range(patch_count - 1) if step != last for k in slots[step]]
    own, core = slots[-1][0], slots[-1][1:]
    pairs = [
        exchange_pairs(patch_count, req_count, k // req_count, k % req_count)
        for k in range(patch_count * req_count)
    ]
    axes = ("patch", "req")
    reach = {
        source: abs(target // req_count - source // req_count) for source, target in pairs[late[0]]
    }
    near = min(reach.values())
    outer = sorted({source // req_count for source, hops in reach.items() if hops > near})
    inner_pairs = {k: [pair for pair in pairs[k] if reach[pair[0]] == near] for k in late}
    outer_pairs = {k: [pair for pair in pairs[k] if reach[pair[0]] > near] for k in late}
    flat_query = query[:, 0]

    def send(value, some):
        return lax.ppermute(value, axes, some)

    far_queries = [
        send(flat_query, [(target, source) for source, target in inner_pairs[k]])
        for k in late
    ]
    grouped = group_rows(patch_map, image_places, image_rows, patch_count, req_count)
    arrived = {own: [grouped[own]]}
    for k in early + core:
        arrived[k] = [send(grouped[k], pairs[k])]
    for k in late:
        arrived[k] = [send(grouped[k], some) for some in (inner_pairs[k], outer_pairs[k]) if some]
    chunk_rows = grouped[0].shape[0]
    part_rows = layers * SUBLANES
    far = seq_parts(
        functools.partial(far_kernel, scale, len(late)),
        [*far_queries, *(grouped[k] for k in late)],
        len(late) * part_rows,
        chunk_rows,
        len(late),
    )
    far = merge_far(seq_exchange(far), len(late))
    far = [lax.ppermute(part, axes, inner_pairs[k]) for part, k in zip(far, late)]
    text = text_part(query, text_cache, text_len, scale)
    here = [arrived[k][0] for k in early + core + [own]]
    sure = len(here)
    here += [arrived[k][1] for k in late if outer]
    parts = seq_parts(
        functools.partial(here_kernel, scale, len(here), sure, outer),
        [*text, *here],
        part_rows,
        chunk_rows,
        len(here),
    )
    attended = merge([*seq_exchange(parts), *far], layers, group)
    image_cache = place_rows([arrived[k] for k in range(len(grouped))], layers, band, width)
    return attended[:, None, :], image_cache[:, None]


def plain_body(query, text_cache, text_len, image_rows, patch_map, image_places):
    layers, req_dev, query_width = query.shape
    text_dev = text_cache.shape[2]
    full_width = text_cache.shape[3]
    kv_width = full_width // 2
    head_dim = HEAD_DIM
    kv_heads = KV_HEADS
    heads = HEADS
    group = heads // kv_heads
    src_rows = image_rows.shape[1]
    patch_count = lax.axis_size("patch")
    req_count = lax.axis_size("req")
    seq_count = lax.axis_size("seq")
    seq_index = lax.axis_index("seq")
    per_source = src_rows // (patch_count * req_count * req_dev)
    band_size = per_source * patch_count * req_count
    scale = 1.0 / math.sqrt(head_dim)
    order = jnp.argsort(patch_map, stable=True)
    grouped = jnp.take(image_rows, order, axis=1)
    grouped_places = jnp.take(image_places, order)
    sending = grouped.reshape(layers, patch_count * req_count, req_dev, per_source, full_width)
    arrived = lax.all_to_all(sending, ("patch", "req"), split_axis=1, concat_axis=3, tiled=True)
    place_send = grouped_places.reshape(patch_count * req_count, req_dev, per_source)
    arrived_places = lax.all_to_all(
        place_send, ("patch", "req"), split_axis=0, concat_axis=2, tiled=True
    )
    image_block = arrived.reshape(layers, req_dev, band_size, full_width)
    local_places = arrived_places.reshape(req_dev, band_size) - seq_index * band_size
    inverse = jnp.argsort(local_places, axis=1)
    image_cache = jnp.take_along_axis(image_block, inverse[None, :, :, None], axis=2)
    queries = query.reshape(layers, req_dev, kv_heads, group, head_dim)
    text_keys = text_cache[..., :kv_width].reshape(layers, req_dev, text_dev, kv_heads, head_dim)
    text_values = text_cache[..., kv_width:].reshape(layers, req_dev, text_dev, kv_heads, head_dim)
    image_keys = image_block[..., :kv_width].reshape(layers, req_dev, band_size, kv_heads, head_dim)
    image_values = image_block[..., kv_width:].reshape(
        layers, req_dev, band_size, kv_heads, head_dim
    )
    positions = seq_index * text_dev + jnp.arange(text_dev, dtype=jnp.int32)
    used = positions[None, :] < text_len[:, None]
    text_raw = (
        jnp.einsum("lrkgd,lrtkd->lrkgt", queries, text_keys, preferred_element_type=jnp.float32)
        * scale
    )
    text_scores = jnp.where(used[None, :, None, None, :], text_raw, -jnp.inf)
    image_scores = (
        jnp.einsum("lrkgd,lrtkd->lrkgt", queries, image_keys, preferred_element_type=jnp.float32)
        * scale
    )
    local_top = jnp.maximum(jnp.max(text_scores, axis=-1), jnp.max(image_scores, axis=-1))
    text_weights = jnp.exp(text_scores - local_top[..., None])
    image_weights = jnp.exp(image_scores - local_top[..., None])
    local_total = jnp.sum(text_weights, axis=-1) + jnp.sum(image_weights, axis=-1)
    text_rounded = text_weights.astype(jnp.bfloat16)
    image_rounded = image_weights.astype(jnp.bfloat16)
    local_values = jnp.einsum(
        "lrkgt,lrtkd->lrkgd", image_rounded, image_values, preferred_element_type=jnp.float32
    )
    local_values = local_values + jnp.einsum(
        "lrkgt,lrtkd->lrkgd", text_rounded, text_values, preferred_element_type=jnp.float32
    )
    width_dev = query_width // seq_count
    top = lax.pmax(local_top, "seq")
    factor = jnp.exp(local_top - top)
    scaled_total = factor * local_total
    scaled_values = factor[..., None] * local_values
    total_sum, value_sum = lax.psum((scaled_total, scaled_values), "seq")
    result = (value_sum / total_sum[..., None]).reshape(layers, req_dev, query_width)
    attended = lax.dynamic_slice_in_dim(result, seq_index * width_dev, width_dev, 2).astype(
        jnp.bfloat16
    )
    return (attended, image_cache)


def body(query, text_cache, text_len, image_rows, patch_map, image_places):
    groups = lax.axis_size("patch") * lax.axis_size("req")
    band = image_rows.shape[1]
    per = band // groups
    fast = (
        query.shape[1] == 1
        and lax.axis_size("patch") >= 2
        and groups <= MOST_GROUPS
        and band == per * groups
        and band % LANES == 0
        and per % 16 == 0
        and LANES % per == 0
        and lax.axis_size("seq") == KV_HEADS
        and HEADS // KV_HEADS < SUBLANES
    )
    chosen = fast_body if fast else plain_body
    return chosen(query, text_cache, text_len, image_rows, patch_map, image_places)


def solution(mesh):
    return jax.shard_map(
        body,
        mesh=mesh,
        in_specs=(
            P(None, ("patch", "req"), None),
            P(None, ("patch", "req"), "seq", None),
            P(("patch", "req")),
            P(None, ("patch", "seq", "req"), None),
            P(("patch", "seq", "req")),
            P(("patch", "seq", "req")),
        ),
        out_specs=(P(None, ("patch", "req"), "seq"), P(None, ("patch", "req"), "seq", None)),
        check_vma=False,
    )
```

```python
import functools
import math

import jax
import jax.numpy as jnp
from jax import lax
from jax.experimental import pallas as pl
from jax.experimental.pallas import tpu as pltpu
from jax.sharding import PartitionSpec as P


HEADS = 28
KV_HEADS = 4
HEAD_DIM = 128
LANES = 128
SUBLANES = 8
MASKED = -1e30

MOST_GROUPS = 16
VMEM_LIMIT = 16 * 1024 * 1024
WIDE_VMEM_LIMIT = 62 * 1024 * 1024


def gray(index):
    return index ^ (index >> 1)


def step_of(source, target, count):
    if count & (count - 1) == 0:
        return (gray(target) - gray(source) + count - 1) & (count - 1)
    return (target - source + count - 1) % count


def slot_choice(patch_count, req_count, owner, place):
    src_rows = owner.shape[1]
    per = src_rows // (patch_count * req_count)
    me = lax.axis_index("patch")
    mine = lax.axis_index("req")
    shape = (src_rows, src_rows)
    down = lax.broadcasted_iota(jnp.int32, shape, 0)
    across = lax.broadcasted_iota(jnp.int32, shape, 1)
    owner_row = jnp.broadcast_to(owner, shape)
    owner_col = jnp.sum(
        jnp.where(down == across, owner_row.astype(jnp.float32), 0.0), axis=1, keepdims=True
    ).astype(jnp.int32)
    ahead = (owner_row == owner_col) & (down < across)
    rank = jnp.sum(jnp.where(ahead, 1.0, 0.0), axis=0, keepdims=True).astype(jnp.int32)
    step = step_of(me, owner // req_count, patch_count)
    turn = (owner % req_count - mine + req_count) % req_count
    slot = (step * req_count + turn) * per + rank
    choose = jnp.where(down == slot, 1.0, 0.0).astype(jnp.bfloat16)
    local = place - lax.axis_index("seq") * src_rows
    line = lax.broadcasted_iota(jnp.int32, (SUBLANES, src_rows), 0)
    digits = jnp.where(line == 0, local & (LANES - 1), jnp.where(line == 1, local // LANES, 0))
    places = lax.dot_general(
        digits.astype(jnp.float32).astype(jnp.bfloat16),
        choose,
        (((1,), (1,)), ((), ())),
        preferred_element_type=jnp.float32,
    ).astype(jnp.bfloat16)
    return choose, places


def pack_slots(first, per, choose, places, layer_rows, layers, outs):
    for k, out in enumerate(outs):
        tile = (first + k) * per // LANES
        out[pl.ds(out.shape[0] - SUBLANES, SUBLANES), :] = places[
            :, tile * LANES : (tile + 1) * LANES
        ]
    taken = choose[first * per : (first + len(outs)) * per]
    for layer in range(layers):
        rows = layer_rows(layer)
        blocks = rows.shape[1] // LANES
        moved = jnp.dot(taken, rows, preferred_element_type=jnp.float32).astype(jnp.bfloat16)
        for k, out in enumerate(outs):
            for c in range(blocks):
                out[pl.ds((layer * blocks + c) * per, per), :] = moved[
                    k * per : (k + 1) * per, c * LANES : (c + 1) * LANES
                ]


def first_kernel(patch_count, req_count, map_hbm, place_hbm, rows_hbm, *refs):
    choose_ref, places_ref, *outs = refs[:-5]
    owner_ref, place_ref, rows_ref, small_sem, rows_sem = refs[-5:]
    layers, src_rows, _ = rows_hbm.shape
    small = [
        pltpu.make_async_copy(map_hbm, owner_ref, small_sem.at[0]),
        pltpu.make_async_copy(place_hbm, place_ref, small_sem.at[1]),
    ]
    loads = [
        pltpu.make_async_copy(rows_hbm.at[layer], rows_ref.at[layer], rows_sem.at[layer])
        for layer in range(layers)
    ]
    for copy in small + loads:
        copy.start()
    for copy in small:
        copy.wait()
    choose, places = slot_choice(patch_count, req_count, owner_ref[...], place_ref[...])
    choose_ref[...] = choose
    places_ref[...] = places

    def layer_rows(layer):
        loads[layer].wait()
        return rows_ref[layer]

    per = src_rows // (patch_count * req_count)
    pack_slots(0, per, choose, places, layer_rows, layers, outs)


def rest_kernel(first, per, choose_ref, places_ref, rows_ref, *outs):
    pack_slots(
        first,
        per,
        choose_ref[...],
        places_ref[...],
        lambda layer: rows_ref[layer],
        rows_ref.shape[0],
        outs,
    )


def group_rows(patch_map, image_places, image_rows, patch_count, req_count):
    layers, src_rows, width = image_rows.shape
    groups = patch_count * req_count
    per = src_rows // groups
    chunk = jax.ShapeDtypeStruct((layers * per * width // LANES + SUBLANES, LANES), jnp.bfloat16)
    hbm = pl.BlockSpec(memory_space=pltpu.HBM)
    vmem = pl.BlockSpec(memory_space=pltpu.VMEM)

    def cost(count):
        return pl.CostEstimate(
            flops=2 * layers * src_rows * per * count * width,
            bytes_accessed=2 * layers * (src_rows + per * count) * width,
            transcendentals=0,
        )

    first_call = pl.pallas_call(
        functools.partial(first_kernel, patch_count, req_count),
        out_shape=[
            jax.ShapeDtypeStruct((src_rows, src_rows), jnp.bfloat16),
            jax.ShapeDtypeStruct((SUBLANES, src_rows), jnp.bfloat16),
        ]
        + [chunk] * req_count,
        in_specs=[hbm] * 3,
        out_specs=[vmem] * (2 + req_count),
        scratch_shapes=[
            pltpu.VMEM((1, src_rows), jnp.int32),
            pltpu.VMEM((1, src_rows), jnp.int32),
            pltpu.VMEM(image_rows.shape, jnp.bfloat16),
            pltpu.SemaphoreType.DMA((2,)),
            pltpu.SemaphoreType.DMA((layers,)),
        ],
        cost_estimate=cost(req_count),
        compiler_params=pltpu.CompilerParams(vmem_limit_bytes=WIDE_VMEM_LIMIT),
        name="group_first",
    )
    choose, places, *first = first_call(
        patch_map.reshape(1, src_rows), image_places.reshape(1, src_rows), image_rows
    )
    rest_call = pl.pallas_call(
        functools.partial(rest_kernel, req_count, per),
        out_shape=[chunk] * (groups - req_count),
        in_specs=[vmem] * 3,
        out_specs=[vmem] * (groups - req_count),
        cost_estimate=cost(groups - req_count),
        compiler_params=pltpu.CompilerParams(vmem_limit_bytes=VMEM_LIMIT),
        name="group_rest",
    )
    rest = rest_call(choose, places, image_rows)
    return [*first, *rest]


def heads_of(line, group):
    row = lax.broadcasted_iota(jnp.int32, (SUBLANES, HEAD_DIM), 0)
    tiles = []
    for g in range(KV_HEADS):
        tile = jnp.zeros((SUBLANES, HEAD_DIM), jnp.float32)
        for i in range(group):
            h = g * group + i
            tile = jnp.where(row == i, line[:, h * HEAD_DIM : (h + 1) * HEAD_DIM], tile)
        tiles.append(tile)
    return jnp.concatenate(tiles, axis=0).astype(jnp.bfloat16)


def attend(queries, keys, values, used, scale):
    scores = jnp.concatenate(
        [
            lax.dot_general(
                queries[g * SUBLANES : (g + 1) * SUBLANES],
                keys[g],
                (((1,), (1,)), ((), ())),
                preferred_element_type=jnp.float32,
            )
            for g in range(KV_HEADS)
        ],
        axis=0,
    )
    scores = scores * scale
    if used is not None:
        scores = jnp.where(used, scores, MASKED)
    top = jnp.max(scores, axis=1, keepdims=True)
    weights = jnp.exp(scores - top)
    if used is not None:
        weights = jnp.where(used, weights, 0.0)
    total = jnp.sum(weights, axis=1, keepdims=True)
    rounded = weights.astype(jnp.bfloat16)
    summed = jnp.concatenate(
        [
            jnp.dot(
                rounded[g * SUBLANES : (g + 1) * SUBLANES],
                values[g],
                preferred_element_type=jnp.float32,
            )
            for g in range(KV_HEADS)
        ],
        axis=0,
    )
    return top, total, summed


def text_kernel(scale, len_ref, query_ref, text_ref, q_ref, top_ref, total_ref, sum_ref):
    text_dev, width = text_ref.shape
    group = query_ref.shape[1] // HEAD_DIM // KV_HEADS
    queries = heads_of(query_ref[...].astype(jnp.float32), group)
    q_ref[...] = queries
    rows = KV_HEADS * SUBLANES
    positions = lax.axis_index("seq") * text_dev + lax.broadcasted_iota(
        jnp.int32, (rows, text_dev), 1
    )
    keys = [text_ref[:, g * HEAD_DIM : (g + 1) * HEAD_DIM] for g in range(KV_HEADS)]
    values = [
        text_ref[:, width // 2 + g * HEAD_DIM : width // 2 + (g + 1) * HEAD_DIM]
        for g in range(KV_HEADS)
    ]
    top, total, summed = attend(queries, keys, values, positions < len_ref[0], scale)
    top_ref[...] = jnp.broadcast_to(top, (rows, LANES))
    total_ref[...] = jnp.broadcast_to(total, (rows, LANES))
    sum_ref[...] = summed


def text_part(query, text_cache, text_len, scale):
    layers, _, query_width = query.shape
    text_dev, width = text_cache.shape[2:]
    rows = KV_HEADS * SUBLANES
    part = pl.BlockSpec((None, rows, LANES), lambda layer, _: (layer, 0, 0))
    return pl.pallas_call(
        functools.partial(text_kernel, scale),
        out_shape=[
            jax.ShapeDtypeStruct((layers, rows, HEAD_DIM), jnp.bfloat16),
            jax.ShapeDtypeStruct((layers, rows, LANES), jnp.float32),
            jax.ShapeDtypeStruct((layers, rows, LANES), jnp.float32),
            jax.ShapeDtypeStruct((layers, rows, HEAD_DIM), jnp.float32),
        ],
        grid_spec=pltpu.PrefetchScalarGridSpec(
            num_scalar_prefetch=1,
            grid=(layers,),
            in_specs=[
                pl.BlockSpec((None, 1, query_width), lambda layer, _: (layer, 0, 0)),
                pl.BlockSpec((None, None, text_dev, width), lambda layer, _: (layer, 0, 0, 0)),
            ],
            out_specs=[part] * 4,
        ),
        cost_estimate=pl.CostEstimate(
            flops=8 * layers * SUBLANES * LANES * text_dev * width,
            bytes_accessed=2 * layers * text_dev * width,
            transcendentals=layers * rows * text_dev,
        ),
        compiler_params=pltpu.CompilerParams(vmem_limit_bytes=VMEM_LIMIT),
        name="text_part",
    )(text_len, query, text_cache)


def image_layer(scale, layer, chunks, used, q_ref, top, total, summed):
    layers = q_ref.shape[0]
    blocks = 2 * KV_HEADS
    per = (chunks[0].shape[0] - SUBLANES) // layers // blocks

    def column(c):
        span = pl.ds((layer * blocks + c) * per, per)
        return jnp.concatenate([chunk[span, :] for chunk in chunks], axis=0)

    keys = [column(g) for g in range(KV_HEADS)]
    values = [column(KV_HEADS + g) for g in range(KV_HEADS)]
    new_top, new_total, new_summed = attend(q_ref[layer], keys, values, used, scale)
    both = jnp.maximum(top, new_top)
    old_factor = jnp.exp(top - both)
    new_factor = jnp.exp(new_top - both)
    total = old_factor * total + new_factor * new_total
    summed = old_factor * summed + new_factor * new_summed
    return both, total, summed


def pack_part(top, total, summed):
    row = lax.broadcasted_iota(jnp.int32, (SUBLANES, LANES), 0)
    lane = lax.broadcasted_iota(jnp.int32, (SUBLANES, LANES), 1)
    stats = jnp.where(lane == row, top, jnp.where(lane == row + LANES // 2, total, 0.0))
    stats = jnp.sum(stats, axis=0, keepdims=True)
    return jnp.where(row == SUBLANES - 1, stats, summed)


def unpack_part(tile):
    row = lax.broadcasted_iota(jnp.int32, (SUBLANES, LANES), 0)
    lane = lax.broadcasted_iota(jnp.int32, (SUBLANES, LANES), 1)
    stats = jnp.broadcast_to(tile[SUBLANES - 1 :, :], (SUBLANES, LANES))
    top = jnp.sum(jnp.where(lane == row, stats, 0.0), axis=1, keepdims=True)
    total = jnp.sum(jnp.where(lane == row + LANES // 2, stats, 0.0), axis=1, keepdims=True)
    return top, total, tile


def merge_tiles(tiles, used=None):
    parts = [unpack_part(tile) for tile in tiles]
    for n, part in enumerate(parts):
        if used is not None and used[n] is not None:
            parts[n] = [jnp.where(used[n], a, b) for a, b in zip(part, (MASKED, 0.0, 0.0))]
    top = functools.reduce(jnp.maximum, [part[0] for part in parts])
    factors = [jnp.exp(part[0] - top) for part in parts]
    total = sum(factor * part[1] for factor, part in zip(factors, parts))
    summed = sum(factor * part[2] for factor, part in zip(factors, parts))
    return top, total, summed


def here_kernel(scale, groups, sure, outer, q_ref, top_in, total_in, sum_in, *refs):
    chunks, outs, packed = refs[:groups], refs[groups:-1], refs[-1]
    layers, rows = q_ref.shape[:2]
    per = (chunks[0].shape[0] - SUBLANES) // layers // (2 * KV_HEADS)
    limit = jnp.where(is_outer(outer), groups, sure) * per
    used = lax.broadcasted_iota(jnp.int32, (rows, groups * per), 1) < limit
    for layer in range(q_ref.shape[0]):
        top, total, summed = image_layer(
            scale,
            layer,
            chunks,
            used,
            q_ref,
            top_in[layer][:, :1],
            total_in[layer][:, :1],
            sum_in[layer],
        )
        for g in range(KV_HEADS):
            span = slice(g * SUBLANES, (g + 1) * SUBLANES)
            packed[g, pl.ds(layer * SUBLANES, SUBLANES), :] = pack_part(
                top[span], total[span], summed[span]
            )
    me = lax.axis_index("seq")
    for k in range(KV_HEADS):
        outs[k][...] = packed[me ^ k]


def far_kernel(scale, count, *refs):
    queries, chunks = refs[:count], refs[count : 2 * count]
    outs, packed = refs[2 * count : -1], refs[-1]
    layers = queries[0].shape[0]
    blocks = 2 * KV_HEADS
    group = queries[0].shape[1] // HEAD_DIM // KV_HEADS
    for n in range(count):
        chunk = chunks[n]
        per = (chunk.shape[0] - SUBLANES) // layers // blocks
        for layer in range(layers):
            columns = [
                chunk[pl.ds((layer * blocks + c) * per, per), :] for c in range(blocks)
            ]
            line = queries[n][pl.ds(layer, 1), :].astype(jnp.float32)
            top, total, summed = attend(
                heads_of(line, group), columns[:KV_HEADS], columns[KV_HEADS:], None, scale
            )
            for g in range(KV_HEADS):
                span = slice(g * SUBLANES, (g + 1) * SUBLANES)
                packed[g, pl.ds((n * layers + layer) * SUBLANES, SUBLANES), :] = pack_part(
                    top[span], total[span], summed[span]
                )
    me = lax.axis_index("seq")
    for k in range(KV_HEADS):
        outs[k][...] = packed[me ^ k]


def seq_parts(kernel, operands, part_rows, chunk_rows, groups):
    shape = (part_rows, LANES)
    vmem = pl.BlockSpec(memory_space=pltpu.VMEM)
    return pl.pallas_call(
        kernel,
        out_shape=[jax.ShapeDtypeStruct(shape, jnp.float32)] * KV_HEADS,
        in_specs=[vmem] * len(operands),
        out_specs=[vmem] * KV_HEADS,
        scratch_shapes=[pltpu.VMEM((KV_HEADS,) + shape, jnp.float32)],
        cost_estimate=pl.CostEstimate(
            flops=8 * SUBLANES * chunk_rows * LANES * groups,
            bytes_accessed=2 * chunk_rows * LANES * groups,
            transcendentals=SUBLANES * chunk_rows * groups,
        ),
        compiler_params=pltpu.CompilerParams(vmem_limit_bytes=VMEM_LIMIT),
    )(*operands)


def seq_exchange(outs):
    arrived = [
        lax.ppermute(out, "seq", [(s, s ^ k) for s in range(KV_HEADS)])
        for k, out in enumerate(outs)
        if k
    ]
    return [outs[0], *arrived]


def merge_far_kernel(count, *refs):
    parts, outs = refs[:-count], refs[-count:]
    rows = parts[0].shape[0] // count
    for n, out in enumerate(outs):
        for at in range(0, rows, SUBLANES):
            tiles = [part[pl.ds(n * rows + at, SUBLANES), :] for part in parts]
            out[pl.ds(at, SUBLANES), :] = pack_part(*merge_tiles(tiles))


def merge_far(parts, count):
    rows = parts[0].shape[0] // count
    vmem = pl.BlockSpec(memory_space=pltpu.VMEM)
    return pl.pallas_call(
        functools.partial(merge_far_kernel, count),
        out_shape=[jax.ShapeDtypeStruct((rows, LANES), jnp.float32)] * count,
        in_specs=[vmem] * len(parts),
        out_specs=[vmem] * count,
        compiler_params=pltpu.CompilerParams(vmem_limit_bytes=VMEM_LIMIT),
        name="merge_far",
    )(*parts)


def is_outer(outer):
    patch = lax.axis_index("patch")
    return functools.reduce(jnp.logical_or, [patch == z for z in outer])


def place_kernel(owners, outer, *refs):
    out_hbm, out_ref, sems = refs[-3:]
    groups = len(owners)
    outside = is_outer(outer)

    def rows_of(k, span):
        first, *others = [refs[n][span, :] for n in owners[k]]
        return jnp.where(outside, others[0], first) if others else first

    layers, band, width = out_ref.shape
    blocks = width // LANES
    per = band // groups
    stores = [
        pltpu.make_async_copy(out_ref.at[layer], out_hbm.at[layer], sems.at[layer])
        for layer in range(layers)
    ]
    base = layers * blocks * per
    lane = lax.broadcasted_iota(jnp.int32, (SUBLANES, LANES), 1)
    tiles = []
    for tile in range(band // LANES):
        row = jnp.zeros((SUBLANES, LANES), jnp.float32)
        for k in range(groups):
            if k * per // LANES == tile:
                extra = rows_of(k, pl.ds(base, SUBLANES)).astype(jnp.float32)
                inside = (lane >= k * per % LANES) & (lane < k * per % LANES + per)
                row = jnp.where(inside, extra, row)
        tiles.append(row)
    digits = jnp.concatenate(tiles, axis=1).astype(jnp.int32)
    places = digits[0:1] + digits[1:2] * LANES
    down = lax.broadcasted_iota(jnp.int32, (band, band), 0)
    choose = jnp.where(down == places, 1.0, 0.0).astype(jnp.bfloat16)
    for layer in range(layers):
        for c in range(blocks):
            span = pl.ds((layer * blocks + c) * per, per)
            column = jnp.concatenate([rows_of(k, span) for k in range(groups)], axis=0)
            out_ref[layer, :, c * LANES : (c + 1) * LANES] = jnp.dot(
                choose, column, preferred_element_type=jnp.float32
            ).astype(jnp.bfloat16)
        stores[layer].start()
    for store in stores:
        store.wait()


def place_rows(slots, outer, layers, band, width):
    operands = [chunk for slot in slots for chunk in slot]
    count = iter(range(len(operands)))
    owners = [[next(count) for _ in slot] for slot in slots]
    vmem = pl.BlockSpec(memory_space=pltpu.VMEM)
    return pl.pallas_call(
        functools.partial(place_kernel, owners, outer),
        out_shape=jax.ShapeDtypeStruct((layers, band, width), jnp.bfloat16),
        in_specs=[vmem] * len(operands),
        out_specs=pl.BlockSpec(memory_space=pltpu.HBM),
        scratch_shapes=[
            pltpu.VMEM((layers, band, width), jnp.bfloat16),
            pltpu.SemaphoreType.DMA((layers,)),
        ],
        cost_estimate=pl.CostEstimate(
            flops=2 * layers * band * band * width,
            bytes_accessed=4 * layers * band * width,
            transcendentals=0,
        ),
        compiler_params=pltpu.CompilerParams(vmem_limit_bytes=VMEM_LIMIT),
        name="place_rows",
    )(*operands)


def merge_kernel(group, sure, outer, *refs):
    parts, out_ref, lines = refs[:-2], refs[-2], refs[-1]
    inside = jnp.logical_not(is_outer(outer))
    used = [None if n < sure else inside for n in range(len(parts))]
    for layer in range(out_ref.shape[0]):
        tiles = [part[pl.ds(layer * SUBLANES, SUBLANES), :] for part in parts]
        _, total, summed = merge_tiles(tiles, used)
        result = summed / total
        for i in range(group):
            lines[pl.ds(layer, 1), i * HEAD_DIM : (i + 1) * HEAD_DIM] = result[i : i + 1]
    out_ref[...] = lines[...].astype(jnp.bfloat16)


def merge(parts, sure, outer, layers, group):
    vmem = pl.BlockSpec(memory_space=pltpu.VMEM)
    return pl.pallas_call(
        functools.partial(merge_kernel, group, sure, outer),
        out_shape=jax.ShapeDtypeStruct((layers, group * HEAD_DIM), jnp.bfloat16),
        in_specs=[vmem] * len(parts),
        out_specs=vmem,
        scratch_shapes=[pltpu.VMEM((layers, group * HEAD_DIM), jnp.float32)],
        compiler_params=pltpu.CompilerParams(vmem_limit_bytes=VMEM_LIMIT),
        name="merge",
    )(*parts)


def exchange_pairs(patch_count, req_count, step, turn):
    pairs = []
    for patch in range(patch_count):
        for req in range(req_count):
            target = next(p for p in range(patch_count) if step_of(patch, p, patch_count) == step)
            pairs.append(
                (patch * req_count + req, target * req_count + (req + turn) % req_count)
            )
    return pairs


def fast_body(query, text_cache, text_len, image_rows, patch_map, image_places):
    layers = query.shape[0]
    patch_count = lax.axis_size("patch")
    req_count = lax.axis_size("req")
    band, width = image_rows.shape[1:]
    group = HEADS // KV_HEADS
    scale = 1.0 / math.sqrt(HEAD_DIM)
    slots = [[step * req_count + turn for turn in range(req_count)] for step in range(patch_count)]
    last = patch_count // 2 - 1
    late = slots[last]
    early = [k for step in range(patch_count - 1) if step != last for k in slots[step]]
    own, core = slots[-1][0], slots[-1][1:]
    pairs = [
        exchange_pairs(patch_count, req_count, k // req_count, k % req_count)
        for k in range(patch_count * req_count)
    ]
    axes = ("patch", "req")
    reach = {
        source: abs(target // req_count - source // req_count) for source, target in pairs[late[0]]
    }
    near = min(reach.values())
    outer = sorted({source // req_count for source, hops in reach.items() if hops > near})

    def stay(pair):
        return (pair[0], pair[0] // req_count * req_count + pair[1] % req_count)

    inner_pairs = {k: [p if reach[p[0]] == near else stay(p) for p in pairs[k]] for k in late}
    outer_pairs = {k: [p if reach[p[0]] > near else stay(p) for p in pairs[k]] for k in late}
    flat_query = query[:, 0]

    def send(value, some):
        return lax.ppermute(value, axes, some)

    far_queries = [
        send(flat_query, [(target, source) for source, target in inner_pairs[k]])
        for k in late
    ]
    grouped = group_rows(patch_map, image_places, image_rows, patch_count, req_count)
    arrived = {own: [grouped[own]]}
    for k in early + core:
        arrived[k] = [send(grouped[k], pairs[k])]
    for k in late:
        arrived[k] = [send(grouped[k], some) for some in (inner_pairs[k], outer_pairs[k])]
    chunk_rows = grouped[0].shape[0]
    part_rows = layers * SUBLANES
    far = seq_parts(
        functools.partial(far_kernel, scale, len(late)),
        [*far_queries, *(grouped[k] for k in late)],
        len(late) * part_rows,
        chunk_rows,
        len(late),
    )
    far = merge_far(seq_exchange(far), len(late))
    far = [lax.ppermute(part, axes, inner_pairs[k]) for part, k in zip(far, late)]
    text = text_part(query, text_cache, text_len, scale)
    here = [arrived[k][0] for k in early + core + [own]]
    sure = len(here)
    here += [arrived[k][1] for k in late]
    parts = seq_parts(
        functools.partial(here_kernel, scale, len(here), sure, outer),
        [*text, *here],
        part_rows,
        chunk_rows,
        len(here),
    )
    attended = merge([*seq_exchange(parts), *far], KV_HEADS, outer, layers, group)
    image_cache = place_rows(
        [arrived[k] for k in range(len(grouped))], outer, layers, band, width
    )
    return attended[:, None, :], image_cache[:, None]


def plain_body(query, text_cache, text_len, image_rows, patch_map, image_places):
    layers, req_dev, query_width = query.shape
    text_dev = text_cache.shape[2]
    full_width = text_cache.shape[3]
    kv_width = full_width // 2
    head_dim = HEAD_DIM
    kv_heads = KV_HEADS
    heads = HEADS
    group = heads // kv_heads
    src_rows = image_rows.shape[1]
    patch_count = lax.axis_size("patch")
    req_count = lax.axis_size("req")
    seq_count = lax.axis_size("seq")
    seq_index = lax.axis_index("seq")
    per_source = src_rows // (patch_count * req_count * req_dev)
    band_size = per_source * patch_count * req_count
    scale = 1.0 / math.sqrt(head_dim)
    order = jnp.argsort(patch_map, stable=True)
    grouped = jnp.take(image_rows, order, axis=1)
    grouped_places = jnp.take(image_places, order)
    sending = grouped.reshape(layers, patch_count * req_count, req_dev, per_source, full_width)
    arrived = lax.all_to_all(sending, ("patch", "req"), split_axis=1, concat_axis=3, tiled=True)
    place_send = grouped_places.reshape(patch_count * req_count, req_dev, per_source)
    arrived_places = lax.all_to_all(
        place_send, ("patch", "req"), split_axis=0, concat_axis=2, tiled=True
    )
    image_block = arrived.reshape(layers, req_dev, band_size, full_width)
    local_places = arrived_places.reshape(req_dev, band_size) - seq_index * band_size
    inverse = jnp.argsort(local_places, axis=1)
    image_cache = jnp.take_along_axis(image_block, inverse[None, :, :, None], axis=2)
    queries = query.reshape(layers, req_dev, kv_heads, group, head_dim)
    text_keys = text_cache[..., :kv_width].reshape(layers, req_dev, text_dev, kv_heads, head_dim)
    text_values = text_cache[..., kv_width:].reshape(layers, req_dev, text_dev, kv_heads, head_dim)
    image_keys = image_block[..., :kv_width].reshape(layers, req_dev, band_size, kv_heads, head_dim)
    image_values = image_block[..., kv_width:].reshape(
        layers, req_dev, band_size, kv_heads, head_dim
    )
    positions = seq_index * text_dev + jnp.arange(text_dev, dtype=jnp.int32)
    used = positions[None, :] < text_len[:, None]
    text_raw = (
        jnp.einsum("lrkgd,lrtkd->lrkgt", queries, text_keys, preferred_element_type=jnp.float32)
        * scale
    )
    text_scores = jnp.where(used[None, :, None, None, :], text_raw, -jnp.inf)
    image_scores = (
        jnp.einsum("lrkgd,lrtkd->lrkgt", queries, image_keys, preferred_element_type=jnp.float32)
        * scale
    )
    local_top = jnp.maximum(jnp.max(text_scores, axis=-1), jnp.max(image_scores, axis=-1))
    text_weights = jnp.exp(text_scores - local_top[..., None])
    image_weights = jnp.exp(image_scores - local_top[..., None])
    local_total = jnp.sum(text_weights, axis=-1) + jnp.sum(image_weights, axis=-1)
    text_rounded = text_weights.astype(jnp.bfloat16)
    image_rounded = image_weights.astype(jnp.bfloat16)
    local_values = jnp.einsum(
        "lrkgt,lrtkd->lrkgd", image_rounded, image_values, preferred_element_type=jnp.float32
    )
    local_values = local_values + jnp.einsum(
        "lrkgt,lrtkd->lrkgd", text_rounded, text_values, preferred_element_type=jnp.float32
    )
    width_dev = query_width // seq_count
    top = lax.pmax(local_top, "seq")
    factor = jnp.exp(local_top - top)
    scaled_total = factor * local_total
    scaled_values = factor[..., None] * local_values
    total_sum, value_sum = lax.psum((scaled_total, scaled_values), "seq")
    result = (value_sum / total_sum[..., None]).reshape(layers, req_dev, query_width)
    attended = lax.dynamic_slice_in_dim(result, seq_index * width_dev, width_dev, 2).astype(
        jnp.bfloat16
    )
    return (attended, image_cache)


def body(query, text_cache, text_len, image_rows, patch_map, image_places):
    groups = lax.axis_size("patch") * lax.axis_size("req")
    band = image_rows.shape[1]
    per = band // groups
    fast = (
        query.shape[1] == 1
        and lax.axis_size("patch") == 4
        and groups <= MOST_GROUPS
        and band == per * groups
        and band % LANES == 0
        and per % 16 == 0
        and LANES % per == 0
        and lax.axis_size("seq") == KV_HEADS
        and HEADS // KV_HEADS < SUBLANES
    )
    chosen = fast_body if fast else plain_body
    return chosen(query, text_cache, text_len, image_rows, patch_map, image_places)


def solution(mesh):
    return jax.shard_map(
        body,
        mesh=mesh,
        in_specs=(
            P(None, ("patch", "req"), None),
            P(None, ("patch", "req"), "seq", None),
            P(("patch", "req")),
            P(None, ("patch", "seq", "req"), None),
            P(("patch", "seq", "req")),
            P(("patch", "seq", "req")),
        ),
        out_specs=(P(None, ("patch", "req"), "seq"), P(None, ("patch", "req"), "seq", None)),
        check_vma=False,
    )
```

```python
import functools
import math

import jax
import jax.numpy as jnp
from jax import lax
from jax.experimental import pallas as pl
from jax.experimental.pallas import tpu as pltpu
from jax.sharding import PartitionSpec as P


HEADS = 28
KV_HEADS = 4
HEAD_DIM = 128
LANES = 128
SUBLANES = 8
MASKED = -1e30

MOST_GROUPS = 16
VMEM_LIMIT = 16 * 1024 * 1024


def step_of(source, target, count):
    turned = (source ^ target) ^ (count // 2)
    return turned ^ (turned >> 1)


def slot_choice(patch_count, req_count, owner, place):
    src_rows = owner.shape[1]
    per = src_rows // (patch_count * req_count)
    me = lax.axis_index("patch")
    mine = lax.axis_index("req")
    shape = (src_rows, src_rows)
    down = lax.broadcasted_iota(jnp.int32, shape, 0)
    across = lax.broadcasted_iota(jnp.int32, shape, 1)
    owner_row = jnp.broadcast_to(owner, shape)
    owner_col = jnp.sum(
        jnp.where(down == across, owner_row.astype(jnp.float32), 0.0), axis=1, keepdims=True
    ).astype(jnp.int32)
    ahead = (owner_row == owner_col) & (down < across)
    rank = jnp.sum(jnp.where(ahead, 1.0, 0.0), axis=0, keepdims=True).astype(jnp.int32)
    step = step_of(me, owner // req_count, patch_count)
    turn = (owner % req_count - mine + req_count) % req_count
    slot = (step * req_count + turn) * per + rank
    choose = jnp.where(down == slot, 1.0, 0.0).astype(jnp.bfloat16)
    local = place - lax.axis_index("seq") * src_rows
    line = lax.broadcasted_iota(jnp.int32, (SUBLANES, src_rows), 0)
    digits = jnp.where(line == 0, local & (LANES - 1), jnp.where(line == 1, local // LANES, 0))
    places = lax.dot_general(
        digits.astype(jnp.float32).astype(jnp.bfloat16),
        choose,
        (((1,), (1,)), ((), ())),
        preferred_element_type=jnp.float32,
    ).astype(jnp.bfloat16)
    return choose, places


def pack_slots(first, per, choose, places, layer_rows, layers, outs):
    for k, out in enumerate(outs):
        tile = (first + k) * per // LANES
        out[pl.ds(out.shape[0] - SUBLANES, SUBLANES), :] = places[
            :, tile * LANES : (tile + 1) * LANES
        ]
    taken = choose[first * per : (first + len(outs)) * per]
    for layer in range(layers):
        rows = layer_rows(layer)
        blocks = rows.shape[1] // LANES
        moved = jnp.dot(taken, rows, preferred_element_type=jnp.float32).astype(jnp.bfloat16)
        for k, out in enumerate(outs):
            for c in range(blocks):
                out[pl.ds((layer * blocks + c) * per, per), :] = moved[
                    k * per : (k + 1) * per, c * LANES : (c + 1) * LANES
                ]


def first_kernel(patch_count, req_count, map_hbm, place_hbm, rows_hbm, *refs):
    choose_ref, places_ref, rows_ref, *outs = refs[:-4]
    owner_ref, place_ref, small_sem, rows_sem = refs[-4:]
    layers, src_rows, _ = rows_hbm.shape
    small = [
        pltpu.make_async_copy(map_hbm, owner_ref, small_sem.at[0]),
        pltpu.make_async_copy(place_hbm, place_ref, small_sem.at[1]),
    ]
    loads = [
        pltpu.make_async_copy(rows_hbm.at[layer], rows_ref.at[layer], rows_sem.at[layer])
        for layer in range(layers)
    ]
    for copy in small + loads:
        copy.start()
    for copy in small:
        copy.wait()
    choose, places = slot_choice(patch_count, req_count, owner_ref[...], place_ref[...])
    choose_ref[...] = choose
    places_ref[...] = places

    def layer_rows(layer):
        loads[layer].wait()
        return rows_ref[layer]

    per = src_rows // (patch_count * req_count)
    pack_slots(0, per, choose, places, layer_rows, layers, outs)


def rest_kernel(first, per, choose_ref, places_ref, rows_ref, *outs):
    pack_slots(
        first,
        per,
        choose_ref[...],
        places_ref[...],
        lambda layer: rows_ref[layer],
        rows_ref.shape[0],
        outs,
    )


def in_hbm(array):
    return pltpu.with_memory_space_constraint(array, pltpu.HBM)


def group_rows(patch_map, image_places, image_rows, patch_count, req_count):
    layers, src_rows, width = image_rows.shape
    groups = patch_count * req_count
    per = src_rows // groups
    chunk = jax.ShapeDtypeStruct((layers * per * width // LANES + SUBLANES, LANES), jnp.bfloat16)
    hbm = pl.BlockSpec(memory_space=pltpu.HBM)
    vmem = pl.BlockSpec(memory_space=pltpu.VMEM)

    def cost(count):
        return pl.CostEstimate(
            flops=2 * layers * src_rows * per * count * width,
            bytes_accessed=2 * layers * (src_rows + per * count) * width,
            transcendentals=0,
        )

    first_call = pl.pallas_call(
        functools.partial(first_kernel, patch_count, req_count),
        out_shape=[
            jax.ShapeDtypeStruct((src_rows, src_rows), jnp.bfloat16),
            jax.ShapeDtypeStruct((SUBLANES, src_rows), jnp.bfloat16),
            jax.ShapeDtypeStruct(image_rows.shape, jnp.bfloat16),
        ]
        + [chunk] * req_count,
        in_specs=[hbm] * 3,
        out_specs=[vmem] * (3 + req_count),
        scratch_shapes=[
            pltpu.VMEM((1, src_rows), jnp.int32),
            pltpu.VMEM((1, src_rows), jnp.int32),
            pltpu.SemaphoreType.DMA((2,)),
            pltpu.SemaphoreType.DMA((layers,)),
        ],
        cost_estimate=cost(req_count),
        compiler_params=pltpu.CompilerParams(vmem_limit_bytes=VMEM_LIMIT),
        name="group_first",
    )
    choose, places, rows, *first = first_call(
        in_hbm(patch_map.reshape(1, src_rows)),
        in_hbm(image_places.reshape(1, src_rows)),
        in_hbm(image_rows),
    )
    rest_call = pl.pallas_call(
        functools.partial(rest_kernel, req_count, per),
        out_shape=[chunk] * (groups - req_count),
        in_specs=[vmem] * 3,
        out_specs=[vmem] * (groups - req_count),
        cost_estimate=cost(groups - req_count),
        compiler_params=pltpu.CompilerParams(vmem_limit_bytes=VMEM_LIMIT),
        name="group_rest",
    )
    rest = rest_call(choose, places, rows)
    return [*first, *rest]


def heads_of(line, group):
    row = lax.broadcasted_iota(jnp.int32, (SUBLANES, HEAD_DIM), 0)
    tiles = []
    for g in range(KV_HEADS):
        tile = jnp.zeros((SUBLANES, HEAD_DIM), jnp.float32)
        for i in range(group):
            h = g * group + i
            tile = jnp.where(row == i, line[:, h * HEAD_DIM : (h + 1) * HEAD_DIM], tile)
        tiles.append(tile)
    return jnp.concatenate(tiles, axis=0).astype(jnp.bfloat16)


def attend(queries, keys, values, used, scale):
    scores = jnp.concatenate(
        [
            lax.dot_general(
                queries[g * SUBLANES : (g + 1) * SUBLANES],
                keys[g],
                (((1,), (1,)), ((), ())),
                preferred_element_type=jnp.float32,
            )
            for g in range(KV_HEADS)
        ],
        axis=0,
    )
    scores = scores * scale
    if used is not None:
        scores = jnp.where(used, scores, MASKED)
    top = jnp.max(scores, axis=1, keepdims=True)
    weights = jnp.exp(scores - top)
    if used is not None:
        weights = jnp.where(used, weights, 0.0)
    total = jnp.sum(weights, axis=1, keepdims=True)
    rounded = weights.astype(jnp.bfloat16)
    summed = jnp.concatenate(
        [
            jnp.dot(
                rounded[g * SUBLANES : (g + 1) * SUBLANES],
                values[g],
                preferred_element_type=jnp.float32,
            )
            for g in range(KV_HEADS)
        ],
        axis=0,
    )
    return top, total, summed


def text_kernel(scale, len_ref, query_ref, text_ref, q_ref, top_ref, total_ref, sum_ref):
    text_dev, width = text_ref.shape
    group = query_ref.shape[1] // HEAD_DIM // KV_HEADS
    queries = heads_of(query_ref[...].astype(jnp.float32), group)
    q_ref[...] = queries
    rows = KV_HEADS * SUBLANES
    positions = lax.axis_index("seq") * text_dev + lax.broadcasted_iota(
        jnp.int32, (rows, text_dev), 1
    )
    keys = [text_ref[:, g * HEAD_DIM : (g + 1) * HEAD_DIM] for g in range(KV_HEADS)]
    values = [
        text_ref[:, width // 2 + g * HEAD_DIM : width // 2 + (g + 1) * HEAD_DIM]
        for g in range(KV_HEADS)
    ]
    top, total, summed = attend(queries, keys, values, positions < len_ref[0], scale)
    top_ref[...] = jnp.broadcast_to(top, (rows, LANES))
    total_ref[...] = jnp.broadcast_to(total, (rows, LANES))
    sum_ref[...] = summed


def text_part(query, text_cache, text_len, scale):
    layers, _, query_width = query.shape
    text_dev, width = text_cache.shape[2:]
    rows = KV_HEADS * SUBLANES
    part = pl.BlockSpec((None, rows, LANES), lambda layer, _: (layer, 0, 0))
    return pl.pallas_call(
        functools.partial(text_kernel, scale),
        out_shape=[
            jax.ShapeDtypeStruct((layers, rows, HEAD_DIM), jnp.bfloat16),
            jax.ShapeDtypeStruct((layers, rows, LANES), jnp.float32),
            jax.ShapeDtypeStruct((layers, rows, LANES), jnp.float32),
            jax.ShapeDtypeStruct((layers, rows, HEAD_DIM), jnp.float32),
        ],
        grid_spec=pltpu.PrefetchScalarGridSpec(
            num_scalar_prefetch=1,
            grid=(layers,),
            in_specs=[
                pl.BlockSpec((None, 1, query_width), lambda layer, _: (layer, 0, 0)),
                pl.BlockSpec((None, None, text_dev, width), lambda layer, _: (layer, 0, 0, 0)),
            ],
            out_specs=[part] * 4,
        ),
        cost_estimate=pl.CostEstimate(
            flops=8 * layers * SUBLANES * LANES * text_dev * width,
            bytes_accessed=2 * layers * text_dev * width,
            transcendentals=layers * rows * text_dev,
        ),
        compiler_params=pltpu.CompilerParams(vmem_limit_bytes=VMEM_LIMIT),
        name="text_part",
    )(text_len, query, in_hbm(text_cache))


def image_layer(scale, layer, chunks, used, q_ref, top, total, summed):
    layers = q_ref.shape[0]
    blocks = 2 * KV_HEADS
    per = (chunks[0].shape[0] - SUBLANES) // layers // blocks

    def column(c):
        span = pl.ds((layer * blocks + c) * per, per)
        return jnp.concatenate([chunk[span, :] for chunk in chunks], axis=0)

    keys = [column(g) for g in range(KV_HEADS)]
    values = [column(KV_HEADS + g) for g in range(KV_HEADS)]
    new_top, new_total, new_summed = attend(q_ref[layer], keys, values, used, scale)
    both = jnp.maximum(top, new_top)
    old_factor = jnp.exp(top - both)
    new_factor = jnp.exp(new_top - both)
    total = old_factor * total + new_factor * new_total
    summed = old_factor * summed + new_factor * new_summed
    return both, total, summed


def pack_part(top, total, summed):
    row = lax.broadcasted_iota(jnp.int32, (SUBLANES, LANES), 0)
    lane = lax.broadcasted_iota(jnp.int32, (SUBLANES, LANES), 1)
    stats = jnp.where(lane == row, top, jnp.where(lane == row + LANES // 2, total, 0.0))
    stats = jnp.sum(stats, axis=0, keepdims=True)
    return jnp.where(row == SUBLANES - 1, stats, summed)


def unpack_part(tile):
    row = lax.broadcasted_iota(jnp.int32, (SUBLANES, LANES), 0)
    lane = lax.broadcasted_iota(jnp.int32, (SUBLANES, LANES), 1)
    stats = jnp.broadcast_to(tile[SUBLANES - 1 :, :], (SUBLANES, LANES))
    top = jnp.sum(jnp.where(lane == row, stats, 0.0), axis=1, keepdims=True)
    total = jnp.sum(jnp.where(lane == row + LANES // 2, stats, 0.0), axis=1, keepdims=True)
    return top, total, tile


def merge_tiles(tiles, used=None):
    parts = [unpack_part(tile) for tile in tiles]
    for n, part in enumerate(parts):
        if used is not None and used[n] is not None:
            parts[n] = [jnp.where(used[n], a, b) for a, b in zip(part, (MASKED, 0.0, 0.0))]
    top = functools.reduce(jnp.maximum, [part[0] for part in parts])
    factors = [jnp.exp(part[0] - top) for part in parts]
    total = sum(factor * part[1] for factor, part in zip(factors, parts))
    summed = sum(factor * part[2] for factor, part in zip(factors, parts))
    return top, total, summed


def here_kernel(scale, groups, sure, outer, q_ref, top_in, total_in, sum_in, *refs):
    chunks, outs, packed = refs[:groups], refs[groups:-1], refs[-1]
    layers, rows = q_ref.shape[:2]
    per = (chunks[0].shape[0] - SUBLANES) // layers // (2 * KV_HEADS)
    limit = jnp.where(is_outer(outer), groups, sure) * per
    used = lax.broadcasted_iota(jnp.int32, (rows, groups * per), 1) < limit
    for layer in range(q_ref.shape[0]):
        top, total, summed = image_layer(
            scale,
            layer,
            chunks,
            used,
            q_ref,
            top_in[layer][:, :1],
            total_in[layer][:, :1],
            sum_in[layer],
        )
        for g in range(KV_HEADS):
            span = slice(g * SUBLANES, (g + 1) * SUBLANES)
            packed[g, pl.ds(layer * SUBLANES, SUBLANES), :] = pack_part(
                top[span], total[span], summed[span]
            )
    me = lax.axis_index("seq")
    for k in range(KV_HEADS):
        outs[k][...] = packed[me ^ k]


def far_kernel(scale, count, *refs):
    queries, chunks = refs[:count], refs[count : 2 * count]
    outs, packed = refs[2 * count : -1], refs[-1]
    layers = queries[0].shape[0]
    blocks = 2 * KV_HEADS
    group = queries[0].shape[1] // HEAD_DIM // KV_HEADS
    for n in range(count):
        chunk = chunks[n]
        per = (chunk.shape[0] - SUBLANES) // layers // blocks
        for layer in range(layers):
            columns = [
                chunk[pl.ds((layer * blocks + c) * per, per), :] for c in range(blocks)
            ]
            line = queries[n][pl.ds(layer, 1), :].astype(jnp.float32)
            top, total, summed = attend(
                heads_of(line, group), columns[:KV_HEADS], columns[KV_HEADS:], None, scale
            )
            for g in range(KV_HEADS):
                span = slice(g * SUBLANES, (g + 1) * SUBLANES)
                packed[g, pl.ds((n * layers + layer) * SUBLANES, SUBLANES), :] = pack_part(
                    top[span], total[span], summed[span]
                )
    me = lax.axis_index("seq")
    for k in range(KV_HEADS):
        outs[k][...] = packed[me ^ k]


def seq_parts(kernel, operands, part_rows, chunk_rows, groups):
    shape = (part_rows, LANES)
    vmem = pl.BlockSpec(memory_space=pltpu.VMEM)
    return pl.pallas_call(
        kernel,
        out_shape=[jax.ShapeDtypeStruct(shape, jnp.float32)] * KV_HEADS,
        in_specs=[vmem] * len(operands),
        out_specs=[vmem] * KV_HEADS,
        scratch_shapes=[pltpu.VMEM((KV_HEADS,) + shape, jnp.float32)],
        cost_estimate=pl.CostEstimate(
            flops=8 * SUBLANES * chunk_rows * LANES * groups,
            bytes_accessed=2 * chunk_rows * LANES * groups,
            transcendentals=SUBLANES * chunk_rows * groups,
        ),
        compiler_params=pltpu.CompilerParams(vmem_limit_bytes=VMEM_LIMIT),
    )(*operands)


def seq_exchange(outs):
    arrived = [
        lax.ppermute(out, "seq", [(s, s ^ k) for s in range(KV_HEADS)])
        for k, out in enumerate(outs)
        if k
    ]
    return [outs[0], *arrived]


def merge_far_kernel(count, *refs):
    parts, outs = refs[:-count], refs[-count:]
    rows = parts[0].shape[0] // count
    for n, out in enumerate(outs):
        for at in range(0, rows, SUBLANES):
            tiles = [part[pl.ds(n * rows + at, SUBLANES), :] for part in parts]
            out[pl.ds(at, SUBLANES), :] = pack_part(*merge_tiles(tiles))


def merge_far(parts, count):
    rows = parts[0].shape[0] // count
    vmem = pl.BlockSpec(memory_space=pltpu.VMEM)
    return pl.pallas_call(
        functools.partial(merge_far_kernel, count),
        out_shape=[jax.ShapeDtypeStruct((rows, LANES), jnp.float32)] * count,
        in_specs=[vmem] * len(parts),
        out_specs=[vmem] * count,
        compiler_params=pltpu.CompilerParams(vmem_limit_bytes=VMEM_LIMIT),
        name="merge_far",
    )(*parts)


def is_outer(outer):
    patch = lax.axis_index("patch")
    return functools.reduce(jnp.logical_or, [patch == z for z in outer])


def place_kernel(owners, outer, *refs):
    out_hbm, out_ref, sems = refs[-3:]
    groups = len(owners)
    outside = is_outer(outer)

    def rows_of(k, span):
        first, *others = [refs[n][span, :] for n in owners[k]]
        return jnp.where(outside, others[0], first) if others else first

    layers, band, width = out_ref.shape
    blocks = width // LANES
    per = band // groups
    stores = [
        pltpu.make_async_copy(out_ref.at[layer], out_hbm.at[layer], sems.at[layer])
        for layer in range(layers)
    ]
    base = layers * blocks * per
    lane = lax.broadcasted_iota(jnp.int32, (SUBLANES, LANES), 1)
    tiles = []
    for tile in range(band // LANES):
        row = jnp.zeros((SUBLANES, LANES), jnp.float32)
        for k in range(groups):
            if k * per // LANES == tile:
                extra = rows_of(k, pl.ds(base, SUBLANES)).astype(jnp.float32)
                inside = (lane >= k * per % LANES) & (lane < k * per % LANES + per)
                row = jnp.where(inside, extra, row)
        tiles.append(row)
    digits = jnp.concatenate(tiles, axis=1).astype(jnp.int32)
    places = digits[0:1] + digits[1:2] * LANES
    down = lax.broadcasted_iota(jnp.int32, (band, band), 0)
    choose = jnp.where(down == places, 1.0, 0.0).astype(jnp.bfloat16)
    for layer in range(layers):
        for c in range(0, blocks, 2):
            spans = [pl.ds((layer * blocks + c + n) * per, per) for n in range(2)]
            columns = [
                jnp.concatenate([rows_of(k, span) for k in range(groups)], axis=0)
                for span in spans
            ]
            out_ref[layer, :, c * LANES : (c + 2) * LANES] = jnp.dot(
                choose, jnp.concatenate(columns, axis=1), preferred_element_type=jnp.float32
            ).astype(jnp.bfloat16)
        stores[layer].start()
    for store in stores:
        store.wait()


def place_rows(slots, outer, layers, band, width):
    operands = [chunk for slot in slots for chunk in slot]
    count = iter(range(len(operands)))
    owners = [[next(count) for _ in slot] for slot in slots]
    vmem = pl.BlockSpec(memory_space=pltpu.VMEM)
    return pl.pallas_call(
        functools.partial(place_kernel, owners, outer),
        out_shape=jax.ShapeDtypeStruct((layers, band, width), jnp.bfloat16),
        in_specs=[vmem] * len(operands),
        out_specs=pl.BlockSpec(memory_space=pltpu.HBM),
        scratch_shapes=[
            pltpu.VMEM((layers, band, width), jnp.bfloat16),
            pltpu.SemaphoreType.DMA((layers,)),
        ],
        cost_estimate=pl.CostEstimate(
            flops=2 * layers * band * band * width,
            bytes_accessed=4 * layers * band * width,
            transcendentals=0,
        ),
        compiler_params=pltpu.CompilerParams(vmem_limit_bytes=VMEM_LIMIT),
        name="place_rows",
    )(*operands)


def merge_kernel(group, sure, outer, *refs):
    parts, out_ref, lines = refs[:-2], refs[-2], refs[-1]
    inside = jnp.logical_not(is_outer(outer))
    used = [None if n < sure else inside for n in range(len(parts))]
    for layer in range(out_ref.shape[0]):
        tiles = [part[pl.ds(layer * SUBLANES, SUBLANES), :] for part in parts]
        _, total, summed = merge_tiles(tiles, used)
        result = summed / total
        for i in range(group):
            lines[pl.ds(layer, 1), i * HEAD_DIM : (i + 1) * HEAD_DIM] = result[i : i + 1]
    out_ref[...] = lines[...].astype(jnp.bfloat16)


def merge(parts, sure, outer, layers, group):
    vmem = pl.BlockSpec(memory_space=pltpu.VMEM)
    return pl.pallas_call(
        functools.partial(merge_kernel, group, sure, outer),
        out_shape=jax.ShapeDtypeStruct((layers, group * HEAD_DIM), jnp.bfloat16),
        in_specs=[vmem] * len(parts),
        out_specs=vmem,
        scratch_shapes=[pltpu.VMEM((layers, group * HEAD_DIM), jnp.float32)],
        compiler_params=pltpu.CompilerParams(vmem_limit_bytes=VMEM_LIMIT),
        name="merge",
    )(*parts)


def exchange_pairs(patch_count, req_count, step, turn):
    pairs = []
    for patch in range(patch_count):
        for req in range(req_count):
            target = next(p for p in range(patch_count) if step_of(patch, p, patch_count) == step)
            pairs.append(
                (patch * req_count + req, target * req_count + (req + turn) % req_count)
            )
    return pairs


def fast_body(query, text_cache, text_len, image_rows, patch_map, image_places):
    layers = query.shape[0]
    patch_count = lax.axis_size("patch")
    req_count = lax.axis_size("req")
    band, width = image_rows.shape[1:]
    group = HEADS // KV_HEADS
    scale = 1.0 / math.sqrt(HEAD_DIM)
    slots = [[step * req_count + turn for turn in range(req_count)] for step in range(patch_count)]
    last = patch_count // 2 - 1
    late = slots[last]
    early = [k for step in range(patch_count - 1) if step != last for k in slots[step]]
    own, core = slots[-1][0], slots[-1][1:]
    pairs = [
        exchange_pairs(patch_count, req_count, k // req_count, k % req_count)
        for k in range(patch_count * req_count)
    ]
    axes = ("patch", "req")
    reach = {
        source: abs(target // req_count - source // req_count) for source, target in pairs[late[0]]
    }
    near = min(reach.values())
    outer = sorted({source // req_count for source, hops in reach.items() if hops > near})

    def stay(pair):
        return (pair[0], pair[0] // req_count * req_count + pair[1] % req_count)

    inner_pairs = {k: [p if reach[p[0]] == near else stay(p) for p in pairs[k]] for k in late}
    outer_pairs = {k: [p if reach[p[0]] > near else stay(p) for p in pairs[k]] for k in late}
    flat_query = query[:, 0]

    def send(value, some):
        return lax.ppermute(value, axes, some)

    far_queries = [
        send(flat_query, [(target, source) for source, target in inner_pairs[k]])
        for k in late
    ]
    grouped = group_rows(patch_map, image_places, image_rows, patch_count, req_count)
    arrived = {own: [grouped[own]]}
    for k in early + core:
        arrived[k] = [send(grouped[k], pairs[k])]
    for k in late:
        arrived[k] = [send(grouped[k], some) for some in (inner_pairs[k], outer_pairs[k])]
    chunk_rows = grouped[0].shape[0]
    part_rows = layers * SUBLANES
    far = seq_parts(
        functools.partial(far_kernel, scale, len(late)),
        [*far_queries, *(grouped[k] for k in late)],
        len(late) * part_rows,
        chunk_rows,
        len(late),
    )
    far = merge_far(seq_exchange(far), len(late))
    far = [send(far[n], inner_pairs[k]) for n, k in enumerate(late)]
    text = text_part(query, text_cache, text_len, scale)
    here = [arrived[k][0] for k in early + core + [own]]
    sure = len(here)
    here += [arrived[k][1] for k in late]
    parts = seq_parts(
        functools.partial(here_kernel, scale, len(here), sure, outer),
        [*text, *here],
        part_rows,
        chunk_rows,
        len(here),
    )
    attended = merge([*seq_exchange(parts), *far], KV_HEADS, outer, layers, group)
    image_cache = place_rows(
        [arrived[k] for k in range(len(grouped))], outer, layers, band, width
    )
    return attended[:, None, :], image_cache[:, None]


def plain_body(query, text_cache, text_len, image_rows, patch_map, image_places):
    layers, req_dev, query_width = query.shape
    text_dev = text_cache.shape[2]
    full_width = text_cache.shape[3]
    kv_width = full_width // 2
    head_dim = HEAD_DIM
    kv_heads = KV_HEADS
    heads = HEADS
    group = heads // kv_heads
    src_rows = image_rows.shape[1]
    patch_count = lax.axis_size("patch")
    req_count = lax.axis_size("req")
    seq_count = lax.axis_size("seq")
    seq_index = lax.axis_index("seq")
    per_source = src_rows // (patch_count * req_count * req_dev)
    band_size = per_source * patch_count * req_count
    scale = 1.0 / math.sqrt(head_dim)
    order = jnp.argsort(patch_map, stable=True)
    grouped = jnp.take(image_rows, order, axis=1)
    grouped_places = jnp.take(image_places, order)
    sending = grouped.reshape(layers, patch_count * req_count, req_dev, per_source, full_width)
    arrived = lax.all_to_all(sending, ("patch", "req"), split_axis=1, concat_axis=3, tiled=True)
    place_send = grouped_places.reshape(patch_count * req_count, req_dev, per_source)
    arrived_places = lax.all_to_all(
        place_send, ("patch", "req"), split_axis=0, concat_axis=2, tiled=True
    )
    image_block = arrived.reshape(layers, req_dev, band_size, full_width)
    local_places = arrived_places.reshape(req_dev, band_size) - seq_index * band_size
    inverse = jnp.argsort(local_places, axis=1)
    image_cache = jnp.take_along_axis(image_block, inverse[None, :, :, None], axis=2)
    queries = query.reshape(layers, req_dev, kv_heads, group, head_dim)
    text_keys = text_cache[..., :kv_width].reshape(layers, req_dev, text_dev, kv_heads, head_dim)
    text_values = text_cache[..., kv_width:].reshape(layers, req_dev, text_dev, kv_heads, head_dim)
    image_keys = image_block[..., :kv_width].reshape(layers, req_dev, band_size, kv_heads, head_dim)
    image_values = image_block[..., kv_width:].reshape(
        layers, req_dev, band_size, kv_heads, head_dim
    )
    positions = seq_index * text_dev + jnp.arange(text_dev, dtype=jnp.int32)
    used = positions[None, :] < text_len[:, None]
    text_raw = (
        jnp.einsum("lrkgd,lrtkd->lrkgt", queries, text_keys, preferred_element_type=jnp.float32)
        * scale
    )
    text_scores = jnp.where(used[None, :, None, None, :], text_raw, -jnp.inf)
    image_scores = (
        jnp.einsum("lrkgd,lrtkd->lrkgt", queries, image_keys, preferred_element_type=jnp.float32)
        * scale
    )
    local_top = jnp.maximum(jnp.max(text_scores, axis=-1), jnp.max(image_scores, axis=-1))
    text_weights = jnp.exp(text_scores - local_top[..., None])
    image_weights = jnp.exp(image_scores - local_top[..., None])
    local_total = jnp.sum(text_weights, axis=-1) + jnp.sum(image_weights, axis=-1)
    text_rounded = text_weights.astype(jnp.bfloat16)
    image_rounded = image_weights.astype(jnp.bfloat16)
    local_values = jnp.einsum(
        "lrkgt,lrtkd->lrkgd", image_rounded, image_values, preferred_element_type=jnp.float32
    )
    local_values = local_values + jnp.einsum(
        "lrkgt,lrtkd->lrkgd", text_rounded, text_values, preferred_element_type=jnp.float32
    )
    width_dev = query_width // seq_count
    top = lax.pmax(local_top, "seq")
    factor = jnp.exp(local_top - top)
    scaled_total = factor * local_total
    scaled_values = factor[..., None] * local_values
    total_sum, value_sum = lax.psum((scaled_total, scaled_values), "seq")
    result = (value_sum / total_sum[..., None]).reshape(layers, req_dev, query_width)
    attended = lax.dynamic_slice_in_dim(result, seq_index * width_dev, width_dev, 2).astype(
        jnp.bfloat16
    )
    return (attended, image_cache)


def body(query, text_cache, text_len, image_rows, patch_map, image_places):
    groups = lax.axis_size("patch") * lax.axis_size("req")
    band = image_rows.shape[1]
    per = band // groups
    fast = (
        query.shape[1] == 1
        and lax.axis_size("patch") == 4
        and groups <= MOST_GROUPS
        and band == per * groups
        and band % LANES == 0
        and per % 16 == 0
        and LANES % per == 0
        and lax.axis_size("seq") == KV_HEADS
        and HEADS // KV_HEADS < SUBLANES
    )
    chosen = fast_body if fast else plain_body
    return chosen(query, text_cache, text_len, image_rows, patch_map, image_places)


def solution(mesh):
    return jax.shard_map(
        body,
        mesh=mesh,
        in_specs=(
            P(None, ("patch", "req"), None),
            P(None, ("patch", "req"), "seq", None),
            P(("patch", "req")),
            P(None, ("patch", "seq", "req"), None),
            P(("patch", "seq", "req")),
            P(("patch", "seq", "req")),
        ),
        out_specs=(P(None, ("patch", "req"), "seq"), P(None, ("patch", "req"), "seq", None)),
        check_vma=False,
    )
```

```python
import functools
import math

import jax
import jax.numpy as jnp
from jax import lax
from jax.experimental import pallas as pl
from jax.experimental.pallas import tpu as pltpu
from jax.sharding import PartitionSpec as P


HEADS = 28
KV_HEADS = 4
HEAD_DIM = 128
LANES = 128
SUBLANES = 8
MASKED = -1e30

MOST_GROUPS = 16
LAST_CHUNKS = 1
VMEM_LIMIT = 16 * 1024 * 1024


def step_of(source, target, count):
    turned = (source ^ target) ^ (count // 2)
    return turned ^ (turned >> 1)


def slot_choice(patch_count, req_count, owner, place):
    src_rows = owner.shape[1]
    per = src_rows // (patch_count * req_count)
    me = lax.axis_index("patch")
    mine = lax.axis_index("req")
    shape = (src_rows, src_rows)
    down = lax.broadcasted_iota(jnp.int32, shape, 0)
    across = lax.broadcasted_iota(jnp.int32, shape, 1)
    owner_row = jnp.broadcast_to(owner, shape)
    owner_col = jnp.sum(
        jnp.where(down == across, owner_row.astype(jnp.float32), 0.0), axis=1, keepdims=True
    ).astype(jnp.int32)
    ahead = (owner_row == owner_col) & (down < across)
    rank = jnp.sum(jnp.where(ahead, 1.0, 0.0), axis=0, keepdims=True).astype(jnp.int32)
    step = step_of(me, owner // req_count, patch_count)
    turn = (owner % req_count - mine + req_count) % req_count
    slot = (step * req_count + turn) * per + rank
    choose = jnp.where(down == slot, 1.0, 0.0).astype(jnp.bfloat16)
    local = place - lax.axis_index("seq") * src_rows
    line = lax.broadcasted_iota(jnp.int32, (SUBLANES, src_rows), 0)
    digits = jnp.where(line == 0, local & (LANES - 1), jnp.where(line == 1, local // LANES, 0))
    places = lax.dot_general(
        digits.astype(jnp.float32).astype(jnp.bfloat16),
        choose,
        (((1,), (1,)), ((), ())),
        preferred_element_type=jnp.float32,
    ).astype(jnp.bfloat16)
    return choose, places


def pack_slots(first, per, choose, places, layer_rows, layers, outs):
    for k, out in enumerate(outs):
        tile = (first + k) * per // LANES
        out[pl.ds(out.shape[0] - SUBLANES, SUBLANES), :] = places[
            :, tile * LANES : (tile + 1) * LANES
        ]
    taken = choose[first * per : (first + len(outs)) * per]
    for layer in range(layers):
        rows = layer_rows(layer)
        blocks = rows.shape[1] // LANES
        moved = jnp.dot(taken, rows, preferred_element_type=jnp.float32).astype(jnp.bfloat16)
        for k, out in enumerate(outs):
            for c in range(blocks):
                out[pl.ds((layer * blocks + c) * per, per), :] = moved[
                    k * per : (k + 1) * per, c * LANES : (c + 1) * LANES
                ]


def first_kernel(patch_count, req_count, map_hbm, place_hbm, rows_hbm, *refs):
    choose_ref, places_ref, rows_ref, *outs = refs[:-4]
    owner_ref, place_ref, small_sem, rows_sem = refs[-4:]
    layers, src_rows, _ = rows_hbm.shape
    small = [
        pltpu.make_async_copy(map_hbm, owner_ref, small_sem.at[0]),
        pltpu.make_async_copy(place_hbm, place_ref, small_sem.at[1]),
    ]
    loads = [
        pltpu.make_async_copy(rows_hbm.at[layer], rows_ref.at[layer], rows_sem.at[layer])
        for layer in range(layers)
    ]
    for copy in small + loads:
        copy.start()
    for copy in small:
        copy.wait()
    choose, places = slot_choice(patch_count, req_count, owner_ref[...], place_ref[...])
    choose_ref[...] = choose
    places_ref[...] = places

    def layer_rows(layer):
        loads[layer].wait()
        return rows_ref[layer]

    per = src_rows // (patch_count * req_count)
    pack_slots(0, per, choose, places, layer_rows, layers, outs)


def rest_kernel(first, per, choose_ref, places_ref, rows_ref, *outs):
    pack_slots(
        first,
        per,
        choose_ref[...],
        places_ref[...],
        lambda layer: rows_ref[layer],
        rows_ref.shape[0],
        outs,
    )


def in_hbm(array):
    return pltpu.with_memory_space_constraint(array, pltpu.HBM)


def group_rows(patch_map, image_places, image_rows, patch_count, req_count):
    layers, src_rows, width = image_rows.shape
    groups = patch_count * req_count
    per = src_rows // groups
    chunk = jax.ShapeDtypeStruct((layers * per * width // LANES + SUBLANES, LANES), jnp.bfloat16)
    hbm = pl.BlockSpec(memory_space=pltpu.HBM)
    vmem = pl.BlockSpec(memory_space=pltpu.VMEM)

    def cost(count):
        return pl.CostEstimate(
            flops=2 * layers * src_rows * per * count * width,
            bytes_accessed=2 * layers * (src_rows + per * count) * width,
            transcendentals=0,
        )

    first_call = pl.pallas_call(
        functools.partial(first_kernel, patch_count, req_count),
        out_shape=[
            jax.ShapeDtypeStruct((src_rows, src_rows), jnp.bfloat16),
            jax.ShapeDtypeStruct((SUBLANES, src_rows), jnp.bfloat16),
            jax.ShapeDtypeStruct(image_rows.shape, jnp.bfloat16),
        ]
        + [chunk] * req_count,
        in_specs=[hbm] * 3,
        out_specs=[vmem] * (3 + req_count),
        scratch_shapes=[
            pltpu.VMEM((1, src_rows), jnp.int32),
            pltpu.VMEM((1, src_rows), jnp.int32),
            pltpu.SemaphoreType.DMA((2,)),
            pltpu.SemaphoreType.DMA((layers,)),
        ],
        cost_estimate=cost(req_count),
        compiler_params=pltpu.CompilerParams(vmem_limit_bytes=VMEM_LIMIT),
        name="group_first",
    )
    choose, places, rows, *first = first_call(
        in_hbm(patch_map.reshape(1, src_rows)),
        in_hbm(image_places.reshape(1, src_rows)),
        in_hbm(image_rows),
    )
    rest_call = pl.pallas_call(
        functools.partial(rest_kernel, req_count, per),
        out_shape=[chunk] * (groups - req_count),
        in_specs=[vmem] * 3,
        out_specs=[vmem] * (groups - req_count),
        cost_estimate=cost(groups - req_count),
        compiler_params=pltpu.CompilerParams(vmem_limit_bytes=VMEM_LIMIT),
        name="group_rest",
    )
    rest = rest_call(choose, places, rows)
    return [*first, *rest]


def heads_of(line, group):
    row = lax.broadcasted_iota(jnp.int32, (SUBLANES, HEAD_DIM), 0)
    tiles = []
    for g in range(KV_HEADS):
        tile = jnp.zeros((SUBLANES, HEAD_DIM), jnp.float32)
        for i in range(group):
            h = g * group + i
            tile = jnp.where(row == i, line[:, h * HEAD_DIM : (h + 1) * HEAD_DIM], tile)
        tiles.append(tile)
    return jnp.concatenate(tiles, axis=0).astype(jnp.bfloat16)


def attend(queries, keys, values, used, scale):
    def tile(rows, n):
        return rows[n * SUBLANES : (n + 1) * SUBLANES]

    scores = jnp.concatenate(
        [
            lax.dot_general(
                tile(queries, n), key, (((1,), (1,)), ((), ())), preferred_element_type=jnp.float32
            )
            for n, key in enumerate(keys)
        ],
        axis=0,
    )
    scores = scores * scale
    if used is not None:
        scores = jnp.where(used, scores, MASKED)
    top = jnp.max(scores, axis=1, keepdims=True)
    weights = jnp.exp(scores - top)
    if used is not None:
        weights = jnp.where(used, weights, 0.0)
    total = jnp.sum(weights, axis=1, keepdims=True)
    rounded = weights.astype(jnp.bfloat16)
    summed = jnp.concatenate(
        [
            jnp.dot(tile(rounded, n), value, preferred_element_type=jnp.float32)
            for n, value in enumerate(values)
        ],
        axis=0,
    )
    return top, total, summed


def text_kernel(scale, len_ref, query_ref, text_ref, q_ref, top_ref, total_ref, sum_ref):
    text_dev, width = text_ref.shape
    group = query_ref.shape[1] // HEAD_DIM // KV_HEADS
    queries = heads_of(query_ref[...].astype(jnp.float32), group)
    q_ref[...] = queries
    rows = KV_HEADS * SUBLANES
    positions = lax.axis_index("seq") * text_dev + lax.broadcasted_iota(
        jnp.int32, (rows, text_dev), 1
    )
    keys = [text_ref[:, g * HEAD_DIM : (g + 1) * HEAD_DIM] for g in range(KV_HEADS)]
    values = [
        text_ref[:, width // 2 + g * HEAD_DIM : width // 2 + (g + 1) * HEAD_DIM]
        for g in range(KV_HEADS)
    ]
    top, total, summed = attend(queries, keys, values, positions < len_ref[0], scale)
    top_ref[...] = jnp.broadcast_to(top, (rows, LANES))
    total_ref[...] = jnp.broadcast_to(total, (rows, LANES))
    sum_ref[...] = summed


def text_part(query, text_cache, text_len, scale):
    layers, _, query_width = query.shape
    text_dev, width = text_cache.shape[2:]
    rows = KV_HEADS * SUBLANES
    part = pl.BlockSpec((None, rows, LANES), lambda layer, _: (layer, 0, 0))
    return pl.pallas_call(
        functools.partial(text_kernel, scale),
        out_shape=[
            jax.ShapeDtypeStruct((layers, rows, HEAD_DIM), jnp.bfloat16),
            jax.ShapeDtypeStruct((layers, rows, LANES), jnp.float32),
            jax.ShapeDtypeStruct((layers, rows, LANES), jnp.float32),
            jax.ShapeDtypeStruct((layers, rows, HEAD_DIM), jnp.float32),
        ],
        grid_spec=pltpu.PrefetchScalarGridSpec(
            num_scalar_prefetch=1,
            grid=(layers,),
            in_specs=[
                pl.BlockSpec((None, 1, query_width), lambda layer, _: (layer, 0, 0)),
                pl.BlockSpec((None, None, text_dev, width), lambda layer, _: (layer, 0, 0, 0)),
            ],
            out_specs=[part] * 4,
        ),
        cost_estimate=pl.CostEstimate(
            flops=8 * layers * SUBLANES * LANES * text_dev * width,
            bytes_accessed=2 * layers * text_dev * width,
            transcendentals=layers * rows * text_dev,
        ),
        compiler_params=pltpu.CompilerParams(vmem_limit_bytes=VMEM_LIMIT),
        name="text_part",
    )(text_len, query, in_hbm(text_cache))


def image_columns(chunks, layers):
    blocks = 2 * KV_HEADS
    per = (chunks[0].shape[0] - SUBLANES) // layers // blocks

    def column(layer, c):
        span = pl.ds((layer * blocks + c) * per, per)
        return jnp.concatenate([chunk[span, :] for chunk in chunks], axis=0)

    keys = [column(layer, g) for layer in range(layers) for g in range(KV_HEADS)]
    values = [column(layer, KV_HEADS + g) for layer in range(layers) for g in range(KV_HEADS)]
    return keys, values


def join_image(scale, chunks, used, q_ref, top_in, total_in, sum_in):
    layers, rows, _ = q_ref.shape
    lines = layers * rows
    keys, values = image_columns(chunks, layers)
    queries = q_ref[...].reshape(lines, HEAD_DIM)
    new_top, new_total, new_summed = attend(queries, keys, values, used, scale)
    top = top_in[...].reshape(lines, LANES)[:, :1]
    both = jnp.maximum(top, new_top)
    old_factor = jnp.exp(top - both)
    new_factor = jnp.exp(new_top - both)
    total = old_factor * total_in[...].reshape(lines, LANES)[:, :1] + new_factor * new_total
    summed = old_factor * sum_in[...].reshape(lines, LANES) + new_factor * new_summed
    return both, total, summed


def pack_part(top, total, summed):
    shape = summed.shape
    row = lax.broadcasted_iota(jnp.int32, shape, len(shape) - 2)
    lane = lax.broadcasted_iota(jnp.int32, shape, len(shape) - 1)
    stats = jnp.where(lane == row, top, jnp.where(lane == row + LANES // 2, total, 0.0))
    stats = jnp.sum(stats, axis=-2, keepdims=True)
    return jnp.where(row == SUBLANES - 1, stats, summed)


def unpack_part(tiles):
    shape = tiles.shape
    row = lax.broadcasted_iota(jnp.int32, shape, len(shape) - 2)
    lane = lax.broadcasted_iota(jnp.int32, shape, len(shape) - 1)
    stats = jnp.broadcast_to(tiles[..., SUBLANES - 1 :, :], shape)
    top = jnp.sum(jnp.where(lane == row, stats, 0.0), axis=-1, keepdims=True)
    total = jnp.sum(jnp.where(lane == row + LANES // 2, stats, 0.0), axis=-1, keepdims=True)
    return top, total, tiles


def merge_parts(parts, used=None):
    tiled = (parts[0].shape[0] // SUBLANES, SUBLANES, LANES)
    parts = [unpack_part(part.reshape(tiled)) for part in parts]
    for n, part in enumerate(parts):
        if used is not None and used[n] is not None:
            parts[n] = [jnp.where(used[n], a, b) for a, b in zip(part, (MASKED, 0.0, 0.0))]
    top = functools.reduce(jnp.maximum, [part[0] for part in parts])
    factors = [jnp.exp(part[0] - top) for part in parts]
    total = sum(factor * part[1] for factor, part in zip(factors, parts))
    summed = sum(factor * part[2] for factor, part in zip(factors, parts))
    return top, total, summed


def store_packed(outs, packed, top, total, summed, layers):
    tiled = (layers, KV_HEADS, SUBLANES)
    tiles = pack_part(
        top.reshape(*tiled, 1), total.reshape(*tiled, 1), summed.reshape(*tiled, LANES)
    )
    for g in range(KV_HEADS):
        packed[g] = tiles[:, g].reshape(layers * SUBLANES, LANES)
    me = lax.axis_index("seq")
    for k in range(KV_HEADS):
        outs[k][...] = packed[me ^ k]


def here_kernel(scale, groups, sure, outer, q_ref, top_in, total_in, sum_in, *refs):
    chunks, (top_ref, total_ref, sum_ref) = refs[:groups], refs[groups:]
    layers, rows = q_ref.shape[:2]
    per = (chunks[0].shape[0] - SUBLANES) // layers // (2 * KV_HEADS)
    limit = jnp.where(is_outer(outer), groups, sure) * per
    lines = layers * rows
    used = lax.broadcasted_iota(jnp.int32, (lines, groups * per), 1) < limit
    top, total, summed = join_image(scale, chunks, used, q_ref, top_in, total_in, sum_in)
    whole = (layers, rows, LANES)
    top_ref[...] = jnp.broadcast_to(top, (lines, LANES)).reshape(whole)
    total_ref[...] = jnp.broadcast_to(total, (lines, LANES)).reshape(whole)
    sum_ref[...] = summed.reshape(whole)


def here_part(parts, chunks, sure, outer, scale):
    groups = len(chunks)
    vmem = pl.BlockSpec(memory_space=pltpu.VMEM)
    rows = chunks[0].shape[0]
    made = pl.pallas_call(
        functools.partial(here_kernel, scale, groups, sure, outer),
        out_shape=[jax.ShapeDtypeStruct(part.shape, part.dtype) for part in parts[1:]],
        in_specs=[vmem] * (4 + groups),
        out_specs=[vmem] * 3,
        cost_estimate=pl.CostEstimate(
            flops=8 * SUBLANES * rows * LANES * groups,
            bytes_accessed=2 * rows * LANES * groups,
            transcendentals=SUBLANES * rows * groups,
        ),
        compiler_params=pltpu.CompilerParams(vmem_limit_bytes=VMEM_LIMIT),
        name="here_part",
    )(*parts, *chunks)
    return [parts[0], *made]


def last_kernel(scale, groups, q_ref, top_in, total_in, sum_in, *refs):
    chunks, outs, packed = refs[:groups], refs[groups:-1], refs[-1]
    parts = join_image(scale, chunks, None, q_ref, top_in, total_in, sum_in)
    store_packed(outs, packed, *parts, q_ref.shape[0])


def far_kernel(scale, count, *refs):
    queries, chunks = refs[:count], refs[count : 2 * count]
    outs, packed = refs[2 * count : -1], refs[-1]
    layers = queries[0].shape[0]
    group = queries[0].shape[1] // HEAD_DIM // KV_HEADS
    lines, keys, values = [], [], []
    for query, chunk in zip(queries, chunks):
        for layer in range(layers):
            lines.append(heads_of(query[pl.ds(layer, 1), :].astype(jnp.float32), group))
        new_keys, new_values = image_columns([chunk], layers)
        keys += new_keys
        values += new_values
    parts = attend(jnp.concatenate(lines, axis=0), keys, values, None, scale)
    store_packed(outs, packed, *parts, count * layers)


def seq_parts(kernel, operands, part_rows, chunk_rows, groups):
    shape = (part_rows, LANES)
    vmem = pl.BlockSpec(memory_space=pltpu.VMEM)
    return pl.pallas_call(
        kernel,
        out_shape=[jax.ShapeDtypeStruct(shape, jnp.float32)] * KV_HEADS,
        in_specs=[vmem] * len(operands),
        out_specs=[vmem] * KV_HEADS,
        scratch_shapes=[pltpu.VMEM((KV_HEADS,) + shape, jnp.float32)],
        cost_estimate=pl.CostEstimate(
            flops=8 * SUBLANES * chunk_rows * LANES * groups,
            bytes_accessed=2 * chunk_rows * LANES * groups,
            transcendentals=SUBLANES * chunk_rows * groups,
        ),
        compiler_params=pltpu.CompilerParams(vmem_limit_bytes=VMEM_LIMIT),
    )(*operands)


def seq_exchange(outs):
    arrived = [
        lax.ppermute(out, "seq", [(s, s ^ k) for s in range(KV_HEADS)])
        for k, out in enumerate(outs)
        if k
    ]
    return [outs[0], *arrived]


def merge_far_kernel(count, *refs):
    parts, outs = refs[:-count], refs[-count:]
    rows = parts[0].shape[0] // count
    merged = pack_part(*merge_parts([part[...] for part in parts]))
    merged = merged.reshape(parts[0].shape)
    for n, out in enumerate(outs):
        out[...] = merged[n * rows : (n + 1) * rows]


def merge_far(parts, count):
    rows = parts[0].shape[0] // count
    vmem = pl.BlockSpec(memory_space=pltpu.VMEM)
    return pl.pallas_call(
        functools.partial(merge_far_kernel, count),
        out_shape=[jax.ShapeDtypeStruct((rows, LANES), jnp.float32)] * count,
        in_specs=[vmem] * len(parts),
        out_specs=[vmem] * count,
        compiler_params=pltpu.CompilerParams(vmem_limit_bytes=VMEM_LIMIT),
        name="merge_far",
    )(*parts)


def is_outer(outer):
    patch = lax.axis_index("patch")
    return functools.reduce(jnp.logical_or, [patch == z for z in outer])


def place_kernel(owners, outer, *refs):
    out_hbm, out_ref, sems = refs[-3:]
    groups = len(owners)
    outside = is_outer(outer)

    def rows_of(k, span):
        first, *others = [refs[n][span, :] for n in owners[k]]
        return jnp.where(outside, others[0], first) if others else first

    layers, band, width = out_ref.shape
    blocks = width // LANES
    per = band // groups
    stores = [
        pltpu.make_async_copy(out_ref.at[layer], out_hbm.at[layer], sems.at[layer])
        for layer in range(layers)
    ]
    base = layers * blocks * per
    lane = lax.broadcasted_iota(jnp.int32, (SUBLANES, LANES), 1)
    tiles = []
    for tile in range(band // LANES):
        row = jnp.zeros((SUBLANES, LANES), jnp.float32)
        for k in range(groups):
            if k * per // LANES == tile:
                extra = rows_of(k, pl.ds(base, SUBLANES)).astype(jnp.float32)
                inside = (lane >= k * per % LANES) & (lane < k * per % LANES + per)
                row = jnp.where(inside, extra, row)
        tiles.append(row)
    digits = jnp.concatenate(tiles, axis=1).astype(jnp.int32)
    places = digits[0:1] + digits[1:2] * LANES
    down = lax.broadcasted_iota(jnp.int32, (band, band), 0)
    choose = jnp.where(down == places, 1.0, 0.0).astype(jnp.bfloat16)
    for layer in range(layers):
        for c in range(0, blocks, 2):
            spans = [pl.ds((layer * blocks + c + n) * per, per) for n in range(2)]
            columns = [
                jnp.concatenate([rows_of(k, span) for k in range(groups)], axis=0)
                for span in spans
            ]
            out_ref[layer, :, c * LANES : (c + 2) * LANES] = jnp.dot(
                choose, jnp.concatenate(columns, axis=1), preferred_element_type=jnp.float32
            ).astype(jnp.bfloat16)
        stores[layer].start()
    for store in stores:
        store.wait()


def place_rows(slots, outer, layers, band, width):
    operands = [chunk for slot in slots for chunk in slot]
    count = iter(range(len(operands)))
    owners = [[next(count) for _ in slot] for slot in slots]
    vmem = pl.BlockSpec(memory_space=pltpu.VMEM)
    return pl.pallas_call(
        functools.partial(place_kernel, owners, outer),
        out_shape=jax.ShapeDtypeStruct((layers, band, width), jnp.bfloat16),
        in_specs=[vmem] * len(operands),
        out_specs=pl.BlockSpec(memory_space=pltpu.HBM),
        scratch_shapes=[
            pltpu.VMEM((layers, band, width), jnp.bfloat16),
            pltpu.SemaphoreType.DMA((layers,)),
        ],
        cost_estimate=pl.CostEstimate(
            flops=2 * layers * band * band * width,
            bytes_accessed=4 * layers * band * width,
            transcendentals=0,
        ),
        compiler_params=pltpu.CompilerParams(vmem_limit_bytes=VMEM_LIMIT),
        name="place_rows",
    )(*operands)


def merge_kernel(group, sure, outer, *refs):
    parts, out_ref, lines = refs[:-2], refs[-2], refs[-1]
    inside = jnp.logical_not(is_outer(outer))
    used = [None if n < sure else inside for n in range(len(parts))]
    _, total, summed = merge_parts([part[...] for part in parts], used)
    result = summed / total
    for i in range(group):
        lines[:, i * HEAD_DIM : (i + 1) * HEAD_DIM] = result[:, i, :]
    out_ref[...] = lines[...].astype(jnp.bfloat16)


def merge(parts, sure, outer, layers, group):
    vmem = pl.BlockSpec(memory_space=pltpu.VMEM)
    return pl.pallas_call(
        functools.partial(merge_kernel, group, sure, outer),
        out_shape=jax.ShapeDtypeStruct((layers, group * HEAD_DIM), jnp.bfloat16),
        in_specs=[vmem] * len(parts),
        out_specs=vmem,
        scratch_shapes=[pltpu.VMEM((layers, group * HEAD_DIM), jnp.float32)],
        compiler_params=pltpu.CompilerParams(vmem_limit_bytes=VMEM_LIMIT),
        name="merge",
    )(*parts)


def exchange_pairs(patch_count, req_count, step, turn):
    pairs = []
    for patch in range(patch_count):
        for req in range(req_count):
            target = next(p for p in range(patch_count) if step_of(patch, p, patch_count) == step)
            pairs.append(
                (patch * req_count + req, target * req_count + (req + turn) % req_count)
            )
    return pairs


def fast_body(query, text_cache, text_len, image_rows, patch_map, image_places):
    layers = query.shape[0]
    patch_count = lax.axis_size("patch")
    req_count = lax.axis_size("req")
    band, width = image_rows.shape[1:]
    group = HEADS // KV_HEADS
    scale = 1.0 / math.sqrt(HEAD_DIM)
    slots = [[step * req_count + turn for turn in range(req_count)] for step in range(patch_count)]
    last = patch_count // 2 - 1
    late = slots[last]
    early = [k for step in range(patch_count - 1) if step != last for k in slots[step]]
    own, core = slots[-1][0], slots[-1][1:]
    pairs = [
        exchange_pairs(patch_count, req_count, k // req_count, k % req_count)
        for k in range(patch_count * req_count)
    ]
    axes = ("patch", "req")
    reach = {
        source: abs(target // req_count - source // req_count) for source, target in pairs[late[0]]
    }
    near = min(reach.values())
    outer = sorted({source // req_count for source, hops in reach.items() if hops > near})

    def stay(pair):
        return (pair[0], pair[0] // req_count * req_count + pair[1] % req_count)

    inner_pairs = {k: [p if reach[p[0]] == near else stay(p) for p in pairs[k]] for k in late}
    outer_pairs = {k: [p if reach[p[0]] > near else stay(p) for p in pairs[k]] for k in late}
    flat_query = query[:, 0]

    def send(value, some):
        return lax.ppermute(value, axes, some)

    far_queries = [
        send(flat_query, [(target, source) for source, target in inner_pairs[k]])
        for k in late
    ]
    grouped = group_rows(patch_map, image_places, image_rows, patch_count, req_count)
    arrived = {own: [grouped[own]]}
    for k in early + core:
        arrived[k] = [send(grouped[k], pairs[k])]
    for k in late:
        arrived[k] = [send(grouped[k], some) for some in (inner_pairs[k], outer_pairs[k])]
    chunk_rows = grouped[0].shape[0]
    part_rows = layers * SUBLANES
    far = seq_parts(
        functools.partial(far_kernel, scale, len(late)),
        [*far_queries, *(grouped[k] for k in late)],
        len(late) * part_rows,
        chunk_rows,
        len(late),
    )
    far = merge_far(seq_exchange(far), len(late))
    far = [send(far[n], inner_pairs[k]) for n, k in enumerate(late)]
    text = text_part(query, text_cache, text_len, scale)
    here = [arrived[k][0] for k in early[:-LAST_CHUNKS] + core + [own]]
    sure = len(here)
    here += [arrived[k][1] for k in late]
    ends = [arrived[k][0] for k in early[-LAST_CHUNKS:]]
    parts = seq_parts(
        functools.partial(last_kernel, scale, len(ends)),
        [*here_part(text, here, sure, outer, scale), *ends],
        part_rows,
        chunk_rows,
        len(ends),
    )
    attended = merge([*seq_exchange(parts), *far], KV_HEADS, outer, layers, group)
    image_cache = place_rows(
        [arrived[k] for k in range(len(grouped))], outer, layers, band, width
    )
    return attended[:, None, :], image_cache[:, None]


def plain_body(query, text_cache, text_len, image_rows, patch_map, image_places):
    layers, req_dev, query_width = query.shape
    text_dev = text_cache.shape[2]
    full_width = text_cache.shape[3]
    kv_width = full_width // 2
    head_dim = HEAD_DIM
    kv_heads = KV_HEADS
    heads = HEADS
    group = heads // kv_heads
    src_rows = image_rows.shape[1]
    patch_count = lax.axis_size("patch")
    req_count = lax.axis_size("req")
    seq_count = lax.axis_size("seq")
    seq_index = lax.axis_index("seq")
    per_source = src_rows // (patch_count * req_count * req_dev)
    band_size = per_source * patch_count * req_count
    scale = 1.0 / math.sqrt(head_dim)
    order = jnp.argsort(patch_map, stable=True)
    grouped = jnp.take(image_rows, order, axis=1)
    grouped_places = jnp.take(image_places, order)
    sending = grouped.reshape(layers, patch_count * req_count, req_dev, per_source, full_width)
    arrived = lax.all_to_all(sending, ("patch", "req"), split_axis=1, concat_axis=3, tiled=True)
    place_send = grouped_places.reshape(patch_count * req_count, req_dev, per_source)
    arrived_places = lax.all_to_all(
        place_send, ("patch", "req"), split_axis=0, concat_axis=2, tiled=True
    )
    image_block = arrived.reshape(layers, req_dev, band_size, full_width)
    local_places = arrived_places.reshape(req_dev, band_size) - seq_index * band_size
    inverse = jnp.argsort(local_places, axis=1)
    image_cache = jnp.take_along_axis(image_block, inverse[None, :, :, None], axis=2)
    queries = query.reshape(layers, req_dev, kv_heads, group, head_dim)
    text_keys = text_cache[..., :kv_width].reshape(layers, req_dev, text_dev, kv_heads, head_dim)
    text_values = text_cache[..., kv_width:].reshape(layers, req_dev, text_dev, kv_heads, head_dim)
    image_keys = image_block[..., :kv_width].reshape(layers, req_dev, band_size, kv_heads, head_dim)
    image_values = image_block[..., kv_width:].reshape(
        layers, req_dev, band_size, kv_heads, head_dim
    )
    positions = seq_index * text_dev + jnp.arange(text_dev, dtype=jnp.int32)
    used = positions[None, :] < text_len[:, None]
    text_raw = (
        jnp.einsum("lrkgd,lrtkd->lrkgt", queries, text_keys, preferred_element_type=jnp.float32)
        * scale
    )
    text_scores = jnp.where(used[None, :, None, None, :], text_raw, -jnp.inf)
    image_scores = (
        jnp.einsum("lrkgd,lrtkd->lrkgt", queries, image_keys, preferred_element_type=jnp.float32)
        * scale
    )
    local_top = jnp.maximum(jnp.max(text_scores, axis=-1), jnp.max(image_scores, axis=-1))
    text_weights = jnp.exp(text_scores - local_top[..., None])
    image_weights = jnp.exp(image_scores - local_top[..., None])
    local_total = jnp.sum(text_weights, axis=-1) + jnp.sum(image_weights, axis=-1)
    text_rounded = text_weights.astype(jnp.bfloat16)
    image_rounded = image_weights.astype(jnp.bfloat16)
    local_values = jnp.einsum(
        "lrkgt,lrtkd->lrkgd", image_rounded, image_values, preferred_element_type=jnp.float32
    )
    local_values = local_values + jnp.einsum(
        "lrkgt,lrtkd->lrkgd", text_rounded, text_values, preferred_element_type=jnp.float32
    )
    width_dev = query_width // seq_count
    top = lax.pmax(local_top, "seq")
    factor = jnp.exp(local_top - top)
    scaled_total = factor * local_total
    scaled_values = factor[..., None] * local_values
    total_sum, value_sum = lax.psum((scaled_total, scaled_values), "seq")
    result = (value_sum / total_sum[..., None]).reshape(layers, req_dev, query_width)
    attended = lax.dynamic_slice_in_dim(result, seq_index * width_dev, width_dev, 2).astype(
        jnp.bfloat16
    )
    return (attended, image_cache)


def body(query, text_cache, text_len, image_rows, patch_map, image_places):
    groups = lax.axis_size("patch") * lax.axis_size("req")
    band = image_rows.shape[1]
    per = band // groups
    fast = (
        query.shape[1] == 1
        and lax.axis_size("patch") == 4
        and groups <= MOST_GROUPS
        and band == per * groups
        and band % LANES == 0
        and per % 16 == 0
        and LANES % per == 0
        and lax.axis_size("seq") == KV_HEADS
        and HEADS // KV_HEADS < SUBLANES
    )
    chosen = fast_body if fast else plain_body
    return chosen(query, text_cache, text_len, image_rows, patch_map, image_places)


def solution(mesh):
    return jax.shard_map(
        body,
        mesh=mesh,
        in_specs=(
            P(None, ("patch", "req"), None),
            P(None, ("patch", "req"), "seq", None),
            P(("patch", "req")),
            P(None, ("patch", "seq", "req"), None),
            P(("patch", "seq", "req")),
            P(("patch", "seq", "req")),
        ),
        out_specs=(P(None, ("patch", "req"), "seq"), P(None, ("patch", "req"), "seq", None)),
        check_vma=False,
    )
```

```python
import functools
import math

import jax
import jax.numpy as jnp
from jax import lax
from jax.experimental import pallas as pl
from jax.experimental.pallas import tpu as pltpu
from jax.sharding import PartitionSpec as P


HEADS = 28
KV_HEADS = 4
HEAD_DIM = 128
LANES = 128
SUBLANES = 8
MASKED = -1e30

MOST_GROUPS = 16
LAST_CHUNKS = 1
VMEM_LIMIT = 16 * 1024 * 1024


def step_of(source, target, count):
    turned = (source ^ target) ^ (count // 2)
    return turned ^ (turned >> 1)


def slot_choice(patch_count, req_count, owner, place):
    src_rows = owner.shape[1]
    per = src_rows // (patch_count * req_count)
    me = lax.axis_index("patch")
    mine = lax.axis_index("req")
    shape = (src_rows, src_rows)
    down = lax.broadcasted_iota(jnp.int32, shape, 0)
    across = lax.broadcasted_iota(jnp.int32, shape, 1)
    owner_row = jnp.broadcast_to(owner, shape)
    owner_col = jnp.sum(
        jnp.where(down == across, owner_row.astype(jnp.float32), 0.0), axis=1, keepdims=True
    ).astype(jnp.int32)
    ahead = (owner_row == owner_col) & (down < across)
    rank = jnp.sum(jnp.where(ahead, 1.0, 0.0), axis=0, keepdims=True).astype(jnp.int32)
    step = step_of(me, owner // req_count, patch_count)
    turn = (owner % req_count - mine + req_count) % req_count
    slot = (step * req_count + turn) * per + rank
    choose = jnp.where(down == slot, 1.0, 0.0).astype(jnp.bfloat16)
    local = place - lax.axis_index("seq") * src_rows
    line = lax.broadcasted_iota(jnp.int32, (SUBLANES, src_rows), 0)
    digits = jnp.where(line == 0, local & (LANES - 1), jnp.where(line == 1, local // LANES, 0))
    places = lax.dot_general(
        digits.astype(jnp.float32).astype(jnp.bfloat16),
        choose,
        (((1,), (1,)), ((), ())),
        preferred_element_type=jnp.float32,
    ).astype(jnp.bfloat16)
    return choose, places


def pack_slots(first, per, choose, places, layer_rows, layers, outs):
    for k, out in enumerate(outs):
        tile = (first + k) * per // LANES
        out[pl.ds(out.shape[0] - SUBLANES, SUBLANES), :] = places[
            :, tile * LANES : (tile + 1) * LANES
        ]
    taken = choose[first * per : (first + len(outs)) * per]
    for layer in range(layers):
        rows = layer_rows(layer)
        blocks = rows.shape[1] // LANES
        moved = jnp.dot(taken, rows, preferred_element_type=jnp.float32).astype(jnp.bfloat16)
        for k, out in enumerate(outs):
            for c in range(blocks):
                out[pl.ds((layer * blocks + c) * per, per), :] = moved[
                    k * per : (k + 1) * per, c * LANES : (c + 1) * LANES
                ]


def first_kernel(patch_count, req_count, map_hbm, place_hbm, rows_hbm, *refs):
    choose_ref, places_ref, rows_ref, *outs = refs[:-4]
    owner_ref, place_ref, small_sem, rows_sem = refs[-4:]
    layers, src_rows, _ = rows_hbm.shape
    small = [
        pltpu.make_async_copy(map_hbm, owner_ref, small_sem.at[0]),
        pltpu.make_async_copy(place_hbm, place_ref, small_sem.at[1]),
    ]
    loads = [
        pltpu.make_async_copy(rows_hbm.at[layer], rows_ref.at[layer], rows_sem.at[layer])
        for layer in range(layers)
    ]
    for copy in small + loads:
        copy.start()
    for copy in small:
        copy.wait()
    choose, places = slot_choice(patch_count, req_count, owner_ref[...], place_ref[...])
    choose_ref[...] = choose
    places_ref[...] = places

    def layer_rows(layer):
        loads[layer].wait()
        return rows_ref[layer]

    per = src_rows // (patch_count * req_count)
    pack_slots(0, per, choose, places, layer_rows, layers, outs)


def rest_kernel(first, per, choose_ref, places_ref, rows_ref, *outs):
    pack_slots(
        first,
        per,
        choose_ref[...],
        places_ref[...],
        lambda layer: rows_ref[layer],
        rows_ref.shape[0],
        outs,
    )


def in_hbm(array):
    return pltpu.with_memory_space_constraint(array, pltpu.HBM)


def group_rows(patch_map, image_places, image_rows, patch_count, req_count):
    layers, src_rows, width = image_rows.shape
    groups = patch_count * req_count
    per = src_rows // groups
    chunk = jax.ShapeDtypeStruct((layers * per * width // LANES + SUBLANES, LANES), jnp.bfloat16)
    hbm = pl.BlockSpec(memory_space=pltpu.HBM)
    vmem = pl.BlockSpec(memory_space=pltpu.VMEM)

    def cost(count):
        return pl.CostEstimate(
            flops=2 * layers * src_rows * per * count * width,
            bytes_accessed=2 * layers * (src_rows + per * count) * width,
            transcendentals=0,
        )

    first_call = pl.pallas_call(
        functools.partial(first_kernel, patch_count, req_count),
        out_shape=[
            jax.ShapeDtypeStruct((src_rows, src_rows), jnp.bfloat16),
            jax.ShapeDtypeStruct((SUBLANES, src_rows), jnp.bfloat16),
            jax.ShapeDtypeStruct(image_rows.shape, jnp.bfloat16),
        ]
        + [chunk] * req_count,
        in_specs=[hbm] * 3,
        out_specs=[vmem] * (3 + req_count),
        scratch_shapes=[
            pltpu.VMEM((1, src_rows), jnp.int32),
            pltpu.VMEM((1, src_rows), jnp.int32),
            pltpu.SemaphoreType.DMA((2,)),
            pltpu.SemaphoreType.DMA((layers,)),
        ],
        cost_estimate=cost(req_count),
        compiler_params=pltpu.CompilerParams(vmem_limit_bytes=VMEM_LIMIT),
        name="group_first",
    )
    choose, places, rows, *first = first_call(
        in_hbm(patch_map.reshape(1, src_rows)),
        in_hbm(image_places.reshape(1, src_rows)),
        in_hbm(image_rows),
    )
    rest_call = pl.pallas_call(
        functools.partial(rest_kernel, req_count, per),
        out_shape=[chunk] * (groups - req_count),
        in_specs=[vmem] * 3,
        out_specs=[vmem] * (groups - req_count),
        cost_estimate=cost(groups - req_count),
        compiler_params=pltpu.CompilerParams(vmem_limit_bytes=VMEM_LIMIT),
        name="group_rest",
    )
    rest = rest_call(choose, places, rows)
    return [*first, *rest]


def heads_of(line, group):
    row = lax.broadcasted_iota(jnp.int32, (SUBLANES, HEAD_DIM), 0)
    tiles = []
    for g in range(KV_HEADS):
        tile = jnp.zeros((SUBLANES, HEAD_DIM), jnp.float32)
        for i in range(group):
            h = g * group + i
            tile = jnp.where(row == i, line[:, h * HEAD_DIM : (h + 1) * HEAD_DIM], tile)
        tiles.append(tile)
    return jnp.concatenate(tiles, axis=0).astype(jnp.bfloat16)


def attend(queries, keys, values, used, scale, least=None):
    def tile(rows, n):
        return rows[n * SUBLANES : (n + 1) * SUBLANES]

    scores = jnp.concatenate(
        [
            lax.dot_general(
                tile(queries, n), key, (((1,), (1,)), ((), ())), preferred_element_type=jnp.float32
            )
            for n, key in enumerate(keys)
        ],
        axis=0,
    )
    scores = scores * scale
    if used is not None:
        scores = jnp.where(used, scores, MASKED)
    top = jnp.max(scores, axis=1, keepdims=True)
    if least is not None:
        top = jnp.maximum(top, least)
    weights = jnp.exp(scores - top)
    if used is not None:
        weights = jnp.where(used, weights, 0.0)
    total = jnp.sum(weights, axis=1, keepdims=True)
    rounded = weights.astype(jnp.bfloat16)
    summed = jnp.concatenate(
        [
            jnp.dot(tile(rounded, n), value, preferred_element_type=jnp.float32)
            for n, value in enumerate(values)
        ],
        axis=0,
    )
    return top, total, summed


def text_kernel(scale, len_ref, query_ref, text_ref, q_ref, top_ref, total_ref, sum_ref):
    text_dev, width = text_ref.shape
    group = query_ref.shape[1] // HEAD_DIM // KV_HEADS
    queries = heads_of(query_ref[...].astype(jnp.float32), group)
    q_ref[...] = queries
    rows = KV_HEADS * SUBLANES
    positions = lax.axis_index("seq") * text_dev + lax.broadcasted_iota(
        jnp.int32, (rows, text_dev), 1
    )
    keys = [text_ref[:, g * HEAD_DIM : (g + 1) * HEAD_DIM] for g in range(KV_HEADS)]
    values = [
        text_ref[:, width // 2 + g * HEAD_DIM : width // 2 + (g + 1) * HEAD_DIM]
        for g in range(KV_HEADS)
    ]
    top, total, summed = attend(queries, keys, values, positions < len_ref[0], scale)
    top_ref[...] = jnp.broadcast_to(top, (rows, LANES))
    total_ref[...] = jnp.broadcast_to(total, (rows, LANES))
    sum_ref[...] = summed


def text_part(query, text_cache, text_len, scale):
    layers, _, query_width = query.shape
    text_dev, width = text_cache.shape[2:]
    rows = KV_HEADS * SUBLANES
    part = pl.BlockSpec((None, rows, LANES), lambda layer, _: (layer, 0, 0))
    return pl.pallas_call(
        functools.partial(text_kernel, scale),
        out_shape=[
            jax.ShapeDtypeStruct((layers, rows, HEAD_DIM), jnp.bfloat16),
            jax.ShapeDtypeStruct((layers, rows, LANES), jnp.float32),
            jax.ShapeDtypeStruct((layers, rows, LANES), jnp.float32),
            jax.ShapeDtypeStruct((layers, rows, HEAD_DIM), jnp.float32),
        ],
        grid_spec=pltpu.PrefetchScalarGridSpec(
            num_scalar_prefetch=1,
            grid=(layers,),
            in_specs=[
                pl.BlockSpec((None, 1, query_width), lambda layer, _: (layer, 0, 0)),
                pl.BlockSpec((None, None, text_dev, width), lambda layer, _: (layer, 0, 0, 0)),
            ],
            out_specs=[part] * 4,
        ),
        cost_estimate=pl.CostEstimate(
            flops=8 * layers * SUBLANES * LANES * text_dev * width,
            bytes_accessed=2 * layers * text_dev * width,
            transcendentals=layers * rows * text_dev,
        ),
        compiler_params=pltpu.CompilerParams(vmem_limit_bytes=VMEM_LIMIT),
        name="text_part",
    )(text_len, query, in_hbm(text_cache))


def image_columns(chunks, layers):
    blocks = 2 * KV_HEADS
    per = (chunks[0].shape[0] - SUBLANES) // layers // blocks

    def column(layer, c):
        span = pl.ds((layer * blocks + c) * per, per)
        return jnp.concatenate([chunk[span, :] for chunk in chunks], axis=0)

    keys = [column(layer, g) for layer in range(layers) for g in range(KV_HEADS)]
    values = [column(layer, KV_HEADS + g) for layer in range(layers) for g in range(KV_HEADS)]
    return keys, values


def join_image(scale, chunks, used, q_ref, top_in, total_in, sum_in):
    layers, rows, _ = q_ref.shape
    lines = layers * rows
    keys, values = image_columns(chunks, layers)
    queries = q_ref[...].reshape(lines, HEAD_DIM)
    old_top = top_in[...].reshape(lines, LANES)[:, :1]
    top, total, summed = attend(queries, keys, values, used, scale, old_top)
    factor = jnp.exp(old_top - top)
    total += factor * total_in[...].reshape(lines, LANES)[:, :1]
    summed += factor * sum_in[...].reshape(lines, LANES)
    return top, total, summed


def pack_part(top, total, summed):
    shape = summed.shape
    row = lax.broadcasted_iota(jnp.int32, shape, len(shape) - 2)
    lane = lax.broadcasted_iota(jnp.int32, shape, len(shape) - 1)
    stats = jnp.where(lane == row, top, jnp.where(lane == row + LANES // 2, total, 0.0))
    stats = jnp.sum(stats, axis=-2, keepdims=True)
    return jnp.where(row == SUBLANES - 1, stats, summed)


def unpack_part(tiles):
    shape = tiles.shape
    row = lax.broadcasted_iota(jnp.int32, shape, len(shape) - 2)
    lane = lax.broadcasted_iota(jnp.int32, shape, len(shape) - 1)
    stats = jnp.broadcast_to(tiles[..., SUBLANES - 1 :, :], shape)
    top = jnp.sum(jnp.where(lane == row, stats, 0.0), axis=-1, keepdims=True)
    total = jnp.sum(jnp.where(lane == row + LANES // 2, stats, 0.0), axis=-1, keepdims=True)
    return top, total, tiles


def merge_parts(parts, used=None):
    tiled = (parts[0].shape[0] // SUBLANES, SUBLANES, LANES)
    parts = [unpack_part(part.reshape(tiled)) for part in parts]
    for n, part in enumerate(parts):
        if used is not None and used[n] is not None:
            parts[n] = [jnp.where(used[n], a, b) for a, b in zip(part, (MASKED, 0.0, 0.0))]
    top = functools.reduce(jnp.maximum, [part[0] for part in parts])
    factors = [jnp.exp(part[0] - top) for part in parts]
    total = sum(factor * part[1] for factor, part in zip(factors, parts))
    summed = sum(factor * part[2] for factor, part in zip(factors, parts))
    return top, total, summed


def store_packed(outs, packed, top, total, summed, layers):
    tiled = (layers, KV_HEADS, SUBLANES)
    tiles = pack_part(
        top.reshape(*tiled, 1), total.reshape(*tiled, 1), summed.reshape(*tiled, LANES)
    )
    for g in range(KV_HEADS):
        packed[g] = tiles[:, g].reshape(layers * SUBLANES, LANES)
    me = lax.axis_index("seq")
    for k in range(KV_HEADS):
        outs[k][...] = packed[me ^ k]


def here_kernel(scale, groups, sure, outer, q_ref, top_in, total_in, sum_in, *refs):
    chunks, (top_ref, total_ref, sum_ref) = refs[:groups], refs[groups:]
    layers, rows = q_ref.shape[:2]
    per = (chunks[0].shape[0] - SUBLANES) // layers // (2 * KV_HEADS)
    limit = jnp.where(is_outer(outer), groups, sure) * per
    lines = layers * rows
    used = lax.broadcasted_iota(jnp.int32, (lines, groups * per), 1) < limit
    top, total, summed = join_image(scale, chunks, used, q_ref, top_in, total_in, sum_in)
    whole = (layers, rows, LANES)
    top_ref[...] = jnp.broadcast_to(top, (lines, LANES)).reshape(whole)
    total_ref[...] = jnp.broadcast_to(total, (lines, LANES)).reshape(whole)
    sum_ref[...] = summed.reshape(whole)


def here_part(parts, chunks, sure, outer, scale):
    groups = len(chunks)
    vmem = pl.BlockSpec(memory_space=pltpu.VMEM)
    rows = chunks[0].shape[0]
    made = pl.pallas_call(
        functools.partial(here_kernel, scale, groups, sure, outer),
        out_shape=[jax.ShapeDtypeStruct(part.shape, part.dtype) for part in parts[1:]],
        in_specs=[vmem] * (4 + groups),
        out_specs=[vmem] * 3,
        cost_estimate=pl.CostEstimate(
            flops=8 * SUBLANES * rows * LANES * groups,
            bytes_accessed=2 * rows * LANES * groups,
            transcendentals=SUBLANES * rows * groups,
        ),
        compiler_params=pltpu.CompilerParams(vmem_limit_bytes=VMEM_LIMIT),
        name="here_part",
    )(*parts, *chunks)
    return [parts[0], *made]


def last_kernel(scale, groups, q_ref, top_in, total_in, sum_in, *refs):
    chunks, outs, packed = refs[:groups], refs[groups:-1], refs[-1]
    parts = join_image(scale, chunks, None, q_ref, top_in, total_in, sum_in)
    store_packed(outs, packed, *parts, q_ref.shape[0])


def far_kernel(scale, count, *refs):
    queries, chunks = refs[:count], refs[count : 2 * count]
    outs, packed = refs[2 * count : -1], refs[-1]
    layers = queries[0].shape[0]
    group = queries[0].shape[1] // HEAD_DIM // KV_HEADS
    lines, keys, values = [], [], []
    for query, chunk in zip(queries, chunks):
        for layer in range(layers):
            lines.append(heads_of(query[pl.ds(layer, 1), :].astype(jnp.float32), group))
        new_keys, new_values = image_columns([chunk], layers)
        keys += new_keys
        values += new_values
    parts = attend(jnp.concatenate(lines, axis=0), keys, values, None, scale)
    store_packed(outs, packed, *parts, count * layers)


def seq_parts(kernel, operands, part_rows, chunk_rows, groups):
    shape = (part_rows, LANES)
    vmem = pl.BlockSpec(memory_space=pltpu.VMEM)
    return pl.pallas_call(
        kernel,
        out_shape=[jax.ShapeDtypeStruct(shape, jnp.float32)] * KV_HEADS,
        in_specs=[vmem] * len(operands),
        out_specs=[vmem] * KV_HEADS,
        scratch_shapes=[pltpu.VMEM((KV_HEADS,) + shape, jnp.float32)],
        cost_estimate=pl.CostEstimate(
            flops=8 * SUBLANES * chunk_rows * LANES * groups,
            bytes_accessed=2 * chunk_rows * LANES * groups,
            transcendentals=SUBLANES * chunk_rows * groups,
        ),
        compiler_params=pltpu.CompilerParams(vmem_limit_bytes=VMEM_LIMIT),
    )(*operands)


def seq_exchange(outs):
    arrived = [
        lax.ppermute(out, "seq", [(s, s ^ k) for s in range(KV_HEADS)])
        for k, out in enumerate(outs)
        if k
    ]
    return [outs[0], *arrived]


def merge_far_kernel(count, *refs):
    parts, outs = refs[:-count], refs[-count:]
    rows = parts[0].shape[0] // count
    merged = pack_part(*merge_parts([part[...] for part in parts]))
    merged = merged.reshape(parts[0].shape)
    for n, out in enumerate(outs):
        out[...] = merged[n * rows : (n + 1) * rows]


def merge_far(parts, count):
    rows = parts[0].shape[0] // count
    vmem = pl.BlockSpec(memory_space=pltpu.VMEM)
    return pl.pallas_call(
        functools.partial(merge_far_kernel, count),
        out_shape=[jax.ShapeDtypeStruct((rows, LANES), jnp.float32)] * count,
        in_specs=[vmem] * len(parts),
        out_specs=[vmem] * count,
        compiler_params=pltpu.CompilerParams(vmem_limit_bytes=VMEM_LIMIT),
        name="merge_far",
    )(*parts)


def is_outer(outer):
    patch = lax.axis_index("patch")
    return functools.reduce(jnp.logical_or, [patch == z for z in outer])


def place_kernel(owners, outer, *refs):
    out_hbm, out_ref, sems = refs[-3:]
    groups = len(owners)
    outside = is_outer(outer)

    def rows_of(k, span):
        first, *others = [refs[n][span, :] for n in owners[k]]
        return jnp.where(outside, others[0], first) if others else first

    layers, band, width = out_ref.shape
    blocks = width // LANES
    per = band // groups
    stores = [
        pltpu.make_async_copy(out_ref.at[layer], out_hbm.at[layer], sems.at[layer])
        for layer in range(layers)
    ]
    base = layers * blocks * per
    lane = lax.broadcasted_iota(jnp.int32, (SUBLANES, LANES), 1)
    tiles = []
    for tile in range(band // LANES):
        row = jnp.zeros((SUBLANES, LANES), jnp.float32)
        for k in range(groups):
            if k * per // LANES == tile:
                extra = rows_of(k, pl.ds(base, SUBLANES)).astype(jnp.float32)
                inside = (lane >= k * per % LANES) & (lane < k * per % LANES + per)
                row = jnp.where(inside, extra, row)
        tiles.append(row)
    digits = jnp.concatenate(tiles, axis=1).astype(jnp.int32)
    places = digits[0:1] + digits[1:2] * LANES
    down = lax.broadcasted_iota(jnp.int32, (band, band), 0)
    choose = jnp.where(down == places, 1.0, 0.0).astype(jnp.bfloat16)
    for layer in range(layers):
        for c in range(0, blocks, 2):
            spans = [pl.ds((layer * blocks + c + n) * per, per) for n in range(2)]
            columns = [
                jnp.concatenate([rows_of(k, span) for k in range(groups)], axis=0)
                for span in spans
            ]
            out_ref[layer, :, c * LANES : (c + 2) * LANES] = jnp.dot(
                choose, jnp.concatenate(columns, axis=1), preferred_element_type=jnp.float32
            ).astype(jnp.bfloat16)
        stores[layer].start()
    for store in stores:
        store.wait()


def place_rows(slots, outer, layers, band, width):
    operands = [chunk for slot in slots for chunk in slot]
    count = iter(range(len(operands)))
    owners = [[next(count) for _ in slot] for slot in slots]
    vmem = pl.BlockSpec(memory_space=pltpu.VMEM)
    return pl.pallas_call(
        functools.partial(place_kernel, owners, outer),
        out_shape=jax.ShapeDtypeStruct((layers, band, width), jnp.bfloat16),
        in_specs=[vmem] * len(operands),
        out_specs=pl.BlockSpec(memory_space=pltpu.HBM),
        scratch_shapes=[
            pltpu.VMEM((layers, band, width), jnp.bfloat16),
            pltpu.SemaphoreType.DMA((layers,)),
        ],
        cost_estimate=pl.CostEstimate(
            flops=2 * layers * band * band * width,
            bytes_accessed=4 * layers * band * width,
            transcendentals=0,
        ),
        compiler_params=pltpu.CompilerParams(vmem_limit_bytes=VMEM_LIMIT),
        name="place_rows",
    )(*operands)


def merge_kernel(group, sure, outer, *refs):
    parts, out_ref, lines = refs[:-2], refs[-2], refs[-1]
    inside = jnp.logical_not(is_outer(outer))
    used = [None if n < sure else inside for n in range(len(parts))]
    _, total, summed = merge_parts([part[...] for part in parts], used)
    result = summed / total
    for i in range(group):
        lines[:, i * HEAD_DIM : (i + 1) * HEAD_DIM] = result[:, i, :]
    out_ref[...] = lines[...].astype(jnp.bfloat16)


def merge(parts, sure, outer, layers, group):
    vmem = pl.BlockSpec(memory_space=pltpu.VMEM)
    return pl.pallas_call(
        functools.partial(merge_kernel, group, sure, outer),
        out_shape=jax.ShapeDtypeStruct((layers, group * HEAD_DIM), jnp.bfloat16),
        in_specs=[vmem] * len(parts),
        out_specs=vmem,
        scratch_shapes=[pltpu.VMEM((layers, group * HEAD_DIM), jnp.float32)],
        compiler_params=pltpu.CompilerParams(vmem_limit_bytes=VMEM_LIMIT),
        name="merge",
    )(*parts)


def exchange_pairs(patch_count, req_count, step, turn):
    pairs = []
    for patch in range(patch_count):
        for req in range(req_count):
            target = next(p for p in range(patch_count) if step_of(patch, p, patch_count) == step)
            pairs.append(
                (patch * req_count + req, target * req_count + (req + turn) % req_count)
            )
    return pairs


def fast_body(query, text_cache, text_len, image_rows, patch_map, image_places):
    layers = query.shape[0]
    patch_count = lax.axis_size("patch")
    req_count = lax.axis_size("req")
    band, width = image_rows.shape[1:]
    group = HEADS // KV_HEADS
    scale = 1.0 / math.sqrt(HEAD_DIM)
    slots = [[step * req_count + turn for turn in range(req_count)] for step in range(patch_count)]
    last = patch_count // 2 - 1
    late = slots[last]
    early = [k for step in range(patch_count - 1) if step != last for k in slots[step]]
    own, core = slots[-1][0], slots[-1][1:]
    pairs = [
        exchange_pairs(patch_count, req_count, k // req_count, k % req_count)
        for k in range(patch_count * req_count)
    ]
    axes = ("patch", "req")
    reach = {
        source: abs(target // req_count - source // req_count) for source, target in pairs[late[0]]
    }
    near = min(reach.values())
    outer = sorted({source // req_count for source, hops in reach.items() if hops > near})

    def stay(pair):
        return (pair[0], pair[0] // req_count * req_count + pair[1] % req_count)

    inner_pairs = {k: [p if reach[p[0]] == near else stay(p) for p in pairs[k]] for k in late}
    outer_pairs = {k: [p if reach[p[0]] > near else stay(p) for p in pairs[k]] for k in late}
    flat_query = query[:, 0]

    def send(value, some):
        return lax.ppermute(value, axes, some)

    far_queries = [
        send(flat_query, [(target, source) for source, target in inner_pairs[k]])
        for k in late
    ]
    grouped = group_rows(patch_map, image_places, image_rows, patch_count, req_count)
    arrived = {own: [grouped[own]]}
    for k in early + core:
        arrived[k] = [send(grouped[k], pairs[k])]
    for k in late:
        arrived[k] = [send(grouped[k], some) for some in (inner_pairs[k], outer_pairs[k])]
    chunk_rows = grouped[0].shape[0]
    part_rows = layers * SUBLANES
    far = seq_parts(
        functools.partial(far_kernel, scale, len(late)),
        [*far_queries, *(grouped[k] for k in late)],
        len(late) * part_rows,
        chunk_rows,
        len(late),
    )
    far = merge_far(seq_exchange(far), len(late))
    far = [send(far[n], inner_pairs[k]) for n, k in enumerate(late)]
    text = text_part(query, text_cache, text_len, scale)
    here = [arrived[k][0] for k in early[:-LAST_CHUNKS] + core + [own]]
    sure = len(here)
    here += [arrived[k][1] for k in late]
    ends = [arrived[k][0] for k in early[-LAST_CHUNKS:]]
    parts = seq_parts(
        functools.partial(last_kernel, scale, len(ends)),
        [*here_part(text, here, sure, outer, scale), *ends],
        part_rows,
        chunk_rows,
        len(ends),
    )
    attended = merge([*seq_exchange(parts), *far], KV_HEADS, outer, layers, group)
    image_cache = place_rows(
        [arrived[k] for k in range(len(grouped))], outer, layers, band, width
    )
    return attended[:, None, :], image_cache[:, None]


def plain_body(query, text_cache, text_len, image_rows, patch_map, image_places):
    layers, req_dev, query_width = query.shape
    text_dev = text_cache.shape[2]
    full_width = text_cache.shape[3]
    kv_width = full_width // 2
    head_dim = HEAD_DIM
    kv_heads = KV_HEADS
    heads = HEADS
    group = heads // kv_heads
    src_rows = image_rows.shape[1]
    patch_count = lax.axis_size("patch")
    req_count = lax.axis_size("req")
    seq_count = lax.axis_size("seq")
    seq_index = lax.axis_index("seq")
    per_source = src_rows // (patch_count * req_count * req_dev)
    band_size = per_source * patch_count * req_count
    scale = 1.0 / math.sqrt(head_dim)
    order = jnp.argsort(patch_map, stable=True)
    grouped = jnp.take(image_rows, order, axis=1)
    grouped_places = jnp.take(image_places, order)
    sending = grouped.reshape(layers, patch_count * req_count, req_dev, per_source, full_width)
    arrived = lax.all_to_all(sending, ("patch", "req"), split_axis=1, concat_axis=3, tiled=True)
    place_send = grouped_places.reshape(patch_count * req_count, req_dev, per_source)
    arrived_places = lax.all_to_all(
        place_send, ("patch", "req"), split_axis=0, concat_axis=2, tiled=True
    )
    image_block = arrived.reshape(layers, req_dev, band_size, full_width)
    local_places = arrived_places.reshape(req_dev, band_size) - seq_index * band_size
    inverse = jnp.argsort(local_places, axis=1)
    image_cache = jnp.take_along_axis(image_block, inverse[None, :, :, None], axis=2)
    queries = query.reshape(layers, req_dev, kv_heads, group, head_dim)
    text_keys = text_cache[..., :kv_width].reshape(layers, req_dev, text_dev, kv_heads, head_dim)
    text_values = text_cache[..., kv_width:].reshape(layers, req_dev, text_dev, kv_heads, head_dim)
    image_keys = image_block[..., :kv_width].reshape(layers, req_dev, band_size, kv_heads, head_dim)
    image_values = image_block[..., kv_width:].reshape(
        layers, req_dev, band_size, kv_heads, head_dim
    )
    positions = seq_index * text_dev + jnp.arange(text_dev, dtype=jnp.int32)
    used = positions[None, :] < text_len[:, None]
    text_raw = (
        jnp.einsum("lrkgd,lrtkd->lrkgt", queries, text_keys, preferred_element_type=jnp.float32)
        * scale
    )
    text_scores = jnp.where(used[None, :, None, None, :], text_raw, -jnp.inf)
    image_scores = (
        jnp.einsum("lrkgd,lrtkd->lrkgt", queries, image_keys, preferred_element_type=jnp.float32)
        * scale
    )
    local_top = jnp.maximum(jnp.max(text_scores, axis=-1), jnp.max(image_scores, axis=-1))
    text_weights = jnp.exp(text_scores - local_top[..., None])
    image_weights = jnp.exp(image_scores - local_top[..., None])
    local_total = jnp.sum(text_weights, axis=-1) + jnp.sum(image_weights, axis=-1)
    text_rounded = text_weights.astype(jnp.bfloat16)
    image_rounded = image_weights.astype(jnp.bfloat16)
    local_values = jnp.einsum(
        "lrkgt,lrtkd->lrkgd", image_rounded, image_values, preferred_element_type=jnp.float32
    )
    local_values = local_values + jnp.einsum(
        "lrkgt,lrtkd->lrkgd", text_rounded, text_values, preferred_element_type=jnp.float32
    )
    width_dev = query_width // seq_count
    top = lax.pmax(local_top, "seq")
    factor = jnp.exp(local_top - top)
    scaled_total = factor * local_total
    scaled_values = factor[..., None] * local_values
    total_sum, value_sum = lax.psum((scaled_total, scaled_values), "seq")
    result = (value_sum / total_sum[..., None]).reshape(layers, req_dev, query_width)
    attended = lax.dynamic_slice_in_dim(result, seq_index * width_dev, width_dev, 2).astype(
        jnp.bfloat16
    )
    return (attended, image_cache)


def body(query, text_cache, text_len, image_rows, patch_map, image_places):
    groups = lax.axis_size("patch") * lax.axis_size("req")
    band = image_rows.shape[1]
    per = band // groups
    fast = (
        query.shape[1] == 1
        and lax.axis_size("patch") == 4
        and groups <= MOST_GROUPS
        and band == per * groups
        and band % LANES == 0
        and per % 16 == 0
        and LANES % per == 0
        and lax.axis_size("seq") == KV_HEADS
        and HEADS // KV_HEADS < SUBLANES
    )
    chosen = fast_body if fast else plain_body
    return chosen(query, text_cache, text_len, image_rows, patch_map, image_places)


def solution(mesh):
    return jax.shard_map(
        body,
        mesh=mesh,
        in_specs=(
            P(None, ("patch", "req"), None),
            P(None, ("patch", "req"), "seq", None),
            P(("patch", "req")),
            P(None, ("patch", "seq", "req"), None),
            P(("patch", "seq", "req")),
            P(("patch", "seq", "req")),
        ),
        out_specs=(P(None, ("patch", "req"), "seq"), P(None, ("patch", "req"), "seq", None)),
        check_vma=False,
    )
```

```python
import functools
import math

import jax
import jax.numpy as jnp
from jax import lax
from jax.experimental import pallas as pl
from jax.experimental.pallas import tpu as pltpu
from jax.sharding import PartitionSpec as P


HEADS = 28
KV_HEADS = 4
HEAD_DIM = 128
LANES = 128
SUBLANES = 8
MASKED = -1e30

MOST_GROUPS = 16
LAST_CHUNKS = 1
VMEM_LIMIT = 16 * 1024 * 1024


def step_of(source, target, count):
    turned = (source ^ target) ^ (count // 2)
    return turned ^ (turned >> 1)


def slot_choice(patch_count, req_count, owner, place):
    src_rows = owner.shape[1]
    per = src_rows // (patch_count * req_count)
    me = lax.axis_index("patch")
    mine = lax.axis_index("req")
    shape = (src_rows, src_rows)
    down = lax.broadcasted_iota(jnp.int32, shape, 0)
    across = lax.broadcasted_iota(jnp.int32, shape, 1)
    owner_row = jnp.broadcast_to(owner, shape)
    owner_col = jnp.sum(
        jnp.where(down == across, owner_row.astype(jnp.float32), 0.0), axis=1, keepdims=True
    ).astype(jnp.int32)
    ahead = (owner_row == owner_col) & (down < across)
    rank = jnp.sum(jnp.where(ahead, 1.0, 0.0), axis=0, keepdims=True).astype(jnp.int32)
    step = step_of(me, owner // req_count, patch_count)
    turn = (owner % req_count - mine + req_count) % req_count
    slot = (step * req_count + turn) * per + rank
    choose = jnp.where(down == slot, 1.0, 0.0).astype(jnp.bfloat16)
    local = place - lax.axis_index("seq") * src_rows
    line = lax.broadcasted_iota(jnp.int32, (SUBLANES, src_rows), 0)
    digits = jnp.where(line == 0, local & (LANES - 1), jnp.where(line == 1, local // LANES, 0))
    places = lax.dot_general(
        digits.astype(jnp.float32).astype(jnp.bfloat16),
        choose,
        (((1,), (1,)), ((), ())),
        preferred_element_type=jnp.float32,
    ).astype(jnp.bfloat16)
    return choose, places


def pack_slots(first, per, choose, places, layer_rows, layers, outs):
    for k, out in enumerate(outs):
        tile = (first + k) * per // LANES
        out[pl.ds(out.shape[0] - SUBLANES, SUBLANES), :] = places[
            :, tile * LANES : (tile + 1) * LANES
        ]
    taken = choose[first * per : (first + len(outs)) * per]
    for layer in range(layers):
        rows = layer_rows(layer)
        blocks = rows.shape[1] // LANES
        moved = jnp.dot(taken, rows, preferred_element_type=jnp.float32).astype(jnp.bfloat16)
        for k, out in enumerate(outs):
            for c in range(blocks):
                out[pl.ds((layer * blocks + c) * per, per), :] = moved[
                    k * per : (k + 1) * per, c * LANES : (c + 1) * LANES
                ]


def first_kernel(patch_count, req_count, map_hbm, place_hbm, rows_hbm, *refs):
    choose_ref, places_ref, rows_ref, *outs = refs[:-4]
    owner_ref, place_ref, small_sem, rows_sem = refs[-4:]
    layers, src_rows, _ = rows_hbm.shape
    small = [
        pltpu.make_async_copy(map_hbm, owner_ref, small_sem.at[0]),
        pltpu.make_async_copy(place_hbm, place_ref, small_sem.at[1]),
    ]
    loads = [
        pltpu.make_async_copy(rows_hbm.at[layer], rows_ref.at[layer], rows_sem.at[layer])
        for layer in range(layers)
    ]
    for copy in small + loads:
        copy.start()
    for copy in small:
        copy.wait()
    choose, places = slot_choice(patch_count, req_count, owner_ref[...], place_ref[...])
    choose_ref[...] = choose
    places_ref[...] = places

    def layer_rows(layer):
        loads[layer].wait()
        return rows_ref[layer]

    per = src_rows // (patch_count * req_count)
    pack_slots(0, per, choose, places, layer_rows, layers, outs)


def rest_kernel(first, per, choose_ref, places_ref, rows_ref, *outs):
    pack_slots(
        first,
        per,
        choose_ref[...],
        places_ref[...],
        lambda layer: rows_ref[layer],
        rows_ref.shape[0],
        outs,
    )


def in_hbm(array):
    return pltpu.with_memory_space_constraint(array, pltpu.HBM)


def group_rows(patch_map, image_places, image_rows, patch_count, req_count):
    layers, src_rows, width = image_rows.shape
    groups = patch_count * req_count
    per = src_rows // groups
    chunk = jax.ShapeDtypeStruct((layers * per * width // LANES + SUBLANES, LANES), jnp.bfloat16)
    hbm = pl.BlockSpec(memory_space=pltpu.HBM)
    vmem = pl.BlockSpec(memory_space=pltpu.VMEM)

    def cost(count):
        return pl.CostEstimate(
            flops=2 * layers * src_rows * per * count * width,
            bytes_accessed=2 * layers * (src_rows + per * count) * width,
            transcendentals=0,
        )

    first_call = pl.pallas_call(
        functools.partial(first_kernel, patch_count, req_count),
        out_shape=[
            jax.ShapeDtypeStruct((src_rows, src_rows), jnp.bfloat16),
            jax.ShapeDtypeStruct((SUBLANES, src_rows), jnp.bfloat16),
            jax.ShapeDtypeStruct(image_rows.shape, jnp.bfloat16),
        ]
        + [chunk],
        in_specs=[hbm] * 3,
        out_specs=[vmem] * 4,
        scratch_shapes=[
            pltpu.VMEM((1, src_rows), jnp.int32),
            pltpu.VMEM((1, src_rows), jnp.int32),
            pltpu.SemaphoreType.DMA((2,)),
            pltpu.SemaphoreType.DMA((layers,)),
        ],
        cost_estimate=cost(1),
        compiler_params=pltpu.CompilerParams(vmem_limit_bytes=VMEM_LIMIT),
        name="group_first",
    )
    choose, places, rows, *first = first_call(
        in_hbm(patch_map.reshape(1, src_rows)),
        in_hbm(image_places.reshape(1, src_rows)),
        in_hbm(image_rows),
    )
    rest_call = pl.pallas_call(
        functools.partial(rest_kernel, 1, per),
        out_shape=[chunk] * (groups - 1),
        in_specs=[vmem] * 3,
        out_specs=[vmem] * (groups - 1),
        cost_estimate=cost(groups - 1),
        compiler_params=pltpu.CompilerParams(vmem_limit_bytes=VMEM_LIMIT),
        name="group_rest",
    )
    rest = rest_call(choose, places, rows)
    return [*first, *rest]


def heads_of(line, group):
    row = lax.broadcasted_iota(jnp.int32, (SUBLANES, HEAD_DIM), 0)
    tiles = []
    for g in range(KV_HEADS):
        tile = jnp.zeros((SUBLANES, HEAD_DIM), jnp.float32)
        for i in range(group):
            h = g * group + i
            tile = jnp.where(row == i, line[:, h * HEAD_DIM : (h + 1) * HEAD_DIM], tile)
        tiles.append(tile)
    return jnp.concatenate(tiles, axis=0).astype(jnp.bfloat16)


def attend(queries, keys, values, used, scale, least=None):
    def tile(rows, n):
        return rows[n * SUBLANES : (n + 1) * SUBLANES]

    scores = jnp.concatenate(
        [
            lax.dot_general(
                tile(queries, n), key, (((1,), (1,)), ((), ())), preferred_element_type=jnp.float32
            )
            for n, key in enumerate(keys)
        ],
        axis=0,
    )
    scores = scores * scale
    if used is not None:
        scores = jnp.where(used, scores, MASKED)
    top = jnp.max(scores, axis=1, keepdims=True)
    if least is not None:
        top = jnp.maximum(top, least)
    weights = jnp.exp(scores - top)
    if used is not None:
        weights = jnp.where(used, weights, 0.0)
    total = jnp.sum(weights, axis=1, keepdims=True)
    rounded = weights.astype(jnp.bfloat16)
    summed = jnp.concatenate(
        [
            jnp.dot(tile(rounded, n), value, preferred_element_type=jnp.float32)
            for n, value in enumerate(values)
        ],
        axis=0,
    )
    return top, total, summed


def text_kernel(scale, len_ref, query_ref, text_ref, q_ref, top_ref, total_ref, sum_ref):
    text_dev, width = text_ref.shape
    group = query_ref.shape[1] // HEAD_DIM // KV_HEADS
    queries = heads_of(query_ref[...].astype(jnp.float32), group)
    q_ref[...] = queries
    rows = KV_HEADS * SUBLANES
    positions = lax.axis_index("seq") * text_dev + lax.broadcasted_iota(
        jnp.int32, (rows, text_dev), 1
    )
    keys = [text_ref[:, g * HEAD_DIM : (g + 1) * HEAD_DIM] for g in range(KV_HEADS)]
    values = [
        text_ref[:, width // 2 + g * HEAD_DIM : width // 2 + (g + 1) * HEAD_DIM]
        for g in range(KV_HEADS)
    ]
    top, total, summed = attend(queries, keys, values, positions < len_ref[0], scale)
    top_ref[...] = jnp.broadcast_to(top, (rows, LANES))
    total_ref[...] = jnp.broadcast_to(total, (rows, LANES))
    sum_ref[...] = summed


def text_part(query, text_cache, text_len, scale):
    layers, _, query_width = query.shape
    text_dev, width = text_cache.shape[2:]
    rows = KV_HEADS * SUBLANES
    part = pl.BlockSpec((None, rows, LANES), lambda layer, _: (layer, 0, 0))
    return pl.pallas_call(
        functools.partial(text_kernel, scale),
        out_shape=[
            jax.ShapeDtypeStruct((layers, rows, HEAD_DIM), jnp.bfloat16),
            jax.ShapeDtypeStruct((layers, rows, LANES), jnp.float32),
            jax.ShapeDtypeStruct((layers, rows, LANES), jnp.float32),
            jax.ShapeDtypeStruct((layers, rows, HEAD_DIM), jnp.float32),
        ],
        grid_spec=pltpu.PrefetchScalarGridSpec(
            num_scalar_prefetch=1,
            grid=(layers,),
            in_specs=[
                pl.BlockSpec((None, 1, query_width), lambda layer, _: (layer, 0, 0)),
                pl.BlockSpec((None, None, text_dev, width), lambda layer, _: (layer, 0, 0, 0)),
            ],
            out_specs=[part] * 4,
        ),
        cost_estimate=pl.CostEstimate(
            flops=8 * layers * SUBLANES * LANES * text_dev * width,
            bytes_accessed=2 * layers * text_dev * width,
            transcendentals=layers * rows * text_dev,
        ),
        compiler_params=pltpu.CompilerParams(vmem_limit_bytes=VMEM_LIMIT),
        name="text_part",
    )(text_len, query, in_hbm(text_cache))


def image_columns(chunks, layers):
    blocks = 2 * KV_HEADS
    per = (chunks[0].shape[0] - SUBLANES) // layers // blocks

    def column(layer, c):
        span = pl.ds((layer * blocks + c) * per, per)
        return jnp.concatenate([chunk[span, :] for chunk in chunks], axis=0)

    keys = [column(layer, g) for layer in range(layers) for g in range(KV_HEADS)]
    values = [column(layer, KV_HEADS + g) for layer in range(layers) for g in range(KV_HEADS)]
    return keys, values


def join_image(scale, chunks, used, q_ref, top_in, total_in, sum_in):
    layers, rows, _ = q_ref.shape
    lines = layers * rows
    keys, values = image_columns(chunks, layers)
    queries = q_ref[...].reshape(lines, HEAD_DIM)
    old_top = top_in[...].reshape(lines, LANES)[:, :1]
    top, total, summed = attend(queries, keys, values, used, scale, old_top)
    factor = jnp.exp(old_top - top)
    total += factor * total_in[...].reshape(lines, LANES)[:, :1]
    summed += factor * sum_in[...].reshape(lines, LANES)
    return top, total, summed


def pack_part(top, total, summed):
    shape = summed.shape
    row = lax.broadcasted_iota(jnp.int32, shape, len(shape) - 2)
    lane = lax.broadcasted_iota(jnp.int32, shape, len(shape) - 1)
    stats = jnp.where(lane == row, top, jnp.where(lane == row + LANES // 2, total, 0.0))
    stats = jnp.sum(stats, axis=-2, keepdims=True)
    return jnp.where(row == SUBLANES - 1, stats, summed)


def unpack_part(tiles):
    shape = tiles.shape
    row = lax.broadcasted_iota(jnp.int32, shape, len(shape) - 2)
    lane = lax.broadcasted_iota(jnp.int32, shape, len(shape) - 1)
    stats = jnp.broadcast_to(tiles[..., SUBLANES - 1 :, :], shape)
    top = jnp.sum(jnp.where(lane == row, stats, 0.0), axis=-1, keepdims=True)
    total = jnp.sum(jnp.where(lane == row + LANES // 2, stats, 0.0), axis=-1, keepdims=True)
    return top, total, tiles


def merge_parts(parts, used=None):
    tiled = (parts[0].shape[0] // SUBLANES, SUBLANES, LANES)
    parts = [unpack_part(part.reshape(tiled)) for part in parts]
    for n, part in enumerate(parts):
        if used is not None and used[n] is not None:
            parts[n] = [jnp.where(used[n], a, b) for a, b in zip(part, (MASKED, 0.0, 0.0))]
    top = functools.reduce(jnp.maximum, [part[0] for part in parts])
    factors = [jnp.exp(part[0] - top) for part in parts]
    total = sum(factor * part[1] for factor, part in zip(factors, parts))
    summed = sum(factor * part[2] for factor, part in zip(factors, parts))
    return top, total, summed


def store_packed(outs, packed, top, total, summed, layers):
    tiled = (layers, KV_HEADS, SUBLANES)
    tiles = pack_part(
        top.reshape(*tiled, 1), total.reshape(*tiled, 1), summed.reshape(*tiled, LANES)
    )
    for g in range(KV_HEADS):
        packed[g] = tiles[:, g].reshape(layers * SUBLANES, LANES)
    me = lax.axis_index("seq")
    for k in range(KV_HEADS):
        outs[k][...] = packed[me ^ k]


def here_kernel(scale, groups, sure, outer, q_ref, top_in, total_in, sum_in, *refs):
    chunks, (top_ref, total_ref, sum_ref) = refs[:groups], refs[groups:]
    layers, rows = q_ref.shape[:2]
    per = (chunks[0].shape[0] - SUBLANES) // layers // (2 * KV_HEADS)
    limit = jnp.where(is_outer(outer), groups, sure) * per
    lines = layers * rows
    used = lax.broadcasted_iota(jnp.int32, (lines, groups * per), 1) < limit
    top, total, summed = join_image(scale, chunks, used, q_ref, top_in, total_in, sum_in)
    whole = (layers, rows, LANES)
    top_ref[...] = jnp.broadcast_to(top, (lines, LANES)).reshape(whole)
    total_ref[...] = jnp.broadcast_to(total, (lines, LANES)).reshape(whole)
    sum_ref[...] = summed.reshape(whole)


def here_part(parts, chunks, sure, outer, scale):
    groups = len(chunks)
    vmem = pl.BlockSpec(memory_space=pltpu.VMEM)
    rows = chunks[0].shape[0]
    made = pl.pallas_call(
        functools.partial(here_kernel, scale, groups, sure, outer),
        out_shape=[jax.ShapeDtypeStruct(part.shape, part.dtype) for part in parts[1:]],
        in_specs=[vmem] * (4 + groups),
        out_specs=[vmem] * 3,
        cost_estimate=pl.CostEstimate(
            flops=8 * SUBLANES * rows * LANES * groups,
            bytes_accessed=2 * rows * LANES * groups,
            transcendentals=SUBLANES * rows * groups,
        ),
        compiler_params=pltpu.CompilerParams(vmem_limit_bytes=VMEM_LIMIT),
        name="here_part",
    )(*parts, *chunks)
    return [parts[0], *made]


def last_kernel(scale, groups, q_ref, top_in, total_in, sum_in, *refs):
    chunks, outs, packed = refs[:groups], refs[groups:-1], refs[-1]
    parts = join_image(scale, chunks, None, q_ref, top_in, total_in, sum_in)
    store_packed(outs, packed, *parts, q_ref.shape[0])


def far_kernel(scale, count, *refs):
    queries, chunks = refs[:count], refs[count : 2 * count]
    outs, packed = refs[2 * count : -1], refs[-1]
    layers = queries[0].shape[0]
    group = queries[0].shape[1] // HEAD_DIM // KV_HEADS
    lines, keys, values = [], [], []
    for query, chunk in zip(queries, chunks):
        for layer in range(layers):
            lines.append(heads_of(query[pl.ds(layer, 1), :].astype(jnp.float32), group))
        new_keys, new_values = image_columns([chunk], layers)
        keys += new_keys
        values += new_values
    parts = attend(jnp.concatenate(lines, axis=0), keys, values, None, scale)
    store_packed(outs, packed, *parts, count * layers)


def seq_parts(kernel, operands, part_rows, chunk_rows, groups):
    shape = (part_rows, LANES)
    vmem = pl.BlockSpec(memory_space=pltpu.VMEM)
    return pl.pallas_call(
        kernel,
        out_shape=[jax.ShapeDtypeStruct(shape, jnp.float32)] * KV_HEADS,
        in_specs=[vmem] * len(operands),
        out_specs=[vmem] * KV_HEADS,
        scratch_shapes=[pltpu.VMEM((KV_HEADS,) + shape, jnp.float32)],
        cost_estimate=pl.CostEstimate(
            flops=8 * SUBLANES * chunk_rows * LANES * groups,
            bytes_accessed=2 * chunk_rows * LANES * groups,
            transcendentals=SUBLANES * chunk_rows * groups,
        ),
        compiler_params=pltpu.CompilerParams(vmem_limit_bytes=VMEM_LIMIT),
    )(*operands)


def seq_exchange(outs):
    arrived = [
        lax.ppermute(outs[k], "seq", [(s, s ^ k) for s in range(KV_HEADS)])
        for k in range(KV_HEADS - 1, 0, -1)
    ]
    return [outs[0], *arrived]


def merge_far_kernel(count, *refs):
    parts, outs = refs[:-count], refs[-count:]
    rows = parts[0].shape[0] // count
    merged = pack_part(*merge_parts([part[...] for part in parts]))
    merged = merged.reshape(parts[0].shape)
    for n, out in enumerate(outs):
        out[...] = merged[n * rows : (n + 1) * rows]


def merge_far(parts, count):
    rows = parts[0].shape[0] // count
    vmem = pl.BlockSpec(memory_space=pltpu.VMEM)
    return pl.pallas_call(
        functools.partial(merge_far_kernel, count),
        out_shape=[jax.ShapeDtypeStruct((rows, LANES), jnp.float32)] * count,
        in_specs=[vmem] * len(parts),
        out_specs=[vmem] * count,
        compiler_params=pltpu.CompilerParams(vmem_limit_bytes=VMEM_LIMIT),
        name="merge_far",
    )(*parts)


def is_outer(outer):
    patch = lax.axis_index("patch")
    return functools.reduce(jnp.logical_or, [patch == z for z in outer])


def place_kernel(owners, outer, *refs):
    out_hbm, out_ref, sems = refs[-3:]
    groups = len(owners)
    outside = is_outer(outer)

    def rows_of(k, span):
        first, *others = [refs[n][span, :] for n in owners[k]]
        return jnp.where(outside, others[0], first) if others else first

    layers, band, width = out_ref.shape
    blocks = width // LANES
    per = band // groups
    stores = [
        pltpu.make_async_copy(out_ref.at[layer], out_hbm.at[layer], sems.at[layer])
        for layer in range(layers)
    ]
    base = layers * blocks * per
    lane = lax.broadcasted_iota(jnp.int32, (SUBLANES, LANES), 1)
    tiles = []
    for tile in range(band // LANES):
        row = jnp.zeros((SUBLANES, LANES), jnp.float32)
        for k in range(groups):
            if k * per // LANES == tile:
                extra = rows_of(k, pl.ds(base, SUBLANES)).astype(jnp.float32)
                inside = (lane >= k * per % LANES) & (lane < k * per % LANES + per)
                row = jnp.where(inside, extra, row)
        tiles.append(row)
    digits = jnp.concatenate(tiles, axis=1).astype(jnp.int32)
    places = digits[0:1] + digits[1:2] * LANES
    down = lax.broadcasted_iota(jnp.int32, (band, band), 0)
    choose = jnp.where(down == places, 1.0, 0.0).astype(jnp.bfloat16)
    for layer in range(layers):
        for c in range(0, blocks, 2):
            spans = [pl.ds((layer * blocks + c + n) * per, per) for n in range(2)]
            columns = [
                jnp.concatenate([rows_of(k, span) for k in range(groups)], axis=0)
                for span in spans
            ]
            out_ref[layer, :, c * LANES : (c + 2) * LANES] = jnp.dot(
                choose, jnp.concatenate(columns, axis=1), preferred_element_type=jnp.float32
            ).astype(jnp.bfloat16)
        stores[layer].start()
    for store in stores:
        store.wait()


def place_rows(slots, outer, layers, band, width):
    operands = [chunk for slot in slots for chunk in slot]
    count = iter(range(len(operands)))
    owners = [[next(count) for _ in slot] for slot in slots]
    vmem = pl.BlockSpec(memory_space=pltpu.VMEM)
    return pl.pallas_call(
        functools.partial(place_kernel, owners, outer),
        out_shape=jax.ShapeDtypeStruct((layers, band, width), jnp.bfloat16),
        in_specs=[vmem] * len(operands),
        out_specs=pl.BlockSpec(memory_space=pltpu.HBM),
        scratch_shapes=[
            pltpu.VMEM((layers, band, width), jnp.bfloat16),
            pltpu.SemaphoreType.DMA((layers,)),
        ],
        cost_estimate=pl.CostEstimate(
            flops=2 * layers * band * band * width,
            bytes_accessed=4 * layers * band * width,
            transcendentals=0,
        ),
        compiler_params=pltpu.CompilerParams(vmem_limit_bytes=VMEM_LIMIT),
        name="place_rows",
    )(*operands)


def merge_kernel(group, sure, outer, *refs):
    parts, out_ref, lines = refs[:-2], refs[-2], refs[-1]
    inside = jnp.logical_not(is_outer(outer))
    used = [None if n < sure else inside for n in range(len(parts))]
    _, total, summed = merge_parts([part[...] for part in parts], used)
    result = summed / total
    for i in range(group):
        lines[:, i * HEAD_DIM : (i + 1) * HEAD_DIM] = result[:, i, :]
    out_ref[...] = lines[...].astype(jnp.bfloat16)


def merge(parts, sure, outer, layers, group):
    vmem = pl.BlockSpec(memory_space=pltpu.VMEM)
    return pl.pallas_call(
        functools.partial(merge_kernel, group, sure, outer),
        out_shape=jax.ShapeDtypeStruct((layers, group * HEAD_DIM), jnp.bfloat16),
        in_specs=[vmem] * len(parts),
        out_specs=vmem,
        scratch_shapes=[pltpu.VMEM((layers, group * HEAD_DIM), jnp.float32)],
        compiler_params=pltpu.CompilerParams(vmem_limit_bytes=VMEM_LIMIT),
        name="merge",
    )(*parts)


def exchange_pairs(patch_count, req_count, step, turn):
    pairs = []
    for patch in range(patch_count):
        for req in range(req_count):
            target = next(p for p in range(patch_count) if step_of(patch, p, patch_count) == step)
            pairs.append(
                (patch * req_count + req, target * req_count + (req + turn) % req_count)
            )
    return pairs


def fast_body(query, text_cache, text_len, image_rows, patch_map, image_places):
    layers = query.shape[0]
    patch_count = lax.axis_size("patch")
    req_count = lax.axis_size("req")
    band, width = image_rows.shape[1:]
    group = HEADS // KV_HEADS
    scale = 1.0 / math.sqrt(HEAD_DIM)
    slots = [[step * req_count + turn for turn in range(req_count)] for step in range(patch_count)]
    last = patch_count // 2 - 1
    late = slots[last]
    early = [k for step in range(patch_count - 1) if step != last for k in slots[step]]
    own, core = slots[-1][0], slots[-1][1:]
    pairs = [
        exchange_pairs(patch_count, req_count, k // req_count, k % req_count)
        for k in range(patch_count * req_count)
    ]
    axes = ("patch", "req")
    reach = {
        source: abs(target // req_count - source // req_count) for source, target in pairs[late[0]]
    }
    near = min(reach.values())
    outer = sorted({source // req_count for source, hops in reach.items() if hops > near})

    def stay(pair):
        return (pair[0], pair[0] // req_count * req_count + pair[1] % req_count)

    inner_pairs = {k: [p if reach[p[0]] == near else stay(p) for p in pairs[k]] for k in late}
    outer_pairs = {k: [p if reach[p[0]] > near else stay(p) for p in pairs[k]] for k in late}
    flat_query = query[:, 0]

    def send(value, some):
        return lax.ppermute(value, axes, some)

    far_queries = [
        send(flat_query, [(target, source) for source, target in inner_pairs[k]])
        for k in late
    ]
    grouped = group_rows(patch_map, image_places, image_rows, patch_count, req_count)
    arrived = {own: [grouped[own]]}
    for k in early + core:
        arrived[k] = [send(grouped[k], pairs[k])]
    for k in late:
        arrived[k] = [send(grouped[k], some) for some in (inner_pairs[k], outer_pairs[k])]
    chunk_rows = grouped[0].shape[0]
    part_rows = layers * SUBLANES
    far = seq_parts(
        functools.partial(far_kernel, scale, len(late)),
        [*far_queries, *(grouped[k] for k in late)],
        len(late) * part_rows,
        chunk_rows,
        len(late),
    )
    far = merge_far(seq_exchange(far), len(late))
    far = [send(far[n], inner_pairs[k]) for n, k in enumerate(late)]
    text = text_part(query, text_cache, text_len, scale)
    here = [arrived[k][0] for k in early[:-LAST_CHUNKS] + core + [own]]
    sure = len(here)
    here += [arrived[k][1] for k in late]
    ends = [arrived[k][0] for k in early[-LAST_CHUNKS:]]
    parts = seq_parts(
        functools.partial(last_kernel, scale, len(ends)),
        [*here_part(text, here, sure, outer, scale), *ends],
        part_rows,
        chunk_rows,
        len(ends),
    )
    attended = merge([*seq_exchange(parts), *far], KV_HEADS, outer, layers, group)
    image_cache = place_rows(
        [arrived[k] for k in range(len(grouped))], outer, layers, band, width
    )
    return attended[:, None, :], image_cache[:, None]


def plain_body(query, text_cache, text_len, image_rows, patch_map, image_places):
    layers, req_dev, query_width = query.shape
    text_dev = text_cache.shape[2]
    full_width = text_cache.shape[3]
    kv_width = full_width // 2
    head_dim = HEAD_DIM
    kv_heads = KV_HEADS
    heads = HEADS
    group = heads // kv_heads
    src_rows = image_rows.shape[1]
    patch_count = lax.axis_size("patch")
    req_count = lax.axis_size("req")
    seq_count = lax.axis_size("seq")
    seq_index = lax.axis_index("seq")
    per_source = src_rows // (patch_count * req_count * req_dev)
    band_size = per_source * patch_count * req_count
    scale = 1.0 / math.sqrt(head_dim)
    order = jnp.argsort(patch_map, stable=True)
    grouped = jnp.take(image_rows, order, axis=1)
    grouped_places = jnp.take(image_places, order)
    sending = grouped.reshape(layers, patch_count * req_count, req_dev, per_source, full_width)
    arrived = lax.all_to_all(sending, ("patch", "req"), split_axis=1, concat_axis=3, tiled=True)
    place_send = grouped_places.reshape(patch_count * req_count, req_dev, per_source)
    arrived_places = lax.all_to_all(
        place_send, ("patch", "req"), split_axis=0, concat_axis=2, tiled=True
    )
    image_block = arrived.reshape(layers, req_dev, band_size, full_width)
    local_places = arrived_places.reshape(req_dev, band_size) - seq_index * band_size
    inverse = jnp.argsort(local_places, axis=1)
    image_cache = jnp.take_along_axis(image_block, inverse[None, :, :, None], axis=2)
    queries = query.reshape(layers, req_dev, kv_heads, group, head_dim)
    text_keys = text_cache[..., :kv_width].reshape(layers, req_dev, text_dev, kv_heads, head_dim)
    text_values = text_cache[..., kv_width:].reshape(layers, req_dev, text_dev, kv_heads, head_dim)
    image_keys = image_block[..., :kv_width].reshape(layers, req_dev, band_size, kv_heads, head_dim)
    image_values = image_block[..., kv_width:].reshape(
        layers, req_dev, band_size, kv_heads, head_dim
    )
    positions = seq_index * text_dev + jnp.arange(text_dev, dtype=jnp.int32)
    used = positions[None, :] < text_len[:, None]
    text_raw = (
        jnp.einsum("lrkgd,lrtkd->lrkgt", queries, text_keys, preferred_element_type=jnp.float32)
        * scale
    )
    text_scores = jnp.where(used[None, :, None, None, :], text_raw, -jnp.inf)
    image_scores = (
        jnp.einsum("lrkgd,lrtkd->lrkgt", queries, image_keys, preferred_element_type=jnp.float32)
        * scale
    )
    local_top = jnp.maximum(jnp.max(text_scores, axis=-1), jnp.max(image_scores, axis=-1))
    text_weights = jnp.exp(text_scores - local_top[..., None])
    image_weights = jnp.exp(image_scores - local_top[..., None])
    local_total = jnp.sum(text_weights, axis=-1) + jnp.sum(image_weights, axis=-1)
    text_rounded = text_weights.astype(jnp.bfloat16)
    image_rounded = image_weights.astype(jnp.bfloat16)
    local_values = jnp.einsum(
        "lrkgt,lrtkd->lrkgd", image_rounded, image_values, preferred_element_type=jnp.float32
    )
    local_values = local_values + jnp.einsum(
        "lrkgt,lrtkd->lrkgd", text_rounded, text_values, preferred_element_type=jnp.float32
    )
    width_dev = query_width // seq_count
    top = lax.pmax(local_top, "seq")
    factor = jnp.exp(local_top - top)
    scaled_total = factor * local_total
    scaled_values = factor[..., None] * local_values
    total_sum, value_sum = lax.psum((scaled_total, scaled_values), "seq")
    result = (value_sum / total_sum[..., None]).reshape(layers, req_dev, query_width)
    attended = lax.dynamic_slice_in_dim(result, seq_index * width_dev, width_dev, 2).astype(
        jnp.bfloat16
    )
    return (attended, image_cache)


def body(query, text_cache, text_len, image_rows, patch_map, image_places):
    groups = lax.axis_size("patch") * lax.axis_size("req")
    band = image_rows.shape[1]
    per = band // groups
    fast = (
        query.shape[1] == 1
        and lax.axis_size("patch") == 4
        and groups <= MOST_GROUPS
        and band == per * groups
        and band % LANES == 0
        and per % 16 == 0
        and LANES % per == 0
        and lax.axis_size("seq") == KV_HEADS
        and HEADS // KV_HEADS < SUBLANES
    )
    chosen = fast_body if fast else plain_body
    return chosen(query, text_cache, text_len, image_rows, patch_map, image_places)


def solution(mesh):
    return jax.shard_map(
        body,
        mesh=mesh,
        in_specs=(
            P(None, ("patch", "req"), None),
            P(None, ("patch", "req"), "seq", None),
            P(("patch", "req")),
            P(None, ("patch", "seq", "req"), None),
            P(("patch", "seq", "req")),
            P(("patch", "seq", "req")),
        ),
        out_specs=(P(None, ("patch", "req"), "seq"), P(None, ("patch", "req"), "seq", None)),
        check_vma=False,
    )
```
